256 devices in a mesh: space: 32 (over y, x, z_hi), coil: 8 (over z_lo, core).
Axes of the slice: x: 4, y: 4, z: 8 (z_hi: 2, z_lo: 4; z = z_hi * 4 + z_lo), core: 2. Of those that a mesh axis runs over, the one named last changes fastest.
Arguments:
- state: bfloat16 [32, 2, 1024, 768], P(None, None, 'space', 'coil'), may hold values from -6 to 6
- sens: float32 [2, 16, 2, 1024, 768], P(None, 'coil', None, 'space'), may hold values from -2 to 2
- kdata: float32 [2, 16, 2, 768, 1024], P(None, 'coil', None, 'space'), may hold values from -3 to 3
- mask: int32 [768, 1024], P('space'), may hold values 0 or 1
- inject: float32 [32, 2], replicated, may hold values from -4 to 4
- kernels: bfloat16 [4, 27, 16, 16], replicated, may hold values from -0.3125 to 0.3125
- biases: float32 [4, 16], replicated, may hold values from -3 to 3
- mixers: bfloat16 [4, 16, 16], replicated, may hold values from -1.5 to 1.5
Outputs:
- new_state: bfloat16 [32, 2, 1024, 768], P(None, None, 'space', 'coil')
- gradient: float32 [2, 2, 1024, 768], P(None, None, 'space', 'coil')
The draws below stay inside these ranges and needn't reach their ends.
All inputs are finite; a program needn't handle non-finite values. No bound on the sum of `mask` on one device may be relied on, other than what follows from the above.
Results may differ from the reference program's by a relative error of at most 0.015.
Values may be sent and summed in bfloat16 or wider, within the bound.
No kernel may reach another device: no remote copies, remote signals or barrier semaphores. Data moves between devices by JAX's collectives and lax.ppermute only.
A program may use at most 64 MiB of HBM per device.

```python
import jax
import jax.numpy as jnp
from jax import lax

NPE = 1024
NPAR = 768
COILS = 16
CH = 32
POS = 2
COUPLINGS = 4


def with_ends(result, key, smallest, largest):
    index_at = [jax.random.randint(jax.random.fold_in(key, axis), (), 0, length) for axis, length in enumerate(result.shape)]
    widest = result.shape.index(max(result.shape))
    neighbour = index_at[:widest] + [(index_at[widest] + 1) % result.shape[widest]] + index_at[widest + 1:]
    return result.at[tuple(index_at)].set(smallest).at[tuple(neighbour)].set(largest)


def steps_of(stream_key, dims, cuts, least, largest):
    loudness = 1.0
    for dim, blocks in cuts:
        steps = jax.random.uniform(jax.random.fold_in(jax.random.fold_in(stream_key, 6), dim), (blocks,), jnp.float32, least / len(cuts), largest / len(cuts))
        loudness = loudness * jnp.repeat(jnp.exp(steps), dims[dim] // blocks).reshape((-1,) + (1,) * (len(dims) - 1 - dim))
    return loudness


def normal_values(key, dims, scale, reach, cuts=(), held_as=jnp.bfloat16):
    values = scale * jax.random.normal(key, dims, jnp.float32)
    if cuts:
        values = values * steps_of(key, dims, cuts, -0.22, 0.18)
    return jnp.clip(values, -reach, reach).astype(held_as)


def setup_inputs(seed: int = 0) -> dict:
    key_of = jax.random.split(jax.random.key(seed), 9)
    state = normal_values(key_of[0], (CH, POS, NPE, NPAR), 1.0, 6.0, ((2, 32), (3, 8)))
    sens = normal_values(key_of[1], (2, COILS, POS, NPE, NPAR), 0.25, 2.0, ((1, 8), (3, 32)), jnp.float32)
    kdata = normal_values(key_of[2], (2, COILS, POS, NPAR, NPE), 0.35, 3.0, ((1, 8), (3, 32)), jnp.float32)
    mask = with_ends((jax.random.randint(key_of[3], (NPAR, NPE), 0, 3) < 1).astype(jnp.int32), jax.random.fold_in(key_of[3], 1), 0, 1)
    inject = normal_values(key_of[4], (CH, 2), 2 ** -0.5, 4.0, (), jnp.float32)
    kernels = normal_values(key_of[5], (COUPLINGS, 27, CH // 2, CH // 2), (27 * (CH // 2)) ** -0.5, 0.3125)
    biases = normal_values(key_of[6], (COUPLINGS, CH // 2), 0.5, 3.0, (), jnp.float32)
    mixers = normal_values(key_of[7], (COUPLINGS, CH // 2, CH // 2), (CH // 2) ** -0.5, 1.5)
    return dict(state=state, sens=sens, kdata=kdata, mask=mask, inject=inject, kernels=kernels, biases=biases, mixers=mixers)


def coupling(source, target, kernel, bias, mixer):
    weight = jnp.transpose(kernel.astype(jnp.float32).reshape(3, 3, 3, kernel.shape[1], kernel.shape[2]), (3, 4, 0, 1, 2))
    raw = lax.conv_general_dilated(source.astype(jnp.float32)[None], weight, (1, 1, 1), "SAME", dimension_numbers=("NCDHW", "OIDHW", "NCDHW"), precision=lax.Precision.HIGHEST)[0]
    hidden = jax.nn.relu(raw + bias[:, None, None, None]).astype(jnp.bfloat16)
    mixed = jnp.einsum("oi,ipqr->opqr", mixer.astype(jnp.float32), hidden.astype(jnp.float32), precision=lax.Precision.HIGHEST)
    return (target.astype(jnp.float32) + mixed).astype(jnp.bfloat16)


def reference(state, sens, kdata, mask, inject, kernels, biases, mixers):
    estimate = state[0].astype(jnp.float32) + 1j * state[1].astype(jnp.float32)
    weight = mask.astype(jnp.float32)

    def one_coil(total, pieces):
        sens_real, sens_imag, data_real, data_imag = pieces
        profile = sens_real + 1j * sens_imag
        spectrum = jnp.fft.fft2(profile * estimate, axes=(-2, -1), norm="ortho")
        spectrum = jnp.swapaxes(spectrum, -1, -2)
        residual = weight * (spectrum - (data_real + 1j * data_imag))
        image = jnp.fft.ifft2(jnp.swapaxes(residual, -1, -2), axes=(-2, -1), norm="ortho")
        term = jnp.conj(profile) * image
        return total + jnp.stack([jnp.real(term), jnp.imag(term)]).astype(jnp.float32), None

    start = jnp.zeros((2, POS, NPE, NPAR), jnp.float32)
    gradient, _ = lax.scan(one_coil, start, (sens[0], sens[1], kdata[0], kdata[1]))
    added = jnp.einsum("cg,gpqr->cpqr", inject, gradient, precision=lax.Precision.HIGHEST)
    merged = (state.astype(jnp.float32) + added).astype(jnp.bfloat16)
    half = CH // 2
    first = merged[:half]
    second = merged[half:]
    for layer in range(COUPLINGS):
        if layer % 2 == 0:
            second = coupling(first, second, kernels[layer], biases[layer], mixers[layer])
        else:
            first = coupling(second, first, kernels[layer], biases[layer], mixers[layer])
    new_state = jnp.concatenate([first, second], axis=0)
    return new_state, gradient
```

```python
import numpy as np

import jax
import jax.numpy as jnp
from jax import lax
from jax.experimental import pallas as pl
from jax.experimental.pallas import tpu as pltpu
from jax.sharding import PartitionSpec as P

F32 = jnp.float32
BF16 = jnp.bfloat16
REACH = 4
VMEM = pl.BlockSpec(memory_space=pltpu.VMEM)
SMEM = pl.BlockSpec(memory_space=pltpu.SMEM)


def call(body, outs, scratch, name, in_specs):
    single = not isinstance(outs, (list, tuple))
    return pl.pallas_call(
        body,
        out_shape=outs,
        in_specs=in_specs,
        out_specs=VMEM if single else [VMEM] * len(outs),
        scratch_shapes=scratch,
        name=name,
    )


def dft_factors(length, columns, step):
    columns = np.asarray(columns)[None, :]
    coarse = (step * np.arange(length // step))[:, None] * columns % length
    fine = np.arange(step)[:, None] * columns % length
    angle_coarse = coarse * (2.0 * np.pi / length)
    angle_fine = fine * (2.0 * np.pi / length)
    scale = 1.0 / np.sqrt(length)
    return [
        np.asarray(part, np.float32)
        for part in (
            np.cos(angle_coarse) * scale,
            np.sin(angle_coarse) * scale,
            np.cos(angle_fine),
            np.sin(angle_fine),
        )
    ]


def dft_tables(length, columns, step):
    cos_a, sin_a, cos_b, sin_b = [jnp.asarray(part) for part in dft_factors(length, columns, step)]
    cos_a, sin_a = cos_a[:, None, :], sin_a[:, None, :]
    cos_b, sin_b = cos_b[None], sin_b[None]
    cos = (cos_a * cos_b - sin_a * sin_b).astype(BF16)
    sin = (sin_a * cos_b + cos_a * sin_b).astype(BF16)
    return cos.reshape(length, -1), sin.reshape(length, -1)


def swap_groups(tiles, group):
    tiles = list(tiles)
    count = len(tiles)
    lane = lax.broadcasted_iota(jnp.int32, tiles[0].shape, 1)
    bit = count // 2
    while bit:
        shift = bit * group
        high = (lane // shift) % 2 == 1
        for low in range(count):
            if low & bit:
                continue
            a, b = tiles[low], tiles[low | bit]
            tiles[low] = jnp.where(high, pltpu.roll(b, shift, 1), a)
            tiles[low | bit] = jnp.where(high, b, pltpu.roll(a, 128 - shift, 1))
        bit //= 2
    return tiles


def nn(a, b):
    return lax.dot_general(a, b, (((1,), (0,)), ((), ())), preferred_element_type=F32)


def nt(a, b):
    return lax.dot_general(a, b, (((1,), (1,)), ((), ())), preferred_element_type=F32)


def forward_columns(est_ref, sens_ref, cos_ref, sin_ref, out_ref, img_ref):
    owners = est_ref.shape[0]
    rows = sens_ref.shape[3]
    npar = sens_ref.shape[4]
    width = npar // owners
    lane = lax.broadcasted_iota(jnp.int32, (rows, 128), 1)
    coils, spots = sens_ref.shape[1:3]
    for spot in range(spots):
        for tile in range(npar // 128):
            full = []
            for part in range(2):
                value = None
                for owner in range(128 * tile // width, (128 * tile + 127) // width + 1):
                    at = width * owner - 128 * tile
                    piece = est_ref[owner, part, spot].astype(F32)
                    if at % 128:
                        piece = pltpu.roll(piece, at % 128, 1)
                    value = piece if value is None else jnp.where(lane >= at, piece, value)
                full.append(value)
            est_re, est_im = full
            cols = pl.ds(128 * tile, 128)
            for coil in range(coils):
                sens_re = sens_ref[0, coil, spot, :, cols]
                sens_im = sens_ref[1, coil, spot, :, cols]
                row = (coil * spots + spot) * rows
                img_ref[pl.ds(row, rows), cols] = (sens_re * est_re - sens_im * est_im).astype(BF16)
                img_ref[pl.ds(128 + row, rows), cols] = (sens_re * est_im + sens_im * est_re).astype(BF16)
    img = img_ref[...]
    step = 256
    for start in range(0, npar, step):
        here = pl.ds(start, step)
        by_cos = nt(cos_ref[here, :], img)
        by_sin = nt(sin_ref[here, :], img)
        out_ref[here, 0:128] = (by_cos[:, :128] + by_sin[:, 128:]).astype(BF16)
        out_ref[here, 128:256] = (by_cos[:, 128:] - by_sin[:, :128]).astype(BF16)


def consistency(recv_ref, kdata_ref, mask_ref, cos_ref, sin_ref, out_ref, x_ref, res_ref):
    lines = mask_ref.shape[0]
    npe = mask_ref.shape[1]
    sources = recv_ref.shape[0] // lines
    half = 4 * lines
    for quad in range(sources // 4):
        stacked = []
        for part in range(2):
            tiles = [
                recv_ref[pl.ds((4 * quad + s) * lines, lines), pl.ds(128 * part, 128)].astype(F32) for s in range(4)
            ]
            stacked += swap_groups(tiles, 32)
        x_ref[:, pl.ds(128 * quad, 128)] = jnp.concatenate(stacked, axis=0).astype(BF16)
    x = x_ref[...]
    step = 256
    for start in range(0, npe, step):
        here = pl.ds(start, step)
        by_cos = nn(x, cos_ref[:, here])
        by_sin = nn(x, sin_ref[:, here])
        sampled = mask_ref[:, here].astype(F32)
        sampled = jnp.concatenate([sampled] * 4, axis=0)
        data = [
            jnp.concatenate([kdata_ref[part, c, p, :, here] for c in range(2) for p in range(2)], axis=0)
            for part in range(2)
        ]
        real = sampled * (by_cos[:half] + by_sin[half:] - data[0])
        imag = sampled * (by_cos[half:] - by_sin[:half] - data[1])
        res_ref[0:half, here] = real.astype(BF16)
        res_ref[half : 2 * half, here] = imag.astype(BF16)
    res = res_ref[...]
    for start in range(0, cos_ref.shape[1], step):
        here = pl.ds(start, step)
        by_cos = nn(res, cos_ref[:, here])
        by_sin = nn(res, sin_ref[:, here])
        parts = (by_cos[:half] - by_sin[half:], by_cos[half:] + by_sin[:half])
        for tile in range(step // 128):
            at = slice(128 * tile, 128 * tile + 128)
            tiles = [part[lines * g : lines * (g + 1), at] for part in parts for g in range(4)]
            if start < npe:
                quad = start // 128 + tile
                for part in range(2):
                    for s, value in enumerate(swap_groups(tiles[4 * part : 4 * part + 4], 32)):
                        out_ref[pl.ds((4 * quad + s) * lines, lines), pl.ds(128 * part, 128)] = value.astype(BF16)
            else:
                group = (start - npe) // 128 + tile
                for s, value in enumerate(swap_groups(tiles, 8)):
                    value = value.astype(BF16)
                    for half_id in range(2):
                        owner = 16 * group + 8 * half_id + s
                        out_ref[pl.ds(owner * lines, lines), 256:384] = value


def backward_columns(recv_ref, sens_ref, edge_ref, place_ref, cos_ref, sin_ref, out_ref, part_ref):
    npar = sens_ref.shape[4]
    coils, spots, rows = sens_ref.shape[1:4]
    cells = coils * spots * rows
    edges = coils * spots * 2 * REACH
    turned = recv_ref[...].astype(F32).T
    low = place_ref[0] // 8 % 2 == 0
    border = jnp.where(low, turned[2 * cells : 2 * cells + 2 * edges], turned[2 * cells + 2 * edges :])
    x = jnp.concatenate([turned[: 2 * cells], border], axis=0).astype(BF16)
    step = 256
    for start in range(0, npar, step):
        here = pl.ds(start, step)
        by_cos = nn(x, cos_ref[:, here])
        by_sin = nn(x, sin_ref[:, here])
        for first, count, profile_ref, offset in ((0, cells, sens_ref, 0), (2 * cells, edges, edge_ref, rows)):
            second = first + count
            last = second + count
            real = by_cos[first:second] - by_sin[second:last]
            imag = by_cos[second:last] + by_sin[first:second]
            per_coil = count // coils
            height = per_coil // spots
            sums = [0.0, 0.0]
            for coil in range(coils):
                profile = [
                    jnp.concatenate([profile_ref[part, coil, spot, :, here] for spot in range(spots)], axis=0).astype(F32)
                    for part in range(2)
                ]
                re = real[coil * per_coil : (coil + 1) * per_coil]
                im = imag[coil * per_coil : (coil + 1) * per_coil]
                sums[0] = sums[0] + (profile[0] * re + profile[1] * im)
                sums[1] = sums[1] + (profile[0] * im - profile[1] * re)
            for part in range(2):
                for spot in range(spots):
                    row = (part * spots + spot) * (rows + 2 * REACH) + offset
                    part_ref[pl.ds(row, height), here] = sums[part][spot * height : (spot + 1) * height]
    total = part_ref.shape[0]
    owners = out_ref.shape[0] // total
    width = npar // owners
    lane = lax.broadcasted_iota(jnp.int32, (total, 128), 1)
    count = npar // 128
    for owner in range(owners):
        tile, off = divmod(width * owner, 128)
        value = part_ref[:, pl.ds(128 * tile, 128)]
        if off:
            value = pltpu.roll(value, 128 - off, 1)
            if tile + 1 < count:
                following = pltpu.roll(part_ref[:, pl.ds(128 * (tile + 1), 128)], 128 - off, 1)
                value = jnp.where((lane >= 128 - off) & (lane < 112), following, value)
        elif tile:
            value = jnp.where(lane >= 112, part_ref[:, pl.ds(128 * (tile - 1), 128)], value)
        out_ref[pl.ds(owner * total, total), :] = value.astype(BF16)


def couple(
    recv_ref, state_ref, place_ref, inject_ref, weight_ref, bias_ref, mixer_ref, new_ref, grad_ref, wide_ref, a_ref, b_ref
):
    channels, spots, tall = state_ref.shape[:3]
    rows = tall - 2 * REACH
    half = channels // 2
    block = spots * half
    total = 2 * spots * tall
    owners = recv_ref.shape[0] // total
    cols = grad_ref.shape[3]
    grad = recv_ref[0:total, :].astype(F32)
    for owner in range(1, owners):
        grad = grad + recv_ref[pl.ds(owner * total, total), :].astype(F32)
    for part in range(2):
        for spot in range(spots):
            row = (part * spots + spot) * tall
            grad_ref[part, spot] = grad[row : row + rows, :cols]
    lane = lax.broadcasted_iota(jnp.int32, (tall, 128), 1)
    row = lax.broadcasted_iota(jnp.int32, (tall, 128), 0)
    col_id = place_ref[1] * cols + jnp.where(lane < 112, lane, lane - 128)
    row_id = place_ref[0] * rows + jnp.where(row < rows + REACH, row, row - tall)
    inside = (col_id >= 0) & (col_id < cols * owners) & (row_id >= 0) & (row_id < place_ref[2])
    for channel in range(channels):
        for spot in range(spots):
            real = grad[spot * tall : (spot + 1) * tall]
            imag = grad[(spots + spot) * tall : (spots + spot + 1) * tall]
            added = inject_ref[channel, 0] * real + inject_ref[channel, 1] * imag
            merged = (state_ref[channel, spot].astype(F32) + added).astype(BF16).astype(F32)
            at = (channel // half * block + spot * half + channel % half) * tall
            wide_ref[pl.ds(at, tall), :] = jnp.where(inside, merged, 0.0)
    for i in range(tall):
        source = (i - REACH) % tall
        a_ref[pl.ds(i * block, block), :] = wide_ref[pl.ds(source, block, stride=tall), :].astype(BF16)
        b_ref[pl.ds(i * block, block), :] = wide_ref[pl.ds(block * tall + source, block, stride=tall), :].astype(BF16)
    keep = inside.astype(F32)
    for layer in range(weight_ref.shape[0]):
        source_ref, target_ref = (a_ref, b_ref) if layer % 2 == 0 else (b_ref, a_ref)
        weight = weight_ref[layer]
        mixer = mixer_ref[layer]
        bias = bias_ref[layer]
        for i in range(1 + layer, tall - 1 - layer, 2):
            cells = jnp.concatenate(
                [source_ref[pl.ds((j - 1) * block, 3 * block), :] for j in (i, i + 1)], axis=1
            )
            taps = nn(weight, cells)
            raw = []
            for j in range(2):
                at = slice(128 * j, 128 * j + 128)
                value = pltpu.roll(taps[0:block, at], 1, 1) + taps[block : 2 * block, at]
                value = value + pltpu.roll(taps[2 * block :, at], 127, 1)
                raw.append(jnp.maximum(value + bias, 0.0).astype(BF16))
            mixed = nn(mixer, jnp.concatenate(raw, axis=1))
            for j in range(2):
                here = pl.ds((i + j) * block, block)
                value = target_ref[here, :].astype(F32) + mixed[:, 128 * j : 128 * j + 128]
                source = (i + j - REACH) % tall
                value = value * keep[source : source + 1, :]
                target_ref[here, :] = value.astype(BF16)
    for i in range(REACH, REACH + rows):
        source = i - REACH
        wide_ref[pl.ds(source, block, stride=tall), :] = a_ref[pl.ds(i * block, block), :].astype(F32)
        wide_ref[pl.ds(block * tall + source, block, stride=tall), :] = b_ref[pl.ds(i * block, block), :].astype(F32)
    for channel in range(channels):
        for spot in range(spots):
            at = (channel // half * block + spot * half + channel % half) * tall
            new_ref[channel, spot] = wide_ref[pl.ds(at, rows), :][:, :cols].astype(BF16)


def coupling_weights(kernels, mixers):
    layers = kernels.shape[0]
    half = kernels.shape[2]
    taps = kernels.reshape(layers, 3, 3, 3, half, half)
    rows = []
    for out_spot in range(2):
        rows.append(jnp.stack([taps[:, in_spot - out_spot + 1] for in_spot in range(2)], axis=1))
    both = jnp.stack(rows, axis=1)
    weight = jnp.transpose(both, (0, 4, 1, 5, 3, 2, 6)).reshape(layers, 6 * half, 6 * half)
    zero = jnp.zeros_like(mixers)
    mixer = jnp.concatenate(
        [jnp.concatenate([mixers, zero], axis=2), jnp.concatenate([zero, mixers], axis=2)], axis=1
    )
    return weight, mixer


def swapped_edges(array, axis, dim):
    count = lax.axis_size(axis)
    ends = count - 1
    size = array.shape[dim]
    head = lax.slice_in_dim(array, 0, REACH, axis=dim)
    tail = lax.slice_in_dim(array, size - REACH, size, axis=dim)
    before = lax.ppermute(tail, axis, [(i, i + 1) for i in range(ends)])
    after = lax.ppermute(head, axis, [(i + 1, i) for i in range(ends)])
    return before, after


def per_device(state, sens, kdata, mask, inject, kernels, biases, mixers):
    channels, spots, rows, cols = state.shape
    coils = sens.shape[1]
    npar = sens.shape[4]
    npe = kdata.shape[4]
    lines = kdata.shape[3]
    groups = lax.axis_size("space")
    owners = lax.axis_size("coil")
    tall = rows + 2 * REACH
    place = jnp.stack([lax.axis_index("space"), lax.axis_index("coil"), jnp.int32(npe)]).astype(jnp.int32)

    estimate = jnp.pad(state[0:2], ((0, 0), (0, 0), (0, 0), (0, 128 - cols)))
    estimate = jnp.broadcast_to(estimate[None], (owners, *estimate.shape))
    estimate = lax.all_to_all(estimate, "coil", 0, 0, tiled=True)

    par_cos, par_sin = dft_tables(npar, np.arange(npar), 32)
    edge_columns = [
        (rows * d + r) % npe for d in range(groups) for r in (*range(rows, rows + REACH), *range(-REACH, 0))
    ]
    pe_cos, pe_sin = dft_tables(npe, [*range(npe), *edge_columns], 32)

    cells = coils * spots * rows
    sent = call(
        forward_columns,
        jax.ShapeDtypeStruct((npar, 2 * cells), BF16),
        [pltpu.VMEM((2 * cells, npar), BF16)],
        "forward_columns",
        [VMEM] * 4,
    )(estimate, sens, par_cos, par_sin)
    spectra = lax.all_to_all(sent, "space", 0, 0, tiled=True)

    sent = call(
        consistency,
        jax.ShapeDtypeStruct((npar, 384), BF16),
        [pltpu.VMEM((8 * lines, npe), BF16), pltpu.VMEM((8 * lines, npe), BF16)],
        "consistency",
        [VMEM] * 5,
    )(spectra, kdata, mask, pe_cos, pe_sin)
    returned = lax.all_to_all(sent, "space", 0, 0, tiled=True)

    above, below = swapped_edges(sens.astype(BF16), "space", 3)
    edge = jnp.concatenate([below, above], axis=3).astype(F32)

    sent = call(
        backward_columns,
        jax.ShapeDtypeStruct((owners * 2 * spots * tall, 128), BF16),
        [pltpu.VMEM((2 * spots * tall, npar), F32)],
        "backward_columns",
        [VMEM, VMEM, VMEM, SMEM, VMEM, VMEM],
    )(returned, sens, edge, place, par_cos, par_sin)
    shares = lax.all_to_all(sent, "coil", 0, 0, tiled=True)

    above, below = swapped_edges(state, "space", 2)
    wide = jnp.concatenate([state, below, above], axis=2)
    left, right = swapped_edges(wide, "coil", 3)
    gap = jnp.zeros((channels, spots, tall, 128 - cols - 2 * REACH), state.dtype)
    wide = jnp.concatenate([wide, right, gap, left], axis=3)

    weight, mixer = coupling_weights(kernels, mixers)
    block = channels // 2 * spots
    bias = jnp.broadcast_to(jnp.tile(biases, (1, spots))[:, :, None], (*biases.shape[:1], block, 128))
    new_state, gradient = call(
        couple,
        [
            jax.ShapeDtypeStruct(state.shape, BF16),
            jax.ShapeDtypeStruct((2, spots, rows, cols), F32),
        ],
        [
            pltpu.VMEM((2 * block * tall, 128), F32),
            pltpu.VMEM((block * tall, 128), BF16),
            pltpu.VMEM((block * tall, 128), BF16),
        ],
        "couple",
        [VMEM, VMEM, SMEM, SMEM, VMEM, VMEM, VMEM],
    )(shares, wide, place, inject, weight, bias, mixer)
    return (new_state, gradient)


def solution(mesh):
    return jax.shard_map(
        per_device,
        mesh=mesh,
        in_specs=(
            P(None, None, "space", "coil"),
            P(None, "coil", None, "space", None),
            P(None, "coil", None, "space", None),
            P("space", None),
            P(),
            P(),
            P(),
            P(),
        ),
        out_specs=(P(None, None, "space", "coil"), P(None, None, "space", "coil")),
        check_vma=False,
    )
```

```python
import numpy as np

import jax
import jax.numpy as jnp
from jax import lax
from jax.experimental import pallas as pl
from jax.experimental.pallas import tpu as pltpu
from jax.sharding import PartitionSpec as P

F32 = jnp.float32
BF16 = jnp.bfloat16
REACH = 4
FINE = 32
BATCH = 12
VMEM = pl.BlockSpec(memory_space=pltpu.VMEM)


def call(body, outs, scratch, name, *args):
    specs, values = [], []
    for arg in args:
        where, value = arg if isinstance(arg, tuple) else ("vmem", arg)
        if where != "plain":
            value = pltpu.with_memory_space_constraint(value, pltpu.HBM if where == "hbm" else pltpu.VMEM)
        specs.append(pl.BlockSpec(memory_space=pltpu.HBM) if where == "hbm" else VMEM)
        values.append(value)
    shapes = []
    for out in outs:
        shapes.append(pltpu.VMEM(*out) if isinstance(out, tuple) else out)
    return pl.pallas_call(
        body,
        out_shape=shapes,
        in_specs=specs,
        out_specs=[VMEM] * len(outs),
        scratch_shapes=[each if not isinstance(each, tuple) else pltpu.VMEM(*each) for each in scratch],
        compiler_params=pltpu.CompilerParams(vmem_limit_bytes=20 * 2**20),
        name=name,
    )(*values)


def in_hbm(value):
    return ("hbm", value)


def plain(value):
    return ("plain", value)


def table_copies(pairs, sems, step):
    blocks = []
    for start in range(0, pairs[0][0].shape[1], step):
        here = pl.ds(start, step)
        block = []
        for source, target in pairs:
            copy = pltpu.make_async_copy(source.at[:, here], target.at[:, here], sems.at[len(blocks) * len(pairs) + len(block)])
            copy.start()
            block.append(copy)
        blocks.append(block)
    return blocks


def arrived(block):
    for copy in block:
        copy.wait()


def dft_factors(length, columns, step):
    columns = np.asarray(columns)[None, :]
    coarse = (step * np.arange(length // step))[:, None] * columns % length
    fine = np.arange(step)[:, None] * columns % length
    angle_coarse = coarse * (2.0 * np.pi / length)
    angle_fine = fine * (2.0 * np.pi / length)
    scale = 1.0 / np.sqrt(length)
    parts = (np.cos(angle_coarse) * scale, np.sin(angle_coarse) * scale, np.cos(angle_fine), np.sin(angle_fine))
    return np.concatenate(parts).astype(np.float32)


def dft_tables(factors_ref, cos_ref, sin_ref):
    count = cos_ref.shape[0] // FINE
    cos_b = factors_ref[pl.ds(2 * count, FINE), :]
    sin_b = factors_ref[pl.ds(2 * count + FINE, FINE), :]
    for a in range(count):
        here = pl.ds(a * FINE, FINE)
        cos, sin = factors_ref[pl.ds(a, 1), :], factors_ref[pl.ds(count + a, 1), :]
        cos_ref[here, :] = (cos * cos_b - sin * sin_b).astype(BF16)
        sin_ref[here, :] = (sin * cos_b + cos * sin_b).astype(BF16)


def swap_groups(tiles, group):
    tiles = list(tiles)
    count = len(tiles)
    lane = lax.broadcasted_iota(jnp.int32, tiles[0].shape, 1)
    bit = count // 2
    while bit:
        shift = bit * group
        high = (lane // shift) % 2 == 1
        for low in range(count):
            if low & bit:
                continue
            a, b = tiles[low], tiles[low | bit]
            tiles[low] = jnp.where(high, pltpu.roll(b, shift, 1), a)
            tiles[low | bit] = jnp.where(high, b, pltpu.roll(a, 128 - shift, 1))
        bit //= 2
    return tiles


def nn(a, b):
    return lax.dot_general(a, b, (((1,), (0,)), ((), ())), preferred_element_type=F32)


def nt(a, b):
    return lax.dot_general(a, b, (((1,), (1,)), ((), ())), preferred_element_type=F32)


def forward_columns(est_ref, sens_ref, cos_hbm, sin_hbm, out_ref, img_ref, cos_ref, sin_ref, sems):
    blocks = table_copies([(cos_hbm, cos_ref), (sin_hbm, sin_ref)], sems, cos_ref.shape[1])
    owners = est_ref.shape[0]
    rows = sens_ref.shape[3]
    npar = sens_ref.shape[4]
    width = npar // owners
    lane = lax.broadcasted_iota(jnp.int32, (rows, 128), 1)
    coils, spots = sens_ref.shape[1:3]
    for spot in range(spots):
        for tile in range(npar // 128):
            full = []
            for part in range(2):
                value = None
                for owner in range(128 * tile // width, (128 * tile + 127) // width + 1):
                    at = width * owner - 128 * tile
                    piece = est_ref[owner, part, spot].astype(F32)
                    if at % 128:
                        piece = pltpu.roll(piece, at % 128, 1)
                    value = piece if value is None else jnp.where(lane >= at, piece, value)
                full.append(value)
            est_re, est_im = full
            cols = pl.ds(128 * tile, 128)
            for coil in range(coils):
                sens_re = sens_ref[0, coil, spot, :, cols]
                sens_im = sens_ref[1, coil, spot, :, cols]
                row = (coil * spots + spot) * rows
                img_ref[pl.ds(row, rows), cols] = (sens_re * est_re - sens_im * est_im).astype(BF16)
                img_ref[pl.ds(128 + row, rows), cols] = (sens_re * est_im + sens_im * est_re).astype(BF16)
    img = img_ref[...]
    arrived(blocks[0])
    step = 256
    for start in range(0, npar, step):
        here = pl.ds(start, step)
        by_cos = nt(cos_ref[here, :], img)
        by_sin = nt(sin_ref[here, :], img)
        out_ref[here, 0:128] = (by_cos[:, :128] + by_sin[:, 128:]).astype(BF16)
        out_ref[here, 128:256] = (by_cos[:, 128:] - by_sin[:, :128]).astype(BF16)


def consistency(recv_ref, kdata_ref, mask_ref, cos_hbm, sin_hbm, out_ref, x_ref, res_ref, cos_ref, sin_ref, sems):
    step = 256
    blocks = table_copies([(cos_hbm, cos_ref), (sin_hbm, sin_ref)], sems, step)
    lines = mask_ref.shape[0]
    npe = mask_ref.shape[1]
    sources = recv_ref.shape[0] // lines
    half = 4 * lines
    for quad in range(sources // 4):
        stacked = []
        for part in range(2):
            tiles = [
                recv_ref[pl.ds((4 * quad + s) * lines, lines), pl.ds(128 * part, 128)].astype(F32) for s in range(4)
            ]
            stacked += swap_groups(tiles, 32)
        x_ref[:, pl.ds(128 * quad, 128)] = jnp.concatenate(stacked, axis=0).astype(BF16)
    x = x_ref[...]
    for start in range(0, npe, step):
        here = pl.ds(start, step)
        arrived(blocks[start // step])
        by_cos = nn(x, cos_ref[:, here])
        by_sin = nn(x, sin_ref[:, here])
        sampled = mask_ref[:, here].astype(F32)
        sampled = jnp.concatenate([sampled] * 4, axis=0)
        data = [
            jnp.concatenate([kdata_ref[part, c, p, :, here] for c in range(2) for p in range(2)], axis=0)
            for part in range(2)
        ]
        real = sampled * (by_cos[:half] + by_sin[half:] - data[0])
        imag = sampled * (by_cos[half:] - by_sin[:half] - data[1])
        res_ref[0:half, here] = real.astype(BF16)
        res_ref[half : 2 * half, here] = imag.astype(BF16)
    res = res_ref[...]
    for start in range(0, cos_ref.shape[1], step):
        here = pl.ds(start, step)
        if start >= npe:
            arrived(blocks[start // step])
        by_cos = nn(res, cos_ref[:, here])
        by_sin = nn(res, sin_ref[:, here])
        parts = (by_cos[:half] - by_sin[half:], by_cos[half:] + by_sin[:half])
        for tile in range(step // 128):
            at = slice(128 * tile, 128 * tile + 128)
            tiles = [part[lines * g : lines * (g + 1), at] for part in parts for g in range(4)]
            if start < npe:
                quad = start // 128 + tile
                for part in range(2):
                    for s, value in enumerate(swap_groups(tiles[4 * part : 4 * part + 4], 32)):
                        out_ref[pl.ds((4 * quad + s) * lines, lines), pl.ds(128 * part, 128)] = value.astype(BF16)
            else:
                group = (start - npe) // 128 + tile
                for s, value in enumerate(swap_groups(tiles, 8)):
                    value = value.astype(BF16)
                    for half_id in range(2):
                        owner = 16 * group + 8 * half_id + s
                        out_ref[pl.ds(owner * lines, lines), 256:384] = value


def backward_columns(
    recv_ref, sens_ref, above_ref, below_ref, cos_hbm, sin_hbm, out_ref, part_ref, edge_ref, cos_ref, sin_ref, sems
):
    step = 256
    blocks = table_copies([(cos_hbm, cos_ref), (sin_hbm, sin_ref)], sems, step)
    npar = sens_ref.shape[4]
    coils, spots, rows = sens_ref.shape[1:4]
    cells = coils * spots * rows
    edges = coils * spots * 2 * REACH
    turned = recv_ref[...].astype(F32).T
    low = lax.axis_index("space") // 8 % 2 == 0
    for tile in range(npar // 128):
        here = pl.ds(tile * 2 * coils * spots * REACH, 2 * coils * spots * REACH)
        above, below = above_ref[here, :].astype(F32), below_ref[here, :].astype(F32)
        for k in range(2 * coils * spots):
            at = slice(k * REACH, (k + 1) * REACH)
            part, coil, spot = k // (coils * spots), k // spots % coils, k % spots
            edge_ref[part, coil, spot, :, pl.ds(128 * tile, 128)] = jnp.concatenate([below[at], above[at]], axis=0)
    border = jnp.where(low, turned[2 * cells : 2 * cells + 2 * edges], turned[2 * cells + 2 * edges :])
    x = jnp.concatenate([turned[: 2 * cells], border], axis=0).astype(BF16)
    for start in range(0, npar, step):
        here = pl.ds(start, step)
        arrived(blocks[start // step])
        by_cos = nn(x, cos_ref[:, here])
        by_sin = nn(x, sin_ref[:, here])
        for first, count, profile_ref, offset in ((0, cells, sens_ref, 0), (2 * cells, edges, edge_ref, rows)):
            second = first + count
            last = second + count
            real = by_cos[first:second] - by_sin[second:last]
            imag = by_cos[second:last] + by_sin[first:second]
            per_coil = count // coils
            height = per_coil // spots
            sums = [0.0, 0.0]
            for coil in range(coils):
                profile = [
                    jnp.concatenate([profile_ref[part, coil, spot, :, here] for spot in range(spots)], axis=0).astype(F32)
                    for part in range(2)
                ]
                re = real[coil * per_coil : (coil + 1) * per_coil]
                im = imag[coil * per_coil : (coil + 1) * per_coil]
                sums[0] = sums[0] + (profile[0] * re + profile[1] * im)
                sums[1] = sums[1] + (profile[0] * im - profile[1] * re)
            for part in range(2):
                for spot in range(spots):
                    row = (part * spots + spot) * (rows + 2 * REACH) + offset
                    part_ref[pl.ds(row, height), here] = sums[part][spot * height : (spot + 1) * height]
    total = part_ref.shape[0]
    owners = out_ref.shape[0] // total
    width = npar // owners
    lane = lax.broadcasted_iota(jnp.int32, (total, 128), 1)
    count = npar // 128
    for owner in range(owners):
        tile, off = divmod(width * owner, 128)
        value = part_ref[:, pl.ds(128 * tile, 128)]
        if off:
            value = pltpu.roll(value, 128 - off, 1)
            if tile + 1 < count:
                following = pltpu.roll(part_ref[:, pl.ds(128 * (tile + 1), 128)], 128 - off, 1)
                value = jnp.where((lane >= 128 - off) & (lane < 112), following, value)
        elif tile:
            value = jnp.where(lane >= 112, part_ref[:, pl.ds(128 * (tile - 1), 128)], value)
        out_ref[pl.ds(owner * total, total), :] = value.astype(BF16)


def pack_rows(state_ref, sens_ref, tail_ref, head_ref):
    channels, spots, rows, cols = state_ref.shape
    coils, npar = sens_ref.shape[1], sens_ref.shape[4]
    at = 0
    for tile in range(npar // 128):
        here = pl.ds(128 * tile, 128)
        for part in range(2):
            for coil in range(coils):
                for ref, low in ((tail_ref, rows - 8), (head_ref, 0)):
                    pair = [sens_ref[part, coil, spot, pl.ds(low, 8), here] for spot in range(2)]
                    ref[pl.ds(at, 8), :] = joined_edges(pair, low).astype(BF16)
                at += 8
    for channel in range(channels):
        for ref, low in ((tail_ref, rows - 8), (head_ref, 0)):
            pair = [state_ref[channel, spot, pl.ds(low, 8), :].astype(F32) for spot in range(2)]
            ref[pl.ds(at, 8), 0:cols] = joined_edges(pair, low).astype(BF16)
        at += 8


def joined_edges(pair, low):
    first, second = pair
    if low:
        return jnp.concatenate([first[REACH:], second[REACH:]], axis=0)
    return jnp.concatenate([first[:REACH], second[:REACH]], axis=0)


def tall_state(state_ref, above_ref, below_ref, channel, spot, skip):
    cols = state_ref.shape[3]
    at = skip + 8 * channel
    below = below_ref[pl.ds(at, 8), 0:cols].astype(F32)[spot * REACH : (spot + 1) * REACH]
    above = above_ref[pl.ds(at, 8), 0:cols].astype(F32)[spot * REACH : (spot + 1) * REACH]
    value = jnp.concatenate([state_ref[channel, spot].astype(F32), jnp.concatenate([below, above], axis=0)], axis=0)
    return jnp.concatenate([value, jnp.zeros((value.shape[0], 128 - cols), F32)], axis=1)


def pack_cols(state_ref, above_ref, below_ref, tail_ref, head_ref):
    channels, spots, rows, cols = state_ref.shape
    tall = rows + 2 * REACH
    skip = above_ref.shape[0] - channels * spots * REACH
    per = 128 // REACH
    lane = lax.broadcasted_iota(jnp.int32, (tall, 128), 1)
    for group in range(channels * spots // per):
        tail = head = jnp.zeros((tall, 128), F32)
        for k in range(per):
            channel, spot = divmod(group * per + k, spots)
            value = tall_state(state_ref, above_ref, below_ref, channel, spot, skip)
            here = lane // REACH == k
            tail = jnp.where(here, pltpu.roll(value, (REACH * k - cols + REACH) % 128, 1), tail)
            head = jnp.where(here, pltpu.roll(value, REACH * k, 1) if k else value, head)
        tail_ref[pl.ds(group * tall, tall), :] = tail.astype(BF16)
        head_ref[pl.ds(group * tall, tall), :] = head.astype(BF16)


def spread_state(state_ref, above_ref, below_ref, left_ref, right_ref, out_ref, wide_ref):
    channels, spots, rows, cols = state_ref.shape
    tall = rows + 2 * REACH
    half = channels // 2
    skip = above_ref.shape[0] - channels * spots * REACH
    per = 128 // REACH
    lane = lax.broadcasted_iota(jnp.int32, (tall, 128), 1)
    for channel in range(channels):
        for spot in range(spots):
            group, k = divmod(channel * spots + spot, per)
            value = tall_state(state_ref, above_ref, below_ref, channel, spot, skip)
            here = pl.ds(group * tall, tall)
            right = pltpu.roll(right_ref[here, :].astype(F32), (cols - REACH * k) % 128, 1)
            left = pltpu.roll(left_ref[here, :].astype(F32), (128 - REACH - REACH * k) % 128, 1)
            value = jnp.where((lane >= cols) & (lane < cols + REACH), right, value)
            value = jnp.where(lane >= 128 - REACH, left, value)
            at = ((channel // half * spots + spot) * half + channel % half) * tall
            wide_ref[pl.ds(at, tall), :] = value
    count = channels * spots
    for i in range(tall):
        out_ref[pl.ds(i * count, count), :] = wide_ref[pl.ds((i - REACH) % tall, count, stride=tall), :].astype(BF16)


def coupling_weights(kernels_ref, biases_ref, mixers_ref, inject_ref, weight_ref, mixer_ref, bias_ref, added_ref):
    layers = kernels_ref.shape[0]
    half = kernels_ref.shape[2]
    eye = lax.broadcasted_iota(jnp.int32, (half, half), 0) == lax.broadcasted_iota(jnp.int32, (half, half), 1)
    zero = jnp.zeros((half, half), F32)
    for layer in range(layers):
        for c in range(3):
            for out_spot in range(2):
                blocks = [
                    kernels_ref[layer, 9 * (in_spot - out_spot + 1) + 3 * b + c].astype(F32)
                    for b in range(3)
                    for in_spot in range(2)
                ]
                weight_ref[layer, pl.ds((2 * c + out_spot) * half, half), :] = jnp.concatenate(blocks, axis=1).astype(BF16)
        mixer = mixers_ref[layer].astype(F32)
        mixer_ref[layer, 0:half, :] = jnp.concatenate([mixer, zero], axis=1).astype(BF16)
        mixer_ref[layer, half : 2 * half, :] = jnp.concatenate([zero, mixer], axis=1).astype(BF16)
        row = jnp.broadcast_to(biases_ref[pl.ds(layer, 1), :], (half, half))
        column = jnp.sum(jnp.where(eye, row, 0.0), axis=1, keepdims=True)
        bias_ref[layer] = jnp.broadcast_to(jnp.concatenate([column, column], axis=0), (2 * half, 128))
    wide = lax.broadcasted_iota(jnp.int32, (2 * half, 2 * half), 0) == lax.broadcasted_iota(jnp.int32, (2 * half, 2 * half), 1)
    for part in range(2):
        row = jnp.broadcast_to(inject_ref[pl.ds(part, 1), :], (2 * half, 2 * half))
        column = jnp.broadcast_to(jnp.sum(jnp.where(wide, row, 0.0), axis=1, keepdims=True), (2 * half, 128))
        added_ref[part] = jnp.concatenate(
            [column[:half], column[:half], column[half:], column[half:]], axis=0
        )


def couple(recv_ref, state_ref, weight_ref, mixer_ref, bias_ref, inject_ref, new_ref, grad_ref, wide_ref, a_ref, b_ref):
    channels, spots, rows, cols = new_ref.shape
    tall = rows + 2 * REACH
    half = channels // 2
    block = spots * half
    total = 2 * spots * tall
    owners = recv_ref.shape[0] // total
    grad = recv_ref[0:total, :].astype(F32)
    for owner in range(1, owners):
        grad = grad + recv_ref[pl.ds(owner * total, total), :].astype(F32)
    for part in range(2):
        for spot in range(spots):
            row = (part * spots + spot) * tall
            grad_ref[part, spot] = grad[row : row + rows, :cols]
    space, coil = lax.axis_index("space"), lax.axis_index("coil")
    lane = lax.broadcasted_iota(jnp.int32, (1, 128), 1)
    col_id = coil * cols + jnp.where(lane < 112, lane, lane - 128)
    col_keep = ((col_id >= 0) & (col_id < cols * owners)).astype(F32)
    upper = jnp.where(space > 0, col_keep, 0.0)
    lower = jnp.where(space < lax.axis_size("space") - 1, col_keep, 0.0)

    def keep(i):
        return upper if i < REACH else lower if i >= REACH + rows else col_keep

    scale = [inject_ref[part] for part in range(2)]
    for i in range(tall):
        source = (i - REACH) % tall
        here = [
            jnp.concatenate(
                [
                    jnp.broadcast_to(grad[at : at + 1, :], (half, 128))
                    for at in ((part * spots + spot) * tall + source for spot in range(spots))
                ],
                axis=0,
            )
            for part in range(2)
        ]
        for which, ref in enumerate((a_ref, b_ref)):
            at = slice(which * block, (which + 1) * block)
            value = state_ref[pl.ds((2 * i + which) * block, block), :].astype(F32)
            value = value + (scale[0][at] * here[0] + scale[1][at] * here[1])
            ref[pl.ds(i * block, block), :] = (value * keep(i)).astype(BF16)
    for layer in range(weight_ref.shape[0]):
        source_ref, target_ref = (a_ref, b_ref) if layer % 2 == 0 else (b_ref, a_ref)
        weight = weight_ref[layer]
        mixer = mixer_ref[layer]
        bias = bias_ref[layer]
        first, last = 1 + layer, tall - 1 - layer
        for start in range(first, last, BATCH):
            lines = range(start, min(start + BATCH, last))
            cells = jnp.concatenate([source_ref[pl.ds((i - 1) * block, 3 * block), :] for i in lines], axis=1)
            taps = nn(weight, cells)
            raw = []
            for j in range(len(lines)):
                at = slice(128 * j, 128 * j + 128)
                value = pltpu.roll(taps[0:block, at], 1, 1) + taps[block : 2 * block, at]
                value = value + pltpu.roll(taps[2 * block :, at], 127, 1)
                raw.append(jnp.maximum(value + bias, 0.0).astype(BF16))
            mixed = nn(mixer, jnp.concatenate(raw, axis=1))
            for j, i in enumerate(lines):
                here = pl.ds(i * block, block)
                value = target_ref[here, :].astype(F32) + mixed[:, 128 * j : 128 * j + 128]
                target_ref[here, :] = (value * keep(i)).astype(BF16)
    for i in range(REACH, REACH + rows):
        source = i - REACH
        wide_ref[pl.ds(source, block, stride=rows), :] = a_ref[pl.ds(i * block, block), :].astype(F32)
        wide_ref[pl.ds(block * rows + source, block, stride=rows), :] = b_ref[pl.ds(i * block, block), :].astype(F32)
    for channel in range(channels):
        for spot in range(spots):
            at = (channel // half * block + spot * half + channel % half) * rows
            new_ref[channel, spot] = wide_ref[pl.ds(at, rows), :][:, :cols].astype(BF16)


def passed_on(tail, head, axis):
    ends = lax.axis_size(axis) - 1
    before = lax.ppermute(tail, axis, [(i, i + 1) for i in range(ends)])
    after = lax.ppermute(head, axis, [(i + 1, i) for i in range(ends)])
    return before, after


def per_device(state, sens, kdata, mask, inject, kernels, biases, mixers):
    channels, spots, rows, cols = state.shape
    coils = sens.shape[1]
    npar = sens.shape[4]
    npe = kdata.shape[4]
    lines = kdata.shape[3]
    groups = lax.axis_size("space")
    owners = lax.axis_size("coil")
    tall = rows + 2 * REACH
    cells = coils * spots * rows
    layers = kernels.shape[0]
    block = channels // 2 * spots

    estimate = jnp.pad(state[0:2], ((0, 0), (0, 0), (0, 0), (0, 128 - cols)))
    estimate = jnp.broadcast_to(estimate[None], (owners, *estimate.shape))
    estimate = lax.all_to_all(estimate, "coil", 0, 0, tiled=True)

    edge_columns = [
        (rows * d + r) % npe for d in range(groups) for r in (*range(rows, rows + REACH), *range(-REACH, 0))
    ]
    pe_columns = [*range(npe), *edge_columns]
    def tables(length, columns):
        out = pltpu.HBM((length, len(columns)), BF16)
        factors = jnp.asarray(dft_factors(length, columns, FINE))
        return [in_hbm(table) for table in call(dft_tables, [out, out], [], "dft_tables", plain(factors))]

    def table_scratch(length, columns, blocks):
        return [((length, columns), BF16)] * 2 + [pltpu.SemaphoreType.DMA((2 * blocks,))]

    par_tables = tables(npar, range(npar))
    pe_tables = tables(npe, pe_columns)

    (sent,) = call(
        forward_columns,
        [jax.ShapeDtypeStruct((npar, 2 * cells), BF16)],
        [((2 * cells, npar), BF16), *table_scratch(npar, npar, 1)],
        "forward_columns",
        estimate, sens, *par_tables,
    )
    spectra = lax.all_to_all(sent, "space", 0, 0, tiled=True)

    depth = 2 * coils * spots * REACH * (npar // 128) + channels * spots * REACH
    tail, head = call(pack_rows, [((depth, 128), BF16)] * 2, [], "pack_rows", state, plain(sens))
    above, below = passed_on(tail, head, "space")

    (sent,) = call(
        consistency,
        [jax.ShapeDtypeStruct((npar, 384), BF16)],
        [((8 * lines, npe), BF16)] * 2 + table_scratch(npe, len(pe_columns), len(pe_columns) // 256),
        "consistency",
        spectra, kdata, mask, *pe_tables,
    )
    sent, above, below = lax.optimization_barrier((sent, above, below))
    returned = lax.all_to_all(sent, "space", 0, 0, tiled=True)

    packed = [((channels * spots * REACH // 128 * tall, 128), BF16)] * 2
    tail, head = call(pack_cols, packed, [], "pack_cols", state, above, below)
    left, right = passed_on(tail, head, "coil")

    (sent,) = call(
        backward_columns,
        [jax.ShapeDtypeStruct((owners * 2 * spots * tall, 128), BF16)],
        [
            ((2 * spots * tall, npar), F32),
            ((2, coils, spots, 2 * REACH, npar), F32),
            *table_scratch(npar, npar, npar // 256),
        ],
        "backward_columns",
        returned, sens, above, below, *par_tables,
    )
    sent, left, right = lax.optimization_barrier((sent, left, right))
    shares = lax.all_to_all(sent, "coil", 0, 0, tiled=True)

    (spread,) = call(
        spread_state,
        [((tall * channels * spots, 128), BF16)],
        [((channels * spots * tall, 128), F32)],
        "spread_state",
        state, above, below, left, right,
    )

    weight, mixer, bias, added = call(
        coupling_weights,
        [
            ((layers, 3 * block, 3 * block), BF16),
            ((layers, block, block), BF16),
            ((layers, block, 128), F32),
            ((2, 2 * block, 128), F32),
        ],
        [],
        "coupling_weights",
        plain(kernels), plain(biases), plain(mixers), plain(inject.T),
    )
    new_state, gradient = call(
        couple,
        [jax.ShapeDtypeStruct(state.shape, BF16), jax.ShapeDtypeStruct((2, spots, rows, cols), F32)],
        [((2 * block * rows, 128), F32), ((block * tall, 128), BF16), ((block * tall, 128), BF16)],
        "couple",
        shares, spread, weight, mixer, bias, added,
    )
    return (new_state, gradient)


def solution(mesh):
    return jax.shard_map(
        per_device,
        mesh=mesh,
        in_specs=(
            P(None, None, "space", "coil"),
            P(None, "coil", None, "space", None),
            P(None, "coil", None, "space", None),
            P("space", None),
            P(),
            P(),
            P(),
            P(),
        ),
        out_specs=(P(None, None, "space", "coil"), P(None, None, "space", "coil")),
        check_vma=False,
    )
```

```python
import numpy as np

import jax
import jax.numpy as jnp
from jax import lax
from jax.experimental import pallas as pl
from jax.experimental.pallas import tpu as pltpu
from jax.sharding import PartitionSpec as P

F32 = jnp.float32
BF16 = jnp.bfloat16
REACH = 4
FINE = 32
BATCH = 12
VMEM = pl.BlockSpec(memory_space=pltpu.VMEM)
HBM = pl.BlockSpec(memory_space=pltpu.HBM)


def call(body, outs, scratch, name, *args):
    specs, values = [], []
    for arg in args:
        where, value = arg if isinstance(arg, tuple) else ("vmem", arg)
        if where != "plain":
            value = pltpu.with_memory_space_constraint(value, pltpu.HBM if where == "hbm" else pltpu.VMEM)
        specs.append(HBM if where == "hbm" else VMEM)
        values.append(value)
    shapes = [pltpu.VMEM(*out) if isinstance(out, tuple) else out for out in outs]
    placed = [VMEM if isinstance(out, (tuple, jax.ShapeDtypeStruct)) else HBM for out in outs]
    return pl.pallas_call(
        body,
        out_shape=shapes,
        in_specs=specs,
        out_specs=placed,
        scratch_shapes=[each if not isinstance(each, tuple) else pltpu.VMEM(*each) for each in scratch],
        compiler_params=pltpu.CompilerParams(vmem_limit_bytes=20 * 2**20),
        name=name,
    )(*values)


def in_hbm(value):
    return ("hbm", value)


def plain(value):
    return ("plain", value)


def table_copies(pairs, sems, step):
    blocks = []
    for start in range(0, pairs[0][0].shape[1], step):
        here = pl.ds(start, step)
        block = []
        for source, target in pairs:
            copy = pltpu.make_async_copy(source.at[:, here], target.at[:, here], sems.at[len(blocks) * len(pairs) + len(block)])
            copy.start()
            block.append(copy)
        blocks.append(block)
    return blocks


def arrived(block):
    for copy in block:
        copy.wait()


def dft_factors(length, columns, step):
    columns = np.asarray(columns)[None, :]
    coarse = (step * np.arange(length // step))[:, None] * columns % length
    fine = np.arange(step)[:, None] * columns % length
    angle_coarse = coarse * (2.0 * np.pi / length)
    angle_fine = fine * (2.0 * np.pi / length)
    scale = 1.0 / np.sqrt(length)
    parts = (np.cos(angle_coarse) * scale, np.sin(angle_coarse) * scale, np.cos(angle_fine), np.sin(angle_fine))
    return np.concatenate(parts).astype(np.float32)


def dft_tables(factors_ref, cos_hbm, sin_hbm, cos_ref, sin_ref, sems):
    count = cos_ref.shape[0] // FINE
    cos_b = factors_ref[pl.ds(2 * count, FINE), :]
    sin_b = factors_ref[pl.ds(2 * count + FINE, FINE), :]
    copies = []
    for a in range(count):
        here = pl.ds(a * FINE, FINE)
        cos, sin = factors_ref[pl.ds(a, 1), :], factors_ref[pl.ds(count + a, 1), :]
        cos_ref[here, :] = (cos * cos_b - sin * sin_b).astype(BF16)
        sin_ref[here, :] = (sin * cos_b + cos * sin_b).astype(BF16)
        if a % 4 == 3:
            done = pl.ds((a - 3) * FINE, 4 * FINE)
            for source, target in ((cos_ref, cos_hbm), (sin_ref, sin_hbm)):
                copy = pltpu.make_async_copy(source.at[done, :], target.at[done, :], sems.at[len(copies)])
                copy.start()
                copies.append(copy)
    arrived(copies)


def swap_groups(tiles, group):
    tiles = list(tiles)
    count = len(tiles)
    lane = lax.broadcasted_iota(jnp.int32, tiles[0].shape, 1)
    bit = count // 2
    while bit:
        shift = bit * group
        high = (lane // shift) % 2 == 1
        for low in range(count):
            if low & bit:
                continue
            a, b = tiles[low], tiles[low | bit]
            tiles[low] = jnp.where(high, pltpu.roll(b, shift, 1), a)
            tiles[low | bit] = jnp.where(high, b, pltpu.roll(a, 128 - shift, 1))
        bit //= 2
    return tiles


def nn(a, b):
    return lax.dot_general(a, b, (((1,), (0,)), ((), ())), preferred_element_type=F32)


def nt(a, b):
    return lax.dot_general(a, b, (((1,), (1,)), ((), ())), preferred_element_type=F32)


def forward_columns(est_ref, sens_ref, cos_hbm, sin_hbm, out_ref, img_ref, cos_ref, sin_ref, sems):
    blocks = table_copies([(cos_hbm, cos_ref), (sin_hbm, sin_ref)], sems, cos_ref.shape[1])
    owners = est_ref.shape[0]
    rows = sens_ref.shape[3]
    npar = sens_ref.shape[4]
    width = npar // owners
    lane = lax.broadcasted_iota(jnp.int32, (rows, 128), 1)
    coils, spots = sens_ref.shape[1:3]
    for spot in range(spots):
        for tile in range(npar // 128):
            full = []
            for part in range(2):
                value = None
                for owner in range(128 * tile // width, (128 * tile + 127) // width + 1):
                    at = width * owner - 128 * tile
                    piece = est_ref[owner, part, spot].astype(F32)
                    if at % 128:
                        piece = pltpu.roll(piece, at % 128, 1)
                    value = piece if value is None else jnp.where(lane >= at, piece, value)
                full.append(value)
            est_re, est_im = full
            cols = pl.ds(128 * tile, 128)
            for coil in range(coils):
                sens_re = sens_ref[0, coil, spot, :, cols]
                sens_im = sens_ref[1, coil, spot, :, cols]
                row = (coil * spots + spot) * rows
                img_ref[pl.ds(row, rows), cols] = (sens_re * est_re - sens_im * est_im).astype(BF16)
                img_ref[pl.ds(128 + row, rows), cols] = (sens_re * est_im + sens_im * est_re).astype(BF16)
    img = img_ref[...]
    arrived(blocks[0])
    step = 256
    for start in range(0, npar, step):
        here = pl.ds(start, step)
        by_cos = nt(cos_ref[here, :], img)
        by_sin = nt(sin_ref[here, :], img)
        out_ref[here, 0:128] = (by_cos[:, :128] + by_sin[:, 128:]).astype(BF16)
        out_ref[here, 128:256] = (by_cos[:, 128:] - by_sin[:, :128]).astype(BF16)


def consistency(recv_ref, kdata_ref, mask_ref, cos_hbm, sin_hbm, out_ref, x_ref, res_ref, cos_ref, sin_ref, sems):
    step = 256
    blocks = table_copies([(cos_hbm, cos_ref), (sin_hbm, sin_ref)], sems, step)
    lines = mask_ref.shape[0]
    npe = mask_ref.shape[1]
    sources = recv_ref.shape[0] // lines
    half = 4 * lines
    for quad in range(sources // 4):
        stacked = []
        for part in range(2):
            tiles = [
                recv_ref[pl.ds((4 * quad + s) * lines, lines), pl.ds(128 * part, 128)].astype(F32) for s in range(4)
            ]
            stacked += swap_groups(tiles, 32)
        x_ref[:, pl.ds(128 * quad, 128)] = jnp.concatenate(stacked, axis=0).astype(BF16)
    x = x_ref[...]
    for start in range(0, npe, step):
        here = pl.ds(start, step)
        arrived(blocks[start // step])
        by_cos = nn(x, cos_ref[:, here])
        by_sin = nn(x, sin_ref[:, here])
        sampled = mask_ref[:, here].astype(F32)
        sampled = jnp.concatenate([sampled] * 4, axis=0)
        data = [
            jnp.concatenate([kdata_ref[part, c, p, :, here] for c in range(2) for p in range(2)], axis=0)
            for part in range(2)
        ]
        real = sampled * (by_cos[:half] + by_sin[half:] - data[0])
        imag = sampled * (by_cos[half:] - by_sin[:half] - data[1])
        res_ref[0:half, here] = real.astype(BF16)
        res_ref[half : 2 * half, here] = imag.astype(BF16)
    res = res_ref[...]
    for start in range(0, cos_ref.shape[1], step):
        here = pl.ds(start, step)
        if start >= npe:
            arrived(blocks[start // step])
        by_cos = nn(res, cos_ref[:, here])
        by_sin = nn(res, sin_ref[:, here])
        parts = (by_cos[:half] - by_sin[half:], by_cos[half:] + by_sin[:half])
        for tile in range(step // 128):
            at = slice(128 * tile, 128 * tile + 128)
            tiles = [part[lines * g : lines * (g + 1), at] for part in parts for g in range(4)]
            if start < npe:
                quad = start // 128 + tile
                for part in range(2):
                    for s, value in enumerate(swap_groups(tiles[4 * part : 4 * part + 4], 32)):
                        out_ref[pl.ds((4 * quad + s) * lines, lines), pl.ds(128 * part, 128)] = value.astype(BF16)
            else:
                group = (start - npe) // 128 + tile
                for s, value in enumerate(swap_groups(tiles, 8)):
                    value = value.astype(BF16)
                    for half_id in range(2):
                        owner = 16 * group + 8 * half_id + s
                        out_ref[pl.ds(owner * lines, lines), 256:384] = value


def backward_columns(
    recv_ref, sens_ref, above_ref, below_ref, cos_hbm, sin_hbm, out_ref, part_ref, edge_ref, cos_ref, sin_ref, sems
):
    step = 256
    blocks = table_copies([(cos_hbm, cos_ref), (sin_hbm, sin_ref)], sems, step)
    npar = sens_ref.shape[4]
    coils, spots, rows = sens_ref.shape[1:4]
    cells = coils * spots * rows
    edges = coils * spots * 2 * REACH
    turned = recv_ref[...].astype(F32).T
    low = lax.axis_index("space") // 8 % 2 == 0
    for tile in range(npar // 128):
        here = pl.ds(tile * 2 * coils * spots * REACH, 2 * coils * spots * REACH)
        above, below = above_ref[here, :].astype(F32), below_ref[here, :].astype(F32)
        for k in range(2 * coils * spots):
            at = slice(k * REACH, (k + 1) * REACH)
            part, coil, spot = k // (coils * spots), k // spots % coils, k % spots
            edge_ref[part, coil, spot, :, pl.ds(128 * tile, 128)] = jnp.concatenate([below[at], above[at]], axis=0)
    border = jnp.where(low, turned[2 * cells : 2 * cells + 2 * edges], turned[2 * cells + 2 * edges :])
    x = jnp.concatenate([turned[: 2 * cells], border], axis=0).astype(BF16)
    for start in range(0, npar, step):
        here = pl.ds(start, step)
        arrived(blocks[start // step])
        by_cos = nn(x, cos_ref[:, here])
        by_sin = nn(x, sin_ref[:, here])
        for first, count, profile_ref, offset in ((0, cells, sens_ref, 0), (2 * cells, edges, edge_ref, rows)):
            second = first + count
            last = second + count
            real = by_cos[first:second] - by_sin[second:last]
            imag = by_cos[second:last] + by_sin[first:second]
            per_coil = count // coils
            height = per_coil // spots
            sums = [0.0, 0.0]
            for coil in range(coils):
                profile = [
                    jnp.concatenate([profile_ref[part, coil, spot, :, here] for spot in range(spots)], axis=0).astype(F32)
                    for part in range(2)
                ]
                re = real[coil * per_coil : (coil + 1) * per_coil]
                im = imag[coil * per_coil : (coil + 1) * per_coil]
                sums[0] = sums[0] + (profile[0] * re + profile[1] * im)
                sums[1] = sums[1] + (profile[0] * im - profile[1] * re)
            for part in range(2):
                for spot in range(spots):
                    row = (part * spots + spot) * (rows + 2 * REACH) + offset
                    part_ref[pl.ds(row, height), here] = sums[part][spot * height : (spot + 1) * height]
    total = part_ref.shape[0]
    owners = out_ref.shape[0] // total
    width = npar // owners
    lane = lax.broadcasted_iota(jnp.int32, (total, 128), 1)
    count = npar // 128
    for owner in range(owners):
        tile, off = divmod(width * owner, 128)
        value = part_ref[:, pl.ds(128 * tile, 128)]
        if off:
            value = pltpu.roll(value, 128 - off, 1)
            if tile + 1 < count:
                following = pltpu.roll(part_ref[:, pl.ds(128 * (tile + 1), 128)], 128 - off, 1)
                value = jnp.where((lane >= 128 - off) & (lane < 112), following, value)
        elif tile:
            value = jnp.where(lane >= 112, part_ref[:, pl.ds(128 * (tile - 1), 128)], value)
        out_ref[pl.ds(owner * total, total), :] = value.astype(BF16)


def pack_rows(*refs):
    count = (len(refs) - 3) // 2
    tail_ref, head_ref, sems = refs[count], refs[count + 1], refs[-1]
    copies = []
    for k in range(count):
        copy = pltpu.make_async_copy(refs[k], refs[count + 2 + k], sems.at[k])
        copy.start()
        copies.append(copy)
    arrived(copies)
    state_ref, sens_ref = refs[count + 2], refs[count + 3]
    channels, spots, rows, cols = state_ref.shape
    coils, npar = sens_ref.shape[1], sens_ref.shape[4]
    at = 0
    for tile in range(npar // 128):
        here = pl.ds(128 * tile, 128)
        for part in range(2):
            for coil in range(coils):
                for ref, low in ((tail_ref, rows - 8), (head_ref, 0)):
                    pair = [sens_ref[part, coil, spot, pl.ds(low, 8), here] for spot in range(2)]
                    ref[pl.ds(at, 8), :] = joined_edges(pair, low).astype(BF16)
                at += 8
    for channel in range(channels):
        for ref, low in ((tail_ref, rows - 8), (head_ref, 0)):
            pair = [state_ref[channel, spot, pl.ds(low, 8), :].astype(F32) for spot in range(2)]
            ref[pl.ds(at, 8), 0:cols] = joined_edges(pair, low).astype(BF16)
        at += 8


def joined_edges(pair, low):
    first, second = pair
    if low:
        return jnp.concatenate([first[REACH:], second[REACH:]], axis=0)
    return jnp.concatenate([first[:REACH], second[:REACH]], axis=0)


def tall_state(state_ref, above_ref, below_ref, channel, spot, skip):
    cols = state_ref.shape[3]
    at = skip + 8 * channel
    below = below_ref[pl.ds(at, 8), 0:cols].astype(F32)[spot * REACH : (spot + 1) * REACH]
    above = above_ref[pl.ds(at, 8), 0:cols].astype(F32)[spot * REACH : (spot + 1) * REACH]
    value = jnp.concatenate([state_ref[channel, spot].astype(F32), jnp.concatenate([below, above], axis=0)], axis=0)
    return jnp.concatenate([value, jnp.zeros((value.shape[0], 128 - cols), F32)], axis=1)


def pack_cols(state_ref, above_ref, below_ref, tail_ref, head_ref):
    channels, spots, rows, cols = state_ref.shape
    tall = rows + 2 * REACH
    skip = above_ref.shape[0] - channels * spots * REACH
    per = 128 // REACH
    lane = lax.broadcasted_iota(jnp.int32, (tall, 128), 1)
    for group in range(channels * spots // per):
        tail = head = jnp.zeros((tall, 128), F32)
        for k in range(per):
            channel, spot = divmod(group * per + k, spots)
            value = tall_state(state_ref, above_ref, below_ref, channel, spot, skip)
            here = lane // REACH == k
            tail = jnp.where(here, pltpu.roll(value, (REACH * k - cols + REACH) % 128, 1), tail)
            head = jnp.where(here, pltpu.roll(value, REACH * k, 1) if k else value, head)
        tail_ref[pl.ds(group * tall, tall), :] = tail.astype(BF16)
        head_ref[pl.ds(group * tall, tall), :] = head.astype(BF16)


def spread_state(state_ref, above_ref, below_ref, left_ref, right_ref, out_ref, wide_ref):
    channels, spots, rows, cols = state_ref.shape
    tall = rows + 2 * REACH
    half = channels // 2
    skip = above_ref.shape[0] - channels * spots * REACH
    per = 128 // REACH
    lane = lax.broadcasted_iota(jnp.int32, (tall, 128), 1)
    for channel in range(channels):
        for spot in range(spots):
            group, k = divmod(channel * spots + spot, per)
            value = tall_state(state_ref, above_ref, below_ref, channel, spot, skip)
            here = pl.ds(group * tall, tall)
            right = pltpu.roll(right_ref[here, :].astype(F32), (cols - REACH * k) % 128, 1)
            left = pltpu.roll(left_ref[here, :].astype(F32), (128 - REACH - REACH * k) % 128, 1)
            value = jnp.where((lane >= cols) & (lane < cols + REACH), right, value)
            value = jnp.where(lane >= 128 - REACH, left, value)
            at = ((channel // half * spots + spot) * half + channel % half) * tall
            wide_ref[pl.ds(at, tall), :] = value
    count = channels * spots
    for i in range(tall):
        out_ref[pl.ds(i * count, count), :] = wide_ref[pl.ds((i - REACH) % tall, count, stride=tall), :].astype(BF16)


def coupling_weights(kernels_ref, biases_ref, mixers_ref, inject_ref, weight_ref, mixer_ref, bias_ref, added_ref):
    layers = kernels_ref.shape[0]
    half = kernels_ref.shape[2]
    eye = lax.broadcasted_iota(jnp.int32, (half, half), 0) == lax.broadcasted_iota(jnp.int32, (half, half), 1)
    zero = jnp.zeros((half, half), F32)
    for layer in range(layers):
        for c in range(3):
            for out_spot in range(2):
                blocks = [
                    kernels_ref[layer, 9 * (in_spot - out_spot + 1) + 3 * b + c].astype(F32)
                    for b in range(3)
                    for in_spot in range(2)
                ]
                weight_ref[layer, pl.ds((2 * c + out_spot) * half, half), :] = jnp.concatenate(blocks, axis=1).astype(BF16)
        mixer = mixers_ref[layer].astype(F32)
        mixer_ref[layer, 0:half, :] = jnp.concatenate([mixer, zero], axis=1).astype(BF16)
        mixer_ref[layer, half : 2 * half, :] = jnp.concatenate([zero, mixer], axis=1).astype(BF16)
        row = jnp.broadcast_to(biases_ref[pl.ds(layer, 1), :], (half, half))
        column = jnp.sum(jnp.where(eye, row, 0.0), axis=1, keepdims=True)
        bias_ref[layer] = jnp.broadcast_to(jnp.concatenate([column, column], axis=0), (2 * half, 128))
    wide = lax.broadcasted_iota(jnp.int32, (2 * half, 2 * half), 0) == lax.broadcasted_iota(jnp.int32, (2 * half, 2 * half), 1)
    for part in range(2):
        row = jnp.broadcast_to(inject_ref[pl.ds(part, 1), :], (2 * half, 2 * half))
        column = jnp.broadcast_to(jnp.sum(jnp.where(wide, row, 0.0), axis=1, keepdims=True), (2 * half, 128))
        added_ref[part] = jnp.concatenate(
            [column[:half], column[:half], column[half:], column[half:]], axis=0
        )


def couple(recv_ref, state_ref, weight_ref, mixer_ref, bias_ref, inject_ref, new_ref, grad_ref, wide_ref, a_ref, b_ref):
    channels, spots, rows, cols = new_ref.shape
    tall = rows + 2 * REACH
    half = channels // 2
    block = spots * half
    total = 2 * spots * tall
    owners = recv_ref.shape[0] // total
    grad = recv_ref[0:total, :].astype(F32)
    for owner in range(1, owners):
        grad = grad + recv_ref[pl.ds(owner * total, total), :].astype(F32)
    for part in range(2):
        for spot in range(spots):
            row = (part * spots + spot) * tall
            grad_ref[part, spot] = grad[row : row + rows, :cols]
    space, coil = lax.axis_index("space"), lax.axis_index("coil")
    lane = lax.broadcasted_iota(jnp.int32, (1, 128), 1)
    col_id = coil * cols + jnp.where(lane < 112, lane, lane - 128)
    col_keep = ((col_id >= 0) & (col_id < cols * owners)).astype(F32)
    upper = jnp.where(space > 0, col_keep, 0.0)
    lower = jnp.where(space < lax.axis_size("space") - 1, col_keep, 0.0)

    def keep(i):
        return upper if i < REACH else lower if i >= REACH + rows else col_keep

    scale = [inject_ref[part] for part in range(2)]
    for i in range(tall):
        source = (i - REACH) % tall
        here = [
            jnp.concatenate(
                [
                    jnp.broadcast_to(grad[at : at + 1, :], (half, 128))
                    for at in ((part * spots + spot) * tall + source for spot in range(spots))
                ],
                axis=0,
            )
            for part in range(2)
        ]
        for which, ref in enumerate((a_ref, b_ref)):
            at = slice(which * block, (which + 1) * block)
            value = state_ref[pl.ds((2 * i + which) * block, block), :].astype(F32)
            value = value + (scale[0][at] * here[0] + scale[1][at] * here[1])
            ref[pl.ds(i * block, block), :] = (value * keep(i)).astype(BF16)
    for layer in range(weight_ref.shape[0]):
        source_ref, target_ref = (a_ref, b_ref) if layer % 2 == 0 else (b_ref, a_ref)
        weight = weight_ref[layer]
        mixer = mixer_ref[layer]
        bias = bias_ref[layer]
        first, last = 1 + layer, tall - 1 - layer
        for start in range(first, last, BATCH):
            lines = range(start, min(start + BATCH, last))
            cells = jnp.concatenate([source_ref[pl.ds((i - 1) * block, 3 * block), :] for i in lines], axis=1)
            taps = nn(weight, cells)
            raw = []
            for j in range(len(lines)):
                at = slice(128 * j, 128 * j + 128)
                value = pltpu.roll(taps[0:block, at], 1, 1) + taps[block : 2 * block, at]
                value = value + pltpu.roll(taps[2 * block :, at], 127, 1)
                raw.append(jnp.maximum(value + bias, 0.0).astype(BF16))
            mixed = nn(mixer, jnp.concatenate(raw, axis=1))
            for j, i in enumerate(lines):
                here = pl.ds(i * block, block)
                value = target_ref[here, :].astype(F32) + mixed[:, 128 * j : 128 * j + 128]
                target_ref[here, :] = (value * keep(i)).astype(BF16)
    for i in range(REACH, REACH + rows):
        source = i - REACH
        wide_ref[pl.ds(source, block, stride=rows), :] = a_ref[pl.ds(i * block, block), :].astype(F32)
        wide_ref[pl.ds(block * rows + source, block, stride=rows), :] = b_ref[pl.ds(i * block, block), :].astype(F32)
    for channel in range(channels):
        for spot in range(spots):
            at = (channel // half * block + spot * half + channel % half) * rows
            new_ref[channel, spot] = wide_ref[pl.ds(at, rows), :][:, :cols].astype(BF16)


def passed_on(tail, head, axis):
    ends = lax.axis_size(axis) - 1
    before = lax.ppermute(tail, axis, [(i, i + 1) for i in range(ends)])
    after = lax.ppermute(head, axis, [(i + 1, i) for i in range(ends)])
    return before, after


def per_device(state, sens, kdata, mask, inject, kernels, biases, mixers):
    channels, spots, rows, cols = state.shape
    coils = sens.shape[1]
    npar = sens.shape[4]
    npe = kdata.shape[4]
    lines = kdata.shape[3]
    groups = lax.axis_size("space")
    owners = lax.axis_size("coil")
    tall = rows + 2 * REACH
    cells = coils * spots * rows
    layers = kernels.shape[0]
    block = channels // 2 * spots

    estimate = jnp.pad(state[0:2], ((0, 0), (0, 0), (0, 0), (0, 128 - cols)))
    estimate = jnp.broadcast_to(estimate[None], (owners, *estimate.shape))
    estimate = lax.all_to_all(estimate, "coil", 0, 0, tiled=True)

    edge_columns = [
        (rows * d + r) % npe for d in range(groups) for r in (*range(rows, rows + REACH), *range(-REACH, 0))
    ]
    pe_columns = [*range(npe), *edge_columns]
    def table_scratch(length, columns, blocks):
        return [((length, columns), BF16)] * 2 + [pltpu.SemaphoreType.DMA((2 * blocks,))]

    def tables(length, columns):
        out = pltpu.HBM((length, len(columns)), BF16)
        factors = jnp.asarray(dft_factors(length, columns, FINE))
        scratch = table_scratch(length, len(columns), length // FINE // 4)
        return [in_hbm(table) for table in call(dft_tables, [out, out], scratch, "dft_tables", plain(factors))]

    depth = 2 * coils * spots * REACH * (npar // 128) + channels * spots * REACH
    brought = [state, sens, jnp.asarray(dft_factors(npar, range(npar), FINE)), jnp.asarray(dft_factors(npe, pe_columns, FINE))]
    tail, head, state, sens, par_factors, pe_factors = call(
        pack_rows,
        [((depth, 128), BF16)] * 2 + [(each.shape, each.dtype) for each in brought],
        [pltpu.SemaphoreType.DMA((len(brought),))],
        "pack_rows",
        *[in_hbm(each) for each in brought],
    )
    above, below = passed_on(tail, head, "space")

    par_tables = tables(npar, range(npar))
    pe_tables = tables(npe, pe_columns)

    (sent,) = call(
        forward_columns,
        [jax.ShapeDtypeStruct((npar, 2 * cells), BF16)],
        [((2 * cells, npar), BF16), *table_scratch(npar, npar, 1)],
        "forward_columns",
        estimate, sens, *par_tables,
    )
    sent, above, below = lax.optimization_barrier((sent, above, below))
    spectra = lax.all_to_all(sent, "space", 0, 0, tiled=True)

    (sent,) = call(
        consistency,
        [jax.ShapeDtypeStruct((npar, 384), BF16)],
        [((8 * lines, npe), BF16)] * 2 + table_scratch(npe, len(pe_columns), len(pe_columns) // 256),
        "consistency",
        spectra, kdata, mask, *pe_tables,
    )
    returned = lax.all_to_all(sent, "space", 0, 0, tiled=True)

    packed = [((channels * spots * REACH // 128 * tall, 128), BF16)] * 2
    tail, head = call(pack_cols, packed, [], "pack_cols", state, above, below)
    left, right = passed_on(tail, head, "coil")

    (sent,) = call(
        backward_columns,
        [jax.ShapeDtypeStruct((owners * 2 * spots * tall, 128), BF16)],
        [
            ((2 * spots * tall, npar), F32),
            ((2, coils, spots, 2 * REACH, npar), F32),
            *table_scratch(npar, npar, npar // 256),
        ],
        "backward_columns",
        returned, sens, above, below, *par_tables,
    )
    sent, left, right = lax.optimization_barrier((sent, left, right))
    shares = lax.all_to_all(sent, "coil", 0, 0, tiled=True)

    (spread,) = call(
        spread_state,
        [((tall * channels * spots, 128), BF16)],
        [((channels * spots * tall, 128), F32)],
        "spread_state",
        state, above, below, left, right,
    )

    weight, mixer, bias, added = call(
        coupling_weights,
        [
            ((layers, 3 * block, 3 * block), BF16),
            ((layers, block, block), BF16),
            ((layers, block, 128), F32),
            ((2, 2 * block, 128), F32),
        ],
        [],
        "coupling_weights",
        plain(kernels), plain(biases), plain(mixers), plain(inject.T),
    )
    new_state, gradient = call(
        couple,
        [jax.ShapeDtypeStruct(state.shape, BF16), jax.ShapeDtypeStruct((2, spots, rows, cols), F32)],
        [((2 * block * rows, 128), F32), ((block * tall, 128), BF16), ((block * tall, 128), BF16)],
        "couple",
        shares, spread, weight, mixer, bias, added,
    )
    return (new_state, gradient)


def solution(mesh):
    return jax.shard_map(
        per_device,
        mesh=mesh,
        in_specs=(
            P(None, None, "space", "coil"),
            P(None, "coil", None, "space", None),
            P(None, "coil", None, "space", None),
            P("space", None),
            P(),
            P(),
            P(),
            P(),
        ),
        out_specs=(P(None, None, "space", "coil"), P(None, None, "space", "coil")),
        check_vma=False,
    )
```

```python
import numpy as np

import jax
import jax.numpy as jnp
from jax import lax
from jax.experimental import pallas as pl
from jax.experimental.pallas import tpu as pltpu
from jax.sharding import PartitionSpec as P

F32 = jnp.float32
BF16 = jnp.bfloat16
REACH = 4
FINE = 32
BATCH = 12
VMEM = pl.BlockSpec(memory_space=pltpu.VMEM)
HBM = pl.BlockSpec(memory_space=pltpu.HBM)


def call(body, outs, scratch, name, *args):
    specs, values = [], []
    for arg in args:
        where, value = arg if isinstance(arg, tuple) else ("vmem", arg)
        if where != "plain":
            value = pltpu.with_memory_space_constraint(value, pltpu.HBM if where == "hbm" else pltpu.VMEM)
        specs.append(HBM if where == "hbm" else VMEM)
        values.append(value)
    shapes = [pltpu.VMEM(*out) if isinstance(out, tuple) else out for out in outs]
    placed = [VMEM if isinstance(out, (tuple, jax.ShapeDtypeStruct)) else HBM for out in outs]
    return pl.pallas_call(
        body,
        out_shape=shapes,
        in_specs=specs,
        out_specs=placed,
        scratch_shapes=[each if not isinstance(each, tuple) else pltpu.VMEM(*each) for each in scratch],
        compiler_params=pltpu.CompilerParams(vmem_limit_bytes=20 * 2**20),
        name=name,
    )(*values)


def in_hbm(value):
    return ("hbm", value)


def plain(value):
    return ("plain", value)


def table_copies(pairs, sems, step):
    blocks = []
    for start in range(0, pairs[0][0].shape[1], step):
        here = pl.ds(start, step)
        block = []
        for source, target in pairs:
            copy = pltpu.make_async_copy(source.at[:, here], target.at[:, here], sems.at[len(blocks) * len(pairs) + len(block)])
            copy.start()
            block.append(copy)
        blocks.append(block)
    return blocks


def arrived(block):
    for copy in block:
        copy.wait()


def dft_factors(length, columns, step):
    columns = np.asarray(columns)[None, :]
    coarse = (step * np.arange(length // step))[:, None] * columns % length
    fine = np.arange(step)[:, None] * columns % length
    angle_coarse = coarse * (2.0 * np.pi / length)
    angle_fine = fine * (2.0 * np.pi / length)
    scale = 1.0 / np.sqrt(length)
    parts = (np.cos(angle_coarse) * scale, np.sin(angle_coarse) * scale, np.cos(angle_fine), np.sin(angle_fine))
    return np.concatenate(parts).astype(np.float32)


def fill_tables(factors_ref, cos_hbm, sin_hbm, cos_ref, sin_ref, sems):
    count = cos_ref.shape[0] // FINE
    cos_b = factors_ref[pl.ds(2 * count, FINE), :]
    sin_b = factors_ref[pl.ds(2 * count + FINE, FINE), :]
    copies = []
    for a in range(count):
        here = pl.ds(a * FINE, FINE)
        cos, sin = factors_ref[pl.ds(a, 1), :], factors_ref[pl.ds(count + a, 1), :]
        cos_ref[here, :] = (cos * cos_b - sin * sin_b).astype(BF16)
        sin_ref[here, :] = (sin * cos_b + cos * sin_b).astype(BF16)
        if a % 4 == 3:
            done = pl.ds((a - 3) * FINE, 4 * FINE)
            for source, target in ((cos_ref, cos_hbm), (sin_ref, sin_hbm)):
                copy = pltpu.make_async_copy(source.at[done, :], target.at[done, :], sems.at[len(copies)])
                copy.start()
                copies.append(copy)
    return copies


def prepare(
    state_hbm, sens_hbm, par_hbm, pe_hbm,
    tail_ref, head_ref, state_ref, sens_ref, par_cos_hbm, par_sin_hbm, pe_cos_hbm, pe_sin_hbm,
    par_ref, pe_ref, par_cos, par_sin, pe_cos, pe_sin, sems, par_sems, pe_sems,
):
    pairs = ((par_hbm, par_ref), (pe_hbm, pe_ref), (state_hbm, state_ref), (sens_hbm, sens_ref))
    copies = []
    for k, (source, target) in enumerate(pairs):
        copy = pltpu.make_async_copy(source, target, sems.at[k])
        copy.start()
        copies.append(copy)
    arrived(copies[0:1])
    sent = fill_tables(par_ref, par_cos_hbm, par_sin_hbm, par_cos, par_sin, par_sems)
    arrived(copies[1:2])
    sent = sent + fill_tables(pe_ref, pe_cos_hbm, pe_sin_hbm, pe_cos, pe_sin, pe_sems)
    arrived(copies[2:])
    pack_rows(state_ref, sens_ref, tail_ref, head_ref)
    arrived(sent)


def swap_groups(tiles, group):
    tiles = list(tiles)
    count = len(tiles)
    lane = lax.broadcasted_iota(jnp.int32, tiles[0].shape, 1)
    bit = count // 2
    while bit:
        shift = bit * group
        high = (lane // shift) % 2 == 1
        for low in range(count):
            if low & bit:
                continue
            a, b = tiles[low], tiles[low | bit]
            tiles[low] = jnp.where(high, pltpu.roll(b, shift, 1), a)
            tiles[low | bit] = jnp.where(high, b, pltpu.roll(a, 128 - shift, 1))
        bit //= 2
    return tiles


def nn(a, b):
    return lax.dot_general(a, b, (((1,), (0,)), ((), ())), preferred_element_type=F32)


def nt(a, b):
    return lax.dot_general(a, b, (((1,), (1,)), ((), ())), preferred_element_type=F32)


def forward_columns(est_ref, sens_ref, cos_hbm, sin_hbm, out_ref, img_ref, cos_ref, sin_ref, sems):
    blocks = table_copies([(cos_hbm, cos_ref), (sin_hbm, sin_ref)], sems, cos_ref.shape[1])
    owners = est_ref.shape[0]
    rows = sens_ref.shape[3]
    npar = sens_ref.shape[4]
    width = npar // owners
    lane = lax.broadcasted_iota(jnp.int32, (rows, 128), 1)
    coils, spots = sens_ref.shape[1:3]
    for spot in range(spots):
        for tile in range(npar // 128):
            full = []
            for part in range(2):
                value = None
                for owner in range(128 * tile // width, (128 * tile + 127) // width + 1):
                    at = width * owner - 128 * tile
                    piece = est_ref[owner, part, spot].astype(F32)
                    if at % 128:
                        piece = pltpu.roll(piece, at % 128, 1)
                    value = piece if value is None else jnp.where(lane >= at, piece, value)
                full.append(value)
            est_re, est_im = full
            cols = pl.ds(128 * tile, 128)
            for coil in range(coils):
                sens_re = sens_ref[0, coil, spot, :, cols]
                sens_im = sens_ref[1, coil, spot, :, cols]
                row = (coil * spots + spot) * rows
                img_ref[pl.ds(row, rows), cols] = (sens_re * est_re - sens_im * est_im).astype(BF16)
                img_ref[pl.ds(128 + row, rows), cols] = (sens_re * est_im + sens_im * est_re).astype(BF16)
    img = img_ref[...]
    arrived(blocks[0])
    step = 256
    for start in range(0, npar, step):
        here = pl.ds(start, step)
        by_cos = nt(cos_ref[here, :], img)
        by_sin = nt(sin_ref[here, :], img)
        out_ref[here, 0:128] = (by_cos[:, :128] + by_sin[:, 128:]).astype(BF16)
        out_ref[here, 128:256] = (by_cos[:, 128:] - by_sin[:, :128]).astype(BF16)


def consistency(recv_ref, kdata_ref, mask_ref, cos_hbm, sin_hbm, out_ref, x_ref, res_ref, cos_ref, sin_ref, sems):
    step = 256
    blocks = table_copies([(cos_hbm, cos_ref), (sin_hbm, sin_ref)], sems, step)
    lines = mask_ref.shape[0]
    npe = mask_ref.shape[1]
    sources = recv_ref.shape[0] // lines
    half = 4 * lines
    for quad in range(sources // 4):
        stacked = []
        for part in range(2):
            tiles = [
                recv_ref[pl.ds((4 * quad + s) * lines, lines), pl.ds(128 * part, 128)].astype(F32) for s in range(4)
            ]
            stacked += swap_groups(tiles, 32)
        x_ref[:, pl.ds(128 * quad, 128)] = jnp.concatenate(stacked, axis=0).astype(BF16)
    x = x_ref[...]
    for start in range(0, npe, step):
        here = pl.ds(start, step)
        arrived(blocks[start // step])
        by_cos = nn(x, cos_ref[:, here])
        by_sin = nn(x, sin_ref[:, here])
        sampled = mask_ref[:, here].astype(F32)
        sampled = jnp.concatenate([sampled] * 4, axis=0)
        data = [
            jnp.concatenate([kdata_ref[part, c, p, :, here] for c in range(2) for p in range(2)], axis=0)
            for part in range(2)
        ]
        real = sampled * (by_cos[:half] + by_sin[half:] - data[0])
        imag = sampled * (by_cos[half:] - by_sin[:half] - data[1])
        res_ref[0:half, here] = real.astype(BF16)
        res_ref[half : 2 * half, here] = imag.astype(BF16)
    res = res_ref[...]
    for start in range(0, cos_ref.shape[1], step):
        here = pl.ds(start, step)
        if start >= npe:
            arrived(blocks[start // step])
        by_cos = nn(res, cos_ref[:, here])
        by_sin = nn(res, sin_ref[:, here])
        parts = (by_cos[:half] - by_sin[half:], by_cos[half:] + by_sin[:half])
        for tile in range(step // 128):
            at = slice(128 * tile, 128 * tile + 128)
            tiles = [part[lines * g : lines * (g + 1), at] for part in parts for g in range(4)]
            if start < npe:
                quad = start // 128 + tile
                for part in range(2):
                    for s, value in enumerate(swap_groups(tiles[4 * part : 4 * part + 4], 32)):
                        out_ref[pl.ds((4 * quad + s) * lines, lines), pl.ds(128 * part, 128)] = value.astype(BF16)
            else:
                group = (start - npe) // 128 + tile
                for s, value in enumerate(swap_groups(tiles, 8)):
                    value = value.astype(BF16)
                    for half_id in range(2):
                        owner = 16 * group + 8 * half_id + s
                        out_ref[pl.ds(owner * lines, lines), 256:384] = value


def backward_columns(
    recv_ref, sens_ref, above_ref, below_ref, cos_hbm, sin_hbm, out_ref, part_ref, edge_ref, cos_ref, sin_ref, sems
):
    step = 256
    blocks = table_copies([(cos_hbm, cos_ref), (sin_hbm, sin_ref)], sems, step)
    npar = sens_ref.shape[4]
    coils, spots, rows = sens_ref.shape[1:4]
    cells = coils * spots * rows
    edges = coils * spots * 2 * REACH
    turned = recv_ref[...].astype(F32).T
    low = lax.axis_index("space") // 8 % 2 == 0
    for tile in range(npar // 128):
        here = pl.ds(tile * 2 * coils * spots * REACH, 2 * coils * spots * REACH)
        above, below = above_ref[here, :].astype(F32), below_ref[here, :].astype(F32)
        for k in range(2 * coils * spots):
            at = slice(k * REACH, (k + 1) * REACH)
            part, coil, spot = k // (coils * spots), k // spots % coils, k % spots
            edge_ref[part, coil, spot, :, pl.ds(128 * tile, 128)] = jnp.concatenate([below[at], above[at]], axis=0)
    border = jnp.where(low, turned[2 * cells : 2 * cells + 2 * edges], turned[2 * cells + 2 * edges :])
    x = jnp.concatenate([turned[: 2 * cells], border], axis=0).astype(BF16)
    for start in range(0, npar, step):
        here = pl.ds(start, step)
        arrived(blocks[start // step])
        by_cos = nn(x, cos_ref[:, here])
        by_sin = nn(x, sin_ref[:, here])
        for first, count, profile_ref, offset in ((0, cells, sens_ref, 0), (2 * cells, edges, edge_ref, rows)):
            second = first + count
            last = second + count
            real = by_cos[first:second] - by_sin[second:last]
            imag = by_cos[second:last] + by_sin[first:second]
            per_coil = count // coils
            height = per_coil // spots
            sums = [0.0, 0.0]
            for coil in range(coils):
                profile = [
                    jnp.concatenate([profile_ref[part, coil, spot, :, here] for spot in range(spots)], axis=0).astype(F32)
                    for part in range(2)
                ]
                re = real[coil * per_coil : (coil + 1) * per_coil]
                im = imag[coil * per_coil : (coil + 1) * per_coil]
                sums[0] = sums[0] + (profile[0] * re + profile[1] * im)
                sums[1] = sums[1] + (profile[0] * im - profile[1] * re)
            for part in range(2):
                for spot in range(spots):
                    row = (part * spots + spot) * (rows + 2 * REACH) + offset
                    part_ref[pl.ds(row, height), here] = sums[part][spot * height : (spot + 1) * height]
    total = part_ref.shape[0]
    owners = out_ref.shape[0] // total
    width = npar // owners
    lane = lax.broadcasted_iota(jnp.int32, (total, 128), 1)
    count = npar // 128
    for owner in range(owners):
        tile, off = divmod(width * owner, 128)
        value = part_ref[:, pl.ds(128 * tile, 128)]
        if off:
            value = pltpu.roll(value, 128 - off, 1)
            if tile + 1 < count:
                following = pltpu.roll(part_ref[:, pl.ds(128 * (tile + 1), 128)], 128 - off, 1)
                value = jnp.where((lane >= 128 - off) & (lane < 112), following, value)
        elif tile:
            value = jnp.where(lane >= 112, part_ref[:, pl.ds(128 * (tile - 1), 128)], value)
        out_ref[pl.ds(owner * total, total), :] = value.astype(BF16)


def pack_rows(state_ref, sens_ref, tail_ref, head_ref):
    channels, spots, rows, cols = state_ref.shape
    coils, npar = sens_ref.shape[1], sens_ref.shape[4]
    at = 0
    for tile in range(npar // 128):
        here = pl.ds(128 * tile, 128)
        for part in range(2):
            for coil in range(coils):
                for ref, low in ((tail_ref, rows - 8), (head_ref, 0)):
                    pair = [sens_ref[part, coil, spot, pl.ds(low, 8), here] for spot in range(2)]
                    ref[pl.ds(at, 8), :] = joined_edges(pair, low).astype(BF16)
                at += 8
    for channel in range(channels):
        for ref, low in ((tail_ref, rows - 8), (head_ref, 0)):
            pair = [state_ref[channel, spot, pl.ds(low, 8), :].astype(F32) for spot in range(2)]
            ref[pl.ds(at, 8), 0:cols] = joined_edges(pair, low).astype(BF16)
        at += 8


def joined_edges(pair, low):
    first, second = pair
    if low:
        return jnp.concatenate([first[REACH:], second[REACH:]], axis=0)
    return jnp.concatenate([first[:REACH], second[:REACH]], axis=0)


def tall_state(state_ref, above_ref, below_ref, channel, spot, skip):
    cols = state_ref.shape[3]
    at = skip + 8 * channel
    below = below_ref[pl.ds(at, 8), 0:cols].astype(F32)[spot * REACH : (spot + 1) * REACH]
    above = above_ref[pl.ds(at, 8), 0:cols].astype(F32)[spot * REACH : (spot + 1) * REACH]
    value = jnp.concatenate([state_ref[channel, spot].astype(F32), jnp.concatenate([below, above], axis=0)], axis=0)
    return jnp.concatenate([value, jnp.zeros((value.shape[0], 128 - cols), F32)], axis=1)


def pack_cols(state_ref, above_ref, below_ref, tail_ref, head_ref):
    channels, spots, rows, cols = state_ref.shape
    tall = rows + 2 * REACH
    skip = above_ref.shape[0] - channels * spots * REACH
    per = 128 // REACH
    lane = lax.broadcasted_iota(jnp.int32, (tall, 128), 1)
    for group in range(channels * spots // per):
        tail = head = jnp.zeros((tall, 128), F32)
        for k in range(per):
            channel, spot = divmod(group * per + k, spots)
            value = tall_state(state_ref, above_ref, below_ref, channel, spot, skip)
            here = lane // REACH == k
            tail = jnp.where(here, pltpu.roll(value, (REACH * k - cols + REACH) % 128, 1), tail)
            head = jnp.where(here, pltpu.roll(value, REACH * k, 1) if k else value, head)
        tail_ref[pl.ds(group * tall, tall), :] = tail.astype(BF16)
        head_ref[pl.ds(group * tall, tall), :] = head.astype(BF16)


def spread_state(state_ref, above_ref, below_ref, left_ref, right_ref, out_ref, wide_ref):
    channels, spots, rows, cols = state_ref.shape
    tall = rows + 2 * REACH
    half = channels // 2
    skip = above_ref.shape[0] - channels * spots * REACH
    per = 128 // REACH
    lane = lax.broadcasted_iota(jnp.int32, (tall, 128), 1)
    for channel in range(channels):
        for spot in range(spots):
            group, k = divmod(channel * spots + spot, per)
            value = tall_state(state_ref, above_ref, below_ref, channel, spot, skip)
            here = pl.ds(group * tall, tall)
            right = pltpu.roll(right_ref[here, :].astype(F32), (cols - REACH * k) % 128, 1)
            left = pltpu.roll(left_ref[here, :].astype(F32), (128 - REACH - REACH * k) % 128, 1)
            value = jnp.where((lane >= cols) & (lane < cols + REACH), right, value)
            value = jnp.where(lane >= 128 - REACH, left, value)
            at = ((channel // half * spots + spot) * half + channel % half) * tall
            wide_ref[pl.ds(at, tall), :] = value
    count = channels * spots
    for i in range(tall):
        out_ref[pl.ds(i * count, count), :] = wide_ref[pl.ds((i - REACH) % tall, count, stride=tall), :].astype(BF16)


def coupling_weights(kernels_ref, biases_ref, mixers_ref, inject_ref, weight_ref, mixer_ref, bias_ref, added_ref):
    layers = kernels_ref.shape[0]
    half = kernels_ref.shape[2]
    eye = lax.broadcasted_iota(jnp.int32, (half, half), 0) == lax.broadcasted_iota(jnp.int32, (half, half), 1)
    zero = jnp.zeros((half, half), F32)
    for layer in range(layers):
        for c in range(3):
            for out_spot in range(2):
                blocks = [
                    kernels_ref[layer, 9 * (in_spot - out_spot + 1) + 3 * b + c].astype(F32)
                    for b in range(3)
                    for in_spot in range(2)
                ]
                weight_ref[layer, pl.ds((2 * c + out_spot) * half, half), :] = jnp.concatenate(blocks, axis=1).astype(BF16)
        mixer = mixers_ref[layer].astype(F32)
        mixer_ref[layer, 0:half, :] = jnp.concatenate([mixer, zero], axis=1).astype(BF16)
        mixer_ref[layer, half : 2 * half, :] = jnp.concatenate([zero, mixer], axis=1).astype(BF16)
        row = jnp.broadcast_to(biases_ref[pl.ds(layer, 1), :], (half, half))
        column = jnp.sum(jnp.where(eye, row, 0.0), axis=1, keepdims=True)
        bias_ref[layer] = jnp.broadcast_to(jnp.concatenate([column, column], axis=0), (2 * half, 128))
    wide = lax.broadcasted_iota(jnp.int32, (2 * half, 2 * half), 0) == lax.broadcasted_iota(jnp.int32, (2 * half, 2 * half), 1)
    for part in range(2):
        row = jnp.broadcast_to(inject_ref[pl.ds(part, 1), :], (2 * half, 2 * half))
        column = jnp.broadcast_to(jnp.sum(jnp.where(wide, row, 0.0), axis=1, keepdims=True), (2 * half, 128))
        added_ref[part] = jnp.concatenate(
            [column[:half], column[:half], column[half:], column[half:]], axis=0
        )


def couple(recv_ref, state_ref, weight_ref, mixer_ref, bias_ref, inject_ref, new_ref, grad_ref, wide_ref, a_ref, b_ref):
    channels, spots, rows, cols = new_ref.shape
    tall = rows + 2 * REACH
    half = channels // 2
    block = spots * half
    total = 2 * spots * tall
    owners = recv_ref.shape[0] // total
    grad = recv_ref[0:total, :].astype(F32)
    for owner in range(1, owners):
        grad = grad + recv_ref[pl.ds(owner * total, total), :].astype(F32)
    for part in range(2):
        for spot in range(spots):
            row = (part * spots + spot) * tall
            grad_ref[part, spot] = grad[row : row + rows, :cols]
    space, coil = lax.axis_index("space"), lax.axis_index("coil")
    lane = lax.broadcasted_iota(jnp.int32, (1, 128), 1)
    col_id = coil * cols + jnp.where(lane < 112, lane, lane - 128)
    col_keep = ((col_id >= 0) & (col_id < cols * owners)).astype(F32)
    upper = jnp.where(space > 0, col_keep, 0.0)
    lower = jnp.where(space < lax.axis_size("space") - 1, col_keep, 0.0)

    def keep(i):
        return upper if i < REACH else lower if i >= REACH + rows else col_keep

    scale = [inject_ref[part] for part in range(2)]
    for i in range(tall):
        source = (i - REACH) % tall
        here = [
            jnp.concatenate(
                [
                    jnp.broadcast_to(grad[at : at + 1, :], (half, 128))
                    for at in ((part * spots + spot) * tall + source for spot in range(spots))
                ],
                axis=0,
            )
            for part in range(2)
        ]
        for which, ref in enumerate((a_ref, b_ref)):
            at = slice(which * block, (which + 1) * block)
            value = state_ref[pl.ds((2 * i + which) * block, block), :].astype(F32)
            value = value + (scale[0][at] * here[0] + scale[1][at] * here[1])
            ref[pl.ds(i * block, block), :] = (value * keep(i)).astype(BF16)
    for layer in range(weight_ref.shape[0]):
        source_ref, target_ref = (a_ref, b_ref) if layer % 2 == 0 else (b_ref, a_ref)
        weight = weight_ref[layer]
        mixer = mixer_ref[layer]
        bias = bias_ref[layer]
        first, last = 1 + layer, tall - 1 - layer
        for start in range(first, last, BATCH):
            lines = range(start, min(start + BATCH, last))
            cells = jnp.concatenate([source_ref[pl.ds((i - 1) * block, 3 * block), :] for i in lines], axis=1)
            taps = nn(weight, cells)
            raw = []
            for j in range(len(lines)):
                at = slice(128 * j, 128 * j + 128)
                value = pltpu.roll(taps[0:block, at], 1, 1) + taps[block : 2 * block, at]
                value = value + pltpu.roll(taps[2 * block :, at], 127, 1)
                raw.append(jnp.maximum(value + bias, 0.0).astype(BF16))
            mixed = nn(mixer, jnp.concatenate(raw, axis=1))
            for j, i in enumerate(lines):
                here = pl.ds(i * block, block)
                value = target_ref[here, :].astype(F32) + mixed[:, 128 * j : 128 * j + 128]
                target_ref[here, :] = (value * keep(i)).astype(BF16)
    for i in range(REACH, REACH + rows):
        source = i - REACH
        wide_ref[pl.ds(source, block, stride=rows), :] = a_ref[pl.ds(i * block, block), :].astype(F32)
        wide_ref[pl.ds(block * rows + source, block, stride=rows), :] = b_ref[pl.ds(i * block, block), :].astype(F32)
    for channel in range(channels):
        for spot in range(spots):
            at = (channel // half * block + spot * half + channel % half) * rows
            new_ref[channel, spot] = wide_ref[pl.ds(at, rows), :][:, :cols].astype(BF16)


def from_previous(tail, axis):
    return lax.ppermute(tail, axis, [(i, i + 1) for i in range(lax.axis_size(axis) - 1)])


def from_next(head, axis):
    return lax.ppermute(head, axis, [(i + 1, i) for i in range(lax.axis_size(axis) - 1)])


def per_device(state, sens, kdata, mask, inject, kernels, biases, mixers):
    channels, spots, rows, cols = state.shape
    coils = sens.shape[1]
    npar = sens.shape[4]
    npe = kdata.shape[4]
    lines = kdata.shape[3]
    groups = lax.axis_size("space")
    owners = lax.axis_size("coil")
    tall = rows + 2 * REACH
    cells = coils * spots * rows
    layers = kernels.shape[0]
    block = channels // 2 * spots

    estimate = jnp.pad(state[0:2], ((0, 0), (0, 0), (0, 0), (0, 128 - cols)))
    estimate = jnp.broadcast_to(estimate[None], (owners, *estimate.shape))
    estimate = lax.all_to_all(estimate, "coil", 0, 0, tiled=True)

    edge_columns = [
        (rows * d + r) % npe for d in range(groups) for r in (*range(rows, rows + REACH), *range(-REACH, 0))
    ]
    pe_columns = [*range(npe), *edge_columns]
    def table_scratch(length, columns, blocks):
        return [((length, columns), BF16)] * 2 + [pltpu.SemaphoreType.DMA((2 * blocks,))]

    def tables(length, columns):
        out = pltpu.HBM((length, len(columns)), BF16)
        factors = jnp.asarray(dft_factors(length, columns, FINE))
        scratch = table_scratch(length, len(columns), length // FINE // 4)
        return [in_hbm(table) for table in call(dft_tables, [out, out], scratch, "dft_tables", plain(factors))]

    depth = 2 * coils * spots * REACH * (npar // 128) + channels * spots * REACH
    par_factors = jnp.asarray(dft_factors(npar, range(npar), FINE))
    pe_factors = jnp.asarray(dft_factors(npe, pe_columns, FINE))

    def table_scratch(length, columns, blocks):
        return [((length, columns), BF16)] * 2 + [pltpu.SemaphoreType.DMA((2 * blocks,))]

    par_scratch = table_scratch(npar, npar, npar // FINE // 4)
    pe_scratch = table_scratch(npe, len(pe_columns), npe // FINE // 4)
    tail, head, state, sens, *tables = call(
        prepare,
        [((depth, 128), BF16)] * 2
        + [(state.shape, BF16), (sens.shape, F32)]
        + [pltpu.HBM((npar, npar), BF16)] * 2
        + [pltpu.HBM((npe, len(pe_columns)), BF16)] * 2,
        [
            (par_factors.shape, F32),
            (pe_factors.shape, F32),
            *par_scratch[:2],
            *pe_scratch[:2],
            pltpu.SemaphoreType.DMA((4,)),
            par_scratch[2],
            pe_scratch[2],
        ],
        "prepare",
        in_hbm(state), in_hbm(sens), in_hbm(par_factors), in_hbm(pe_factors),
    )
    par_tables = [in_hbm(table) for table in tables[:2]]
    pe_tables = [in_hbm(table) for table in tables[2:]]

    (sent,) = call(
        forward_columns,
        [jax.ShapeDtypeStruct((npar, 2 * cells), BF16)],
        [((2 * cells, npar), BF16), *table_scratch(npar, npar, 1)],
        "forward_columns",
        estimate, sens, *par_tables,
    )
    sent, tail = lax.optimization_barrier((sent, tail))
    spectra = lax.all_to_all(sent, "space", 0, 0, tiled=True)
    above = from_previous(tail, "space")

    (sent,) = call(
        consistency,
        [jax.ShapeDtypeStruct((npar, 384), BF16)],
        [((8 * lines, npe), BF16)] * 2 + table_scratch(npe, len(pe_columns), len(pe_columns) // 256),
        "consistency",
        spectra, kdata, mask, *pe_tables,
    )
    sent, above, head = lax.optimization_barrier((sent, above, head))
    returned = lax.all_to_all(sent, "space", 0, 0, tiled=True)
    below = from_next(head, "space")

    (sent,) = call(
        backward_columns,
        [jax.ShapeDtypeStruct((owners * 2 * spots * tall, 128), BF16)],
        [
            ((2 * spots * tall, npar), F32),
            ((2, coils, spots, 2 * REACH, npar), F32),
            *table_scratch(npar, npar, npar // 256),
        ],
        "backward_columns",
        returned, sens, above, below, *par_tables,
    )
    sent, above, below = lax.optimization_barrier((sent, above, below))
    shares = lax.all_to_all(sent, "coil", 0, 0, tiled=True)

    packed = [((channels * spots * REACH // 128 * tall, 128), BF16)] * 2
    tail, head = call(pack_cols, packed, [], "pack_cols", state, above, below)
    left, right = from_previous(tail, "coil"), from_next(head, "coil")

    (spread,) = call(
        spread_state,
        [((tall * channels * spots, 128), BF16)],
        [((channels * spots * tall, 128), F32)],
        "spread_state",
        state, above, below, left, right,
    )

    weight, mixer, bias, added = call(
        coupling_weights,
        [
            ((layers, 3 * block, 3 * block), BF16),
            ((layers, block, block), BF16),
            ((layers, block, 128), F32),
            ((2, 2 * block, 128), F32),
        ],
        [],
        "coupling_weights",
        plain(kernels), plain(biases), plain(mixers), plain(inject.T),
    )
    new_state, gradient = call(
        couple,
        [jax.ShapeDtypeStruct(state.shape, BF16), jax.ShapeDtypeStruct((2, spots, rows, cols), F32)],
        [((2 * block * rows, 128), F32), ((block * tall, 128), BF16), ((block * tall, 128), BF16)],
        "couple",
        shares, spread, weight, mixer, bias, added,
    )
    return (new_state, gradient)


def solution(mesh):
    return jax.shard_map(
        per_device,
        mesh=mesh,
        in_specs=(
            P(None, None, "space", "coil"),
            P(None, "coil", None, "space", None),
            P(None, "coil", None, "space", None),
            P("space", None),
            P(),
            P(),
            P(),
            P(),
        ),
        out_specs=(P(None, None, "space", "coil"), P(None, None, "space", "coil")),
        check_vma=False,
    )
```

```python
import numpy as np

import jax
import jax.numpy as jnp
from jax import lax
from jax.experimental import pallas as pl
from jax.experimental.pallas import tpu as pltpu
from jax.sharding import PartitionSpec as P

F32 = jnp.float32
BF16 = jnp.bfloat16
REACH = 4
FINE = 32
BATCH = 38
VMEM = pl.BlockSpec(memory_space=pltpu.VMEM)
HBM = pl.BlockSpec(memory_space=pltpu.HBM)


def call(body, outs, scratch, name, *args):
    specs, values = [], []
    for arg in args:
        where, value = arg if isinstance(arg, tuple) else ("vmem", arg)
        if where != "plain":
            value = pltpu.with_memory_space_constraint(value, pltpu.HBM if where == "hbm" else pltpu.VMEM)
        specs.append(HBM if where == "hbm" else VMEM)
        values.append(value)
    shapes = [pltpu.VMEM(*out) if isinstance(out, tuple) else out for out in outs]
    placed = [VMEM if isinstance(out, (tuple, jax.ShapeDtypeStruct)) else HBM for out in outs]
    return pl.pallas_call(
        body,
        out_shape=shapes,
        in_specs=specs,
        out_specs=placed,
        scratch_shapes=[each if not isinstance(each, tuple) else pltpu.VMEM(*each) for each in scratch],
        compiler_params=pltpu.CompilerParams(vmem_limit_bytes=20 * 2**20),
        name=name,
    )(*values)


def in_hbm(value):
    return ("hbm", value)


def plain(value):
    return ("plain", value)


def table_copies(pairs, sems, step):
    blocks = []
    for start in range(0, pairs[0][0].shape[1], step):
        here = pl.ds(start, step)
        block = []
        for source, target in pairs:
            copy = pltpu.make_async_copy(source.at[:, here], target.at[:, here], sems.at[len(blocks) * len(pairs) + len(block)])
            copy.start()
            block.append(copy)
        blocks.append(block)
    return blocks


def arrived(block):
    for copy in block:
        copy.wait()


def dft_factors(length, columns, step):
    columns = np.asarray(columns)[None, :]
    coarse = (step * np.arange(length // step))[:, None] * columns % length
    fine = np.arange(step)[:, None] * columns % length
    angle_coarse = coarse * (2.0 * np.pi / length)
    angle_fine = fine * (2.0 * np.pi / length)
    scale = 1.0 / np.sqrt(length)
    parts = (np.cos(angle_coarse) * scale, np.sin(angle_coarse) * scale, np.cos(angle_fine), np.sin(angle_fine))
    return np.concatenate(parts).astype(np.float32)


def fill_tables(factors_ref, cos_hbm, sin_hbm, cos_ref, sin_ref, sems):
    count = cos_ref.shape[0] // FINE
    cos_b = factors_ref[pl.ds(2 * count, FINE), :]
    sin_b = factors_ref[pl.ds(2 * count + FINE, FINE), :]
    copies = []
    for a in range(count):
        here = pl.ds(a * FINE, FINE)
        cos, sin = factors_ref[pl.ds(a, 1), :], factors_ref[pl.ds(count + a, 1), :]
        cos_ref[here, :] = (cos * cos_b - sin * sin_b).astype(BF16)
        sin_ref[here, :] = (sin * cos_b + cos * sin_b).astype(BF16)
        if a % 4 == 3:
            done = pl.ds((a - 3) * FINE, 4 * FINE)
            for source, target in ((cos_ref, cos_hbm), (sin_ref, sin_hbm)):
                copy = pltpu.make_async_copy(source.at[done, :], target.at[done, :], sems.at[len(copies)])
                copy.start()
                copies.append(copy)
    return copies


def prepare(
    state_hbm, sens_hbm, par_hbm, pe_hbm,
    first_ref, second_ref, state_ref, sens_ref, par_cos_hbm, par_sin_hbm, pe_cos_hbm, pe_sin_hbm,
    par_ref, pe_ref, par_cos, par_sin, pe_cos, pe_sin, sems, par_sems, pe_sems,
):
    pairs = ((par_hbm, par_ref), (pe_hbm, pe_ref), (state_hbm, state_ref), (sens_hbm, sens_ref))
    copies = []
    for k, (source, target) in enumerate(pairs):
        copy = pltpu.make_async_copy(source, target, sems.at[k])
        copy.start()
        copies.append(copy)
    arrived(copies[0:1])
    sent = fill_tables(par_ref, par_cos_hbm, par_sin_hbm, par_cos, par_sin, par_sems)
    arrived(copies[1:2])
    sent = sent + fill_tables(pe_ref, pe_cos_hbm, pe_sin_hbm, pe_cos, pe_sin, pe_sems)
    arrived(copies[2:])
    pack_rows(state_ref, sens_ref, first_ref, second_ref)
    arrived(sent)


def swap_groups(tiles, group):
    tiles = list(tiles)
    count = len(tiles)
    lane = lax.broadcasted_iota(jnp.int32, tiles[0].shape, 1)
    bit = count // 2
    while bit:
        shift = bit * group
        high = (lane // shift) % 2 == 1
        for low in range(count):
            if low & bit:
                continue
            a, b = tiles[low], tiles[low | bit]
            tiles[low] = jnp.where(high, pltpu.roll(b, shift, 1), a)
            tiles[low | bit] = jnp.where(high, b, pltpu.roll(a, 128 - shift, 1))
        bit //= 2
    return tiles


def nn(a, b):
    return lax.dot_general(a, b, (((1,), (0,)), ((), ())), preferred_element_type=F32)


def nt(a, b):
    return lax.dot_general(a, b, (((1,), (1,)), ((), ())), preferred_element_type=F32)


def forward_columns(est_ref, sens_ref, cos_hbm, sin_hbm, out_ref, img_ref, cos_ref, sin_ref, sems):
    blocks = table_copies([(cos_hbm, cos_ref), (sin_hbm, sin_ref)], sems, cos_ref.shape[1])
    owners = est_ref.shape[0]
    rows = sens_ref.shape[3]
    npar = sens_ref.shape[4]
    width = npar // owners
    lane = lax.broadcasted_iota(jnp.int32, (rows, 128), 1)
    coils, spots = sens_ref.shape[1:3]
    for spot in range(spots):
        for tile in range(npar // 128):
            full = []
            for part in range(2):
                value = None
                for owner in range(128 * tile // width, (128 * tile + 127) // width + 1):
                    at = width * owner - 128 * tile
                    piece = est_ref[owner, part, spot].astype(F32)
                    if at % 128:
                        piece = pltpu.roll(piece, at % 128, 1)
                    value = piece if value is None else jnp.where(lane >= at, piece, value)
                full.append(value)
            est_re, est_im = full
            cols = pl.ds(128 * tile, 128)
            for coil in range(coils):
                sens_re = sens_ref[0, coil, spot, :, cols]
                sens_im = sens_ref[1, coil, spot, :, cols]
                row = (coil * spots + spot) * rows
                img_ref[pl.ds(row, rows), cols] = (sens_re * est_re - sens_im * est_im).astype(BF16)
                img_ref[pl.ds(128 + row, rows), cols] = (sens_re * est_im + sens_im * est_re).astype(BF16)
    img = img_ref[...]
    arrived(blocks[0])
    step = 256
    for start in range(0, npar, step):
        here = pl.ds(start, step)
        by_cos = nt(cos_ref[here, :], img)
        by_sin = nt(sin_ref[here, :], img)
        out_ref[here, 0:128] = (by_cos[:, :128] + by_sin[:, 128:]).astype(BF16)
        out_ref[here, 128:256] = (by_cos[:, 128:] - by_sin[:, :128]).astype(BF16)


def consistency(recv_ref, kdata_ref, mask_ref, cos_hbm, sin_hbm, out_ref, x_ref, res_ref, cos_ref, sin_ref, sems):
    step = 256
    blocks = table_copies([(cos_hbm, cos_ref), (sin_hbm, sin_ref)], sems, step)
    lines = mask_ref.shape[0]
    npe = mask_ref.shape[1]
    sources = recv_ref.shape[0] // lines
    half = 4 * lines
    for quad in range(sources // 4):
        stacked = []
        for part in range(2):
            tiles = [
                recv_ref[pl.ds((4 * quad + s) * lines, lines), pl.ds(128 * part, 128)].astype(F32) for s in range(4)
            ]
            stacked += swap_groups(tiles, 32)
        x_ref[:, pl.ds(128 * quad, 128)] = jnp.concatenate(stacked, axis=0).astype(BF16)
    x = x_ref[...]
    for start in range(0, npe, step):
        here = pl.ds(start, step)
        arrived(blocks[start // step])
        by_cos = nn(x, cos_ref[:, here])
        by_sin = nn(x, sin_ref[:, here])
        sampled = mask_ref[:, here].astype(F32)
        sampled = jnp.concatenate([sampled] * 4, axis=0)
        data = [
            jnp.concatenate([kdata_ref[part, c, p, :, here] for c in range(2) for p in range(2)], axis=0)
            for part in range(2)
        ]
        real = sampled * (by_cos[:half] + by_sin[half:] - data[0])
        imag = sampled * (by_cos[half:] - by_sin[:half] - data[1])
        res_ref[0:half, here] = real.astype(BF16)
        res_ref[half : 2 * half, here] = imag.astype(BF16)
    res = res_ref[...]
    for start in range(0, cos_ref.shape[1], step):
        here = pl.ds(start, step)
        if start >= npe:
            arrived(blocks[start // step])
        by_cos = nn(res, cos_ref[:, here])
        by_sin = nn(res, sin_ref[:, here])
        parts = (by_cos[:half] - by_sin[half:], by_cos[half:] + by_sin[:half])
        for tile in range(step // 128):
            at = slice(128 * tile, 128 * tile + 128)
            tiles = [part[lines * g : lines * (g + 1), at] for part in parts for g in range(4)]
            if start < npe:
                quad = start // 128 + tile
                for part in range(2):
                    for s, value in enumerate(swap_groups(tiles[4 * part : 4 * part + 4], 32)):
                        out_ref[pl.ds((4 * quad + s) * lines, lines), pl.ds(128 * part, 128)] = value.astype(BF16)
            else:
                group = (start - npe) // 128 + tile
                for s, value in enumerate(swap_groups(tiles, 8)):
                    value = value.astype(BF16)
                    for half_id in range(2):
                        owner = 16 * group + 8 * half_id + s
                        out_ref[pl.ds(owner * lines, lines), 256:384] = value


def backward_columns(
    recv_ref, sens_ref, first_ref, second_ref, cos_hbm, sin_hbm, out_ref, part_ref, edge_ref, cos_ref, sin_ref, sems
):
    step = 256
    blocks = table_copies([(cos_hbm, cos_ref), (sin_hbm, sin_ref)], sems, step)
    npar = sens_ref.shape[4]
    coils, spots, rows = sens_ref.shape[1:4]
    cells = coils * spots * rows
    edges = coils * spots * 2 * REACH
    turned = recv_ref[...].astype(F32).T
    low = lax.axis_index("space") // 8 % 2 == 0
    for tile in range(npar // 128):
        here = pl.ds(tile * 2 * coils * spots * REACH, 2 * coils * spots * REACH)
        above, below = around(first_ref, second_ref, here, slice(0, 128))
        for k in range(2 * coils * spots):
            at = slice(k * REACH, (k + 1) * REACH)
            part, coil, spot = k // (coils * spots), k // spots % coils, k % spots
            edge_ref[part, coil, spot, :, pl.ds(128 * tile, 128)] = jnp.concatenate([below[at], above[at]], axis=0)
    border = jnp.where(low, turned[2 * cells : 2 * cells + 2 * edges], turned[2 * cells + 2 * edges :])
    x = jnp.concatenate([turned[: 2 * cells], border], axis=0).astype(BF16)
    for start in range(0, npar, step):
        here = pl.ds(start, step)
        arrived(blocks[start // step])
        by_cos = nn(x, cos_ref[:, here])
        by_sin = nn(x, sin_ref[:, here])
        for first, count, profile_ref, offset in ((0, cells, sens_ref, 0), (2 * cells, edges, edge_ref, rows)):
            second = first + count
            last = second + count
            real = by_cos[first:second] - by_sin[second:last]
            imag = by_cos[second:last] + by_sin[first:second]
            per_coil = count // coils
            height = per_coil // spots
            sums = [0.0, 0.0]
            for coil in range(coils):
                profile = [
                    jnp.concatenate([profile_ref[part, coil, spot, :, here] for spot in range(spots)], axis=0).astype(F32)
                    for part in range(2)
                ]
                re = real[coil * per_coil : (coil + 1) * per_coil]
                im = imag[coil * per_coil : (coil + 1) * per_coil]
                sums[0] = sums[0] + (profile[0] * re + profile[1] * im)
                sums[1] = sums[1] + (profile[0] * im - profile[1] * re)
            for part in range(2):
                for spot in range(spots):
                    row = (part * spots + spot) * (rows + 2 * REACH) + offset
                    part_ref[pl.ds(row, height), here] = sums[part][spot * height : (spot + 1) * height]
    total = part_ref.shape[0]
    owners = out_ref.shape[0] // total
    width = npar // owners
    lane = lax.broadcasted_iota(jnp.int32, (total, 128), 1)
    count = npar // 128
    for owner in range(owners):
        tile, off = divmod(width * owner, 128)
        value = part_ref[:, pl.ds(128 * tile, 128)]
        if off:
            value = pltpu.roll(value, 128 - off, 1)
            if tile + 1 < count:
                following = pltpu.roll(part_ref[:, pl.ds(128 * (tile + 1), 128)], 128 - off, 1)
                value = jnp.where((lane >= 128 - off) & (lane < 112), following, value)
        elif tile:
            value = jnp.where(lane >= 112, part_ref[:, pl.ds(128 * (tile - 1), 128)], value)
        out_ref[pl.ds(owner * total, total), :] = value.astype(BF16)


def pack_rows(state_ref, sens_ref, first_ref, second_ref):
    channels, spots, rows, cols = state_ref.shape
    coils, npar = sens_ref.shape[1], sens_ref.shape[4]
    even = lax.axis_index("space") % 2 == 0
    at = 0

    def store(tail, head, width):
        first_ref[pl.ds(at, 8), 0:width] = jnp.where(even, tail, head).astype(BF16)
        second_ref[pl.ds(at, 8), 0:width] = jnp.where(even, head, tail).astype(BF16)

    for tile in range(npar // 128):
        here = pl.ds(128 * tile, 128)
        for part in range(2):
            for coil in range(coils):
                pair = [
                    joined_edges([sens_ref[part, coil, spot, pl.ds(low, 8), here] for spot in range(2)], low)
                    for low in (rows - 8, 0)
                ]
                store(*pair, 128)
                at += 8
    for channel in range(channels):
        pair = [
            joined_edges([state_ref[channel, spot, pl.ds(low, 8), :].astype(F32) for spot in range(2)], low)
            for low in (rows - 8, 0)
        ]
        store(*pair, cols)
        at += 8


def joined_edges(pair, low):
    first, second = pair
    if low:
        return jnp.concatenate([first[REACH:], second[REACH:]], axis=0)
    return jnp.concatenate([first[:REACH], second[:REACH]], axis=0)


def around(first_ref, second_ref, here, cols):
    even = lax.axis_index("space") % 2 == 0
    first, second = first_ref[here, cols].astype(F32), second_ref[here, cols].astype(F32)
    return jnp.where(even, second, first), jnp.where(even, first, second)


def tall_state(state_ref, first_ref, second_ref, channel, spot, skip):
    cols = state_ref.shape[3]
    above, below = around(first_ref, second_ref, pl.ds(skip + 8 * channel, 8), slice(0, cols))
    below = below[spot * REACH : (spot + 1) * REACH]
    above = above[spot * REACH : (spot + 1) * REACH]
    value = jnp.concatenate([state_ref[channel, spot].astype(F32), jnp.concatenate([below, above], axis=0)], axis=0)
    return jnp.concatenate([value, jnp.zeros((value.shape[0], 128 - cols), F32)], axis=1)


def pack_cols(state_ref, first_ref, second_ref, tail_ref, head_ref):
    channels, spots, rows, cols = state_ref.shape
    tall = rows + 2 * REACH
    skip = first_ref.shape[0] - channels * spots * REACH
    per = 128 // REACH
    lane = lax.broadcasted_iota(jnp.int32, (tall, 128), 1)
    for group in range(channels * spots // per):
        tail = head = jnp.zeros((tall, 128), F32)
        for k in range(per):
            channel, spot = divmod(group * per + k, spots)
            value = tall_state(state_ref, first_ref, second_ref, channel, spot, skip)
            here = lane // REACH == k
            tail = jnp.where(here, pltpu.roll(value, (REACH * k - cols + REACH) % 128, 1), tail)
            head = jnp.where(here, pltpu.roll(value, REACH * k, 1) if k else value, head)
        tail_ref[pl.ds(group * tall, tall), :] = tail.astype(BF16)
        head_ref[pl.ds(group * tall, tall), :] = head.astype(BF16)


def spread_state(state_ref, first_ref, second_ref, left_ref, right_ref, out_ref, wide_ref):
    channels, spots, rows, cols = state_ref.shape
    tall = rows + 2 * REACH
    half = channels // 2
    skip = first_ref.shape[0] - channels * spots * REACH
    per = 128 // REACH
    lane = lax.broadcasted_iota(jnp.int32, (tall, 128), 1)
    for channel in range(channels):
        for spot in range(spots):
            group, k = divmod(channel * spots + spot, per)
            value = tall_state(state_ref, first_ref, second_ref, channel, spot, skip)
            here = pl.ds(group * tall, tall)
            right = pltpu.roll(right_ref[here, :].astype(F32), (cols - REACH * k) % 128, 1)
            left = pltpu.roll(left_ref[here, :].astype(F32), (128 - REACH - REACH * k) % 128, 1)
            value = jnp.where((lane >= cols) & (lane < cols + REACH), right, value)
            value = jnp.where(lane >= 128 - REACH, left, value)
            at = ((channel // half * spots + spot) * half + channel % half) * tall
            wide_ref[pl.ds(at, tall), :] = value
    count = channels * spots
    for i in range(tall):
        out_ref[pl.ds(i * count, count), :] = wide_ref[pl.ds((i - REACH) % tall, count, stride=tall), :].astype(BF16)


def coupling_weights(kernels_ref, biases_ref, mixers_ref, inject_ref, weight_ref, mixer_ref, bias_ref, added_ref):
    layers = kernels_ref.shape[0]
    half = kernels_ref.shape[2]
    eye = lax.broadcasted_iota(jnp.int32, (half, half), 0) == lax.broadcasted_iota(jnp.int32, (half, half), 1)
    zero = jnp.zeros((half, half), F32)
    for layer in range(layers):
        for c in range(3):
            for out_spot in range(2):
                blocks = [
                    kernels_ref[layer, 9 * (in_spot - out_spot + 1) + 3 * b + c].astype(F32)
                    for b in range(3)
                    for in_spot in range(2)
                ]
                weight_ref[layer, pl.ds((2 * c + out_spot) * half, half), :] = jnp.concatenate(blocks, axis=1).astype(BF16)
        mixer = mixers_ref[layer].astype(F32)
        mixer_ref[layer, 0:half, :] = jnp.concatenate([mixer, zero], axis=1).astype(BF16)
        mixer_ref[layer, half : 2 * half, :] = jnp.concatenate([zero, mixer], axis=1).astype(BF16)
        row = jnp.broadcast_to(biases_ref[pl.ds(layer, 1), :], (half, half))
        column = jnp.sum(jnp.where(eye, row, 0.0), axis=1, keepdims=True)
        bias_ref[layer] = jnp.broadcast_to(jnp.concatenate([column, column], axis=0), (2 * half, 128))
    wide = lax.broadcasted_iota(jnp.int32, (2 * half, 2 * half), 0) == lax.broadcasted_iota(jnp.int32, (2 * half, 2 * half), 1)
    for part in range(2):
        row = jnp.broadcast_to(inject_ref[pl.ds(part, 1), :], (2 * half, 2 * half))
        column = jnp.broadcast_to(jnp.sum(jnp.where(wide, row, 0.0), axis=1, keepdims=True), (2 * half, 128))
        added_ref[part] = jnp.concatenate(
            [column[:half], column[:half], column[half:], column[half:]], axis=0
        )


def couple(recv_ref, state_ref, weight_ref, mixer_ref, bias_ref, inject_ref, new_ref, grad_ref, wide_ref, a_ref, b_ref):
    channels, spots, rows, cols = new_ref.shape
    tall = rows + 2 * REACH
    half = channels // 2
    block = spots * half
    total = 2 * spots * tall
    owners = recv_ref.shape[0] // total
    grad = recv_ref[0:total, :].astype(F32)
    for owner in range(1, owners):
        grad = grad + recv_ref[pl.ds(owner * total, total), :].astype(F32)
    for part in range(2):
        for spot in range(spots):
            row = (part * spots + spot) * tall
            grad_ref[part, spot] = grad[row : row + rows, :cols]
    space, coil = lax.axis_index("space"), lax.axis_index("coil")
    lane = lax.broadcasted_iota(jnp.int32, (1, 128), 1)
    col_id = coil * cols + jnp.where(lane < 112, lane, lane - 128)
    col_keep = ((col_id >= 0) & (col_id < cols * owners)).astype(F32)
    upper = jnp.where(space > 0, col_keep, 0.0)
    lower = jnp.where(space < lax.axis_size("space") - 1, col_keep, 0.0)

    def keep(i):
        return upper if i < REACH else lower if i >= REACH + rows else col_keep

    scale = [inject_ref[part] for part in range(2)]
    for i in range(tall):
        source = (i - REACH) % tall
        here = [
            jnp.concatenate(
                [
                    jnp.broadcast_to(grad[at : at + 1, :], (half, 128))
                    for at in ((part * spots + spot) * tall + source for spot in range(spots))
                ],
                axis=0,
            )
            for part in range(2)
        ]
        for which, ref in enumerate((a_ref, b_ref)):
            at = slice(which * block, (which + 1) * block)
            value = state_ref[pl.ds((2 * i + which) * block, block), :].astype(F32)
            value = value + (scale[0][at] * here[0] + scale[1][at] * here[1])
            ref[pl.ds(i * block, block), :] = (value * keep(i)).astype(BF16)
    for layer in range(weight_ref.shape[0]):
        source_ref, target_ref = (a_ref, b_ref) if layer % 2 == 0 else (b_ref, a_ref)
        weight = weight_ref[layer]
        mixer = mixer_ref[layer]
        bias = bias_ref[layer]
        first, last = 1 + layer, tall - 1 - layer
        for start in range(first, last, BATCH):
            lines = range(start, min(start + BATCH, last))
            cells = jnp.concatenate([source_ref[pl.ds((i - 1) * block, 3 * block), :] for i in lines], axis=1)
            taps = nn(weight, cells)
            raw = []
            for j in range(len(lines)):
                at = slice(128 * j, 128 * j + 128)
                value = pltpu.roll(taps[0:block, at], 1, 1) + taps[block : 2 * block, at]
                value = value + pltpu.roll(taps[2 * block :, at], 127, 1)
                raw.append(jnp.maximum(value + bias, 0.0).astype(BF16))
            mixed = nn(mixer, jnp.concatenate(raw, axis=1))
            for j, i in enumerate(lines):
                here = pl.ds(i * block, block)
                value = target_ref[here, :].astype(F32) + mixed[:, 128 * j : 128 * j + 128]
                target_ref[here, :] = (value * keep(i)).astype(BF16)
    for i in range(REACH, REACH + rows):
        source = i - REACH
        wide_ref[pl.ds(source, block, stride=rows), :] = a_ref[pl.ds(i * block, block), :].astype(F32)
        wide_ref[pl.ds(block * rows + source, block, stride=rows), :] = b_ref[pl.ds(i * block, block), :].astype(F32)
    for channel in range(channels):
        for spot in range(spots):
            at = (channel // half * block + spot * half + channel % half) * rows
            new_ref[channel, spot] = wide_ref[pl.ds(at, rows), :][:, :cols].astype(BF16)


def from_previous(tail, axis):
    return lax.ppermute(tail, axis, [(i, i + 1) for i in range(lax.axis_size(axis) - 1)])


def from_next(head, axis):
    return lax.ppermute(head, axis, [(i + 1, i) for i in range(lax.axis_size(axis) - 1)])


def swapped(array, axis, start):
    count = lax.axis_size(axis)
    pairs = [(i, i + 1) for i in range(start, count - 1, 2)]
    return lax.ppermute(array, axis, pairs + [(j, i) for i, j in pairs])


def per_device(state, sens, kdata, mask, inject, kernels, biases, mixers):
    channels, spots, rows, cols = state.shape
    coils = sens.shape[1]
    npar = sens.shape[4]
    npe = kdata.shape[4]
    lines = kdata.shape[3]
    groups = lax.axis_size("space")
    owners = lax.axis_size("coil")
    tall = rows + 2 * REACH
    cells = coils * spots * rows
    layers = kernels.shape[0]
    block = channels // 2 * spots

    estimate = jnp.pad(state[0:2], ((0, 0), (0, 0), (0, 0), (0, 128 - cols)))
    estimate = jnp.broadcast_to(estimate[None], (owners, *estimate.shape))
    estimate = lax.all_to_all(estimate, "coil", 0, 0, tiled=True)

    edge_columns = [
        (rows * d + r) % npe for d in range(groups) for r in (*range(rows, rows + REACH), *range(-REACH, 0))
    ]
    pe_columns = [*range(npe), *edge_columns]
    def table_scratch(length, columns, blocks):
        return [((length, columns), BF16)] * 2 + [pltpu.SemaphoreType.DMA((2 * blocks,))]

    def tables(length, columns):
        out = pltpu.HBM((length, len(columns)), BF16)
        factors = jnp.asarray(dft_factors(length, columns, FINE))
        scratch = table_scratch(length, len(columns), length // FINE // 4)
        return [in_hbm(table) for table in call(dft_tables, [out, out], scratch, "dft_tables", plain(factors))]

    depth = 2 * coils * spots * REACH * (npar // 128) + channels * spots * REACH
    par_factors = jnp.asarray(dft_factors(npar, range(npar), FINE))
    pe_factors = jnp.asarray(dft_factors(npe, pe_columns, FINE))

    def table_scratch(length, columns, blocks):
        return [((length, columns), BF16)] * 2 + [pltpu.SemaphoreType.DMA((2 * blocks,))]

    par_scratch = table_scratch(npar, npar, npar // FINE // 4)
    pe_scratch = table_scratch(npe, len(pe_columns), npe // FINE // 4)
    first, second, state, sens, *tables = call(
        prepare,
        [((depth, 128), BF16)] * 2
        + [(state.shape, BF16), (sens.shape, F32)]
        + [pltpu.HBM((npar, npar), BF16)] * 2
        + [pltpu.HBM((npe, len(pe_columns)), BF16)] * 2,
        [
            (par_factors.shape, F32),
            (pe_factors.shape, F32),
            *par_scratch[:2],
            *pe_scratch[:2],
            pltpu.SemaphoreType.DMA((4,)),
            par_scratch[2],
            pe_scratch[2],
        ],
        "prepare",
        in_hbm(state), in_hbm(sens), in_hbm(par_factors), in_hbm(pe_factors),
    )
    par_tables = [in_hbm(table) for table in tables[:2]]
    pe_tables = [in_hbm(table) for table in tables[2:]]

    (sent,) = call(
        forward_columns,
        [jax.ShapeDtypeStruct((npar, 2 * cells), BF16)],
        [((2 * cells, npar), BF16), *table_scratch(npar, npar, 1)],
        "forward_columns",
        estimate, sens, *par_tables,
    )
    sent, first, second = lax.optimization_barrier((sent, first, second))
    spectra = lax.all_to_all(sent, "space", 0, 0, tiled=True)
    first, second = swapped(first, "space", 0), swapped(second, "space", 1)

    (sent,) = call(
        consistency,
        [jax.ShapeDtypeStruct((npar, 384), BF16)],
        [((8 * lines, npe), BF16)] * 2 + table_scratch(npe, len(pe_columns), len(pe_columns) // 256),
        "consistency",
        spectra, kdata, mask, *pe_tables,
    )
    sent, first, second = lax.optimization_barrier((sent, first, second))
    returned = lax.all_to_all(sent, "space", 0, 0, tiled=True)

    packed = [((channels * spots * REACH // 128 * tall, 128), BF16)] * 2
    tail, head = call(pack_cols, packed, [], "pack_cols", state, first, second)
    left, right = from_previous(tail, "coil"), from_next(head, "coil")

    (sent,) = call(
        backward_columns,
        [jax.ShapeDtypeStruct((owners * 2 * spots * tall, 128), BF16)],
        [
            ((2 * spots * tall, npar), F32),
            ((2, coils, spots, 2 * REACH, npar), F32),
            *table_scratch(npar, npar, npar // 256),
        ],
        "backward_columns",
        returned, sens, first, second, *par_tables,
    )
    sent, left, right = lax.optimization_barrier((sent, left, right))
    shares = lax.all_to_all(sent, "coil", 0, 0, tiled=True)

    (spread,) = call(
        spread_state,
        [((tall * channels * spots, 128), BF16)],
        [((channels * spots * tall, 128), F32)],
        "spread_state",
        state, first, second, left, right,
    )

    weight, mixer, bias, added = call(
        coupling_weights,
        [
            ((layers, 3 * block, 3 * block), BF16),
            ((layers, block, block), BF16),
            ((layers, block, 128), F32),
            ((2, 2 * block, 128), F32),
        ],
        [],
        "coupling_weights",
        plain(kernels), plain(biases), plain(mixers), plain(inject.T),
    )
    new_state, gradient = call(
        couple,
        [jax.ShapeDtypeStruct(state.shape, BF16), jax.ShapeDtypeStruct((2, spots, rows, cols), F32)],
        [((2 * block * rows, 128), F32), ((block * tall, 128), BF16), ((block * tall, 128), BF16)],
        "couple",
        shares, spread, weight, mixer, bias, added,
    )
    return (new_state, gradient)


def solution(mesh):
    return jax.shard_map(
        per_device,
        mesh=mesh,
        in_specs=(
            P(None, None, "space", "coil"),
            P(None, "coil", None, "space", None),
            P(None, "coil", None, "space", None),
            P("space", None),
            P(),
            P(),
            P(),
            P(),
        ),
        out_specs=(P(None, None, "space", "coil"), P(None, None, "space", "coil")),
        check_vma=False,
    )
```

```python
import numpy as np

import jax
import jax.numpy as jnp
from jax import lax
from jax.experimental import pallas as pl
from jax.experimental.pallas import tpu as pltpu
from jax.sharding import PartitionSpec as P

F32 = jnp.float32
BF16 = jnp.bfloat16
REACH = 4
FINE = 32
BATCH = 38
VMEM = pl.BlockSpec(memory_space=pltpu.VMEM)
HBM = pl.BlockSpec(memory_space=pltpu.HBM)


def call(body, outs, scratch, name, *args):
    specs, values = [], []
    for arg in args:
        where, value = arg if isinstance(arg, tuple) else ("vmem", arg)
        if where != "plain":
            value = pltpu.with_memory_space_constraint(value, pltpu.HBM if where == "hbm" else pltpu.VMEM)
        specs.append(HBM if where == "hbm" else VMEM)
        values.append(value)
    shapes = [pltpu.VMEM(*out) if isinstance(out, tuple) else out for out in outs]
    placed = [VMEM if isinstance(out, (tuple, jax.ShapeDtypeStruct)) else HBM for out in outs]
    return pl.pallas_call(
        body,
        out_shape=shapes,
        in_specs=specs,
        out_specs=placed,
        scratch_shapes=[each if not isinstance(each, tuple) else pltpu.VMEM(*each) for each in scratch],
        compiler_params=pltpu.CompilerParams(vmem_limit_bytes=20 * 2**20),
        name=name,
    )(*values)


def in_hbm(value):
    return ("hbm", value)


def plain(value):
    return ("plain", value)


def table_copies(source, target, sems, step):
    copies = []
    for start in range(0, source.shape[0], step):
        here = pl.ds(start, step)
        copy = pltpu.make_async_copy(source.at[here, :], target.at[here, :], sems.at[len(copies)])
        copy.start()
        copies.append(copy)
    return copies


def arrived(block):
    for copy in block:
        copy.wait()


def dft_factors(length, columns):
    columns = np.asarray(columns)[None, :]
    steps = 2 * FINE * np.arange(length // 2 // FINE)
    coarse = np.concatenate([steps, steps + 1])[:, None] * columns % length
    fine = 2 * np.arange(FINE)[:, None] * columns % length
    angle_coarse = coarse * (2.0 * np.pi / length)
    angle_fine = fine * (2.0 * np.pi / length)
    scale = 1.0 / np.sqrt(length)
    parts = (np.cos(angle_coarse) * scale, np.sin(angle_coarse) * scale, np.cos(angle_fine), np.sin(angle_fine))
    return np.concatenate(parts).astype(np.float32)


def fill_table(factors_ref, table_hbm, table_ref, sems):
    count = table_ref.shape[0] // FINE
    width = factors_ref.shape[1]
    cos_b = factors_ref[pl.ds(2 * count, FINE), :]
    sin_b = factors_ref[pl.ds(2 * count + FINE, FINE), :]
    copies = []
    for a in range(count):
        here = pl.ds(a * FINE, FINE)
        cos, sin = factors_ref[pl.ds(a, 1), :], factors_ref[pl.ds(count + a, 1), :]
        table_ref[here, 0:width] = (cos * cos_b - sin * sin_b).astype(BF16)
        table_ref[here, width : 2 * width] = (sin * cos_b + cos * sin_b).astype(BF16)
        if a % 4 == 3:
            done = pl.ds((a - 3) * FINE, 4 * FINE)
            copy = pltpu.make_async_copy(table_ref.at[done, :], table_hbm.at[done, :], sems.at[len(copies)])
            copy.start()
            copies.append(copy)
    return copies


def prepare(
    state_hbm, sens_hbm, par_factors_hbm, pe_factors_hbm, kdata_hbm, mask_hbm,
    first_ref, second_ref, state_ref, sens_ref, sampled_ref, par_hbm, pe_hbm, data_hbm,
    par_factors, pe_factors, par_ref, pe_ref, kdata_ref, mask_ref, data_ref, sems, par_sems, pe_sems,
):
    pairs = (
        (par_factors_hbm, par_factors), (pe_factors_hbm, pe_factors), (state_hbm, state_ref), (sens_hbm, sens_ref),
        (kdata_hbm, kdata_ref), (mask_hbm, mask_ref),
    )
    copies = []
    for k, (source, target) in enumerate(pairs):
        copy = pltpu.make_async_copy(source, target, sems.at[k])
        copy.start()
        copies.append(copy)
    arrived(copies[0:1])
    sent = fill_table(par_factors, par_hbm, par_ref, par_sems)
    arrived(copies[1:2])
    sent = sent + fill_table(pe_factors, pe_hbm, pe_ref, pe_sems)
    arrived(copies[2:])
    sort_lines(kdata_ref, mask_ref, data_ref, sampled_ref)
    last = pltpu.make_async_copy(data_ref, data_hbm, sems.at[len(pairs)])
    last.start()
    pack_rows(state_ref, sens_ref, first_ref, second_ref)
    arrived(sent + [last])


def sort_lines(kdata_ref, mask_ref, data_ref, sampled_ref):
    step = 256
    row = lax.broadcasted_iota(jnp.int32, (step, step), 0)
    lane = lax.broadcasted_iota(jnp.int32, (step, step), 1)
    pick = jnp.where(row == 2 * (lane % 128) + lane // 128, 1.0, 0.0).astype(BF16)
    coils, spots, lines, npe = kdata_ref.shape[1:]
    for block in range(npe // step):
        here = pl.ds(step * block, step)
        value = jnp.concatenate(
            [kdata_ref[part, c, p, :, here] for part in range(2) for c in range(coils) for p in range(spots)], axis=0
        )
        high = value.astype(BF16)
        low = (value - high.astype(F32)).astype(BF16)
        value = nn(high, pick) + nn(low, pick)
        sampled = nn(mask_ref[:, here].astype(F32).astype(BF16), pick)
        for side in range(2):
            to = pl.ds(side * npe // 2 + 128 * block, 128)
            data_ref[:, to] = value[:, 128 * side : 128 * side + 128]
            sampled_ref[:, to] = sampled[:, 128 * side : 128 * side + 128]


def swap_groups(tiles, group):
    tiles = list(tiles)
    count = len(tiles)
    lane = lax.broadcasted_iota(jnp.int32, tiles[0].shape, 1)
    bit = count // 2
    while bit:
        shift = bit * group
        high = (lane // shift) % 2 == 1
        for low in range(count):
            if low & bit:
                continue
            a, b = tiles[low], tiles[low | bit]
            tiles[low] = jnp.where(high, pltpu.roll(b, shift, 1), a)
            tiles[low | bit] = jnp.where(high, b, pltpu.roll(a, 128 - shift, 1))
        bit //= 2
    return tiles


def nn(a, b):
    return lax.dot_general(a, b, (((1,), (0,)), ((), ())), preferred_element_type=F32)


def nt(a, b):
    return lax.dot_general(a, b, (((1,), (1,)), ((), ())), preferred_element_type=F32)


def forward_columns(est_ref, sens_ref, table_hbm, out_ref, img_ref, line_ref, table_ref, sems):
    owners = est_ref.shape[0]
    coils, spots, rows, npar = sens_ref.shape[1:]
    step = 128
    copies = table_copies(table_hbm, table_ref, sems, step)
    width = npar // owners
    lane = lax.broadcasted_iota(jnp.int32, (rows, 128), 1)
    middle = npar // 2

    def estimate(spot, tile):
        full = []
        for part in range(2):
            value = None
            for owner in range(128 * tile // width, (128 * tile + 127) // width + 1):
                at = width * owner - 128 * tile
                piece = est_ref[owner, part, spot].astype(F32)
                if at % 128:
                    piece = pltpu.roll(piece, at % 128, 1)
                value = piece if value is None else jnp.where(lane >= at, piece, value)
            full.append(value)
        return full

    for spot in range(spots):
        for tile in range(middle // 128):
            sides = [estimate(spot, tile + side * middle // 128) for side in range(2)]
            for coil in range(coils):
                images = []
                for side in range(2):
                    cols = pl.ds(128 * tile + side * middle, 128)
                    sens_re = sens_ref[0, coil, spot, :, cols]
                    sens_im = sens_ref[1, coil, spot, :, cols]
                    est_re, est_im = sides[side]
                    images.append((sens_re * est_re - sens_im * est_im, sens_re * est_im + sens_im * est_re))
                row = (coil * spots + spot) * rows
                cols = pl.ds(128 * tile, 128)
                for part in range(2):
                    here = pl.ds(128 * part + row, rows)
                    img_ref[0, here, cols] = (images[0][part] + images[1][part]).astype(BF16)
                    img_ref[1, here, cols] = (images[0][part] - images[1][part]).astype(BF16)
    for odd in range(2):
        img = img_ref[odd]
        for start in range(0, middle, step):
            here = pl.ds(odd * middle + start, step)
            arrived(copies[(odd * middle + start) // step : (odd * middle + start) // step + 1])
            by_cos = nt(table_ref[here, 0:middle], img)
            by_sin = nt(table_ref[here, middle:npar], img)
            to = pl.ds(2 * start + odd, step, stride=2)
            line_ref[0, to, :] = by_cos[:, :128] + by_sin[:, 128:]
            line_ref[1, to, :] = by_cos[:, 128:] - by_sin[:, :128]
    out_ref[:, 0:128] = line_ref[0].astype(BF16)
    out_ref[:, 128:256] = line_ref[1].astype(BF16)


def consistency(
    recv_ref, data_hbm, sampled_ref, table_hbm, out_ref, x_ref, res_ref, data_ref, table_ref, sems, data_sem
):
    step = 256
    copies = table_copies(table_hbm, table_ref, sems, step)
    data_copy = pltpu.make_async_copy(data_hbm, data_ref, data_sem)
    data_copy.start()
    lines, npe = sampled_ref.shape
    middle = npe // 2
    width = table_ref.shape[1] // 2
    half = 4 * lines
    quads = npe // 128

    def gathered(quad):
        stacked = []
        for part in range(2):
            tiles = [
                recv_ref[pl.ds((4 * quad + s) * lines, lines), pl.ds(128 * part, 128)].astype(F32) for s in range(4)
            ]
            stacked += swap_groups(tiles, 32)
        return jnp.concatenate(stacked, axis=0)

    for quad in range(quads // 2):
        low, high = gathered(quad), gathered(quad + quads // 2)
        x_ref[0, :, pl.ds(128 * quad, 128)] = (low + high).astype(BF16)
        x_ref[1, :, pl.ds(128 * quad, 128)] = (low - high).astype(BF16)
    data_copy.wait()
    for odd in range(2):
        x = x_ref[odd]
        for start in range(odd * middle, (odd + 1) * middle, step):
            here = pl.ds(start, step)
            arrived(copies[start // step : start // step + 1])
            by_cos = nt(x, table_ref[here, 0:middle])
            by_sin = nt(x, table_ref[here, width : width + middle])
            sampled = jnp.concatenate([sampled_ref[:, here]] * 4, axis=0)
            real = sampled * (by_cos[:half] + by_sin[half:] - data_ref[0:half, here])
            imag = sampled * (by_cos[half:] - by_sin[:half] - data_ref[half : 2 * half, here])
            res_ref[0:half, here] = real.astype(BF16)
            res_ref[half : 2 * half, here] = imag.astype(BF16)
    res = [res_ref[:, 0:middle], res_ref[:, middle:npe]]

    for start in range(0, width, step):
        size = min(step, width - start)
        sums = []
        for odd in range(2):
            rows = pl.ds(odd * middle, middle)
            by_cos = nn(res[odd], table_ref[rows, pl.ds(start, size)])
            by_sin = nn(res[odd], table_ref[rows, pl.ds(width + start, size)])
            sums.append((by_cos[:half] - by_sin[half:], by_cos[half:] + by_sin[:half]))
        for side in range(2):
            parts = [sums[0][part] - sums[1][part] if side else sums[0][part] + sums[1][part] for part in range(2)]
            for tile in range(size // 128):
                at = slice(128 * tile, 128 * tile + 128)
                tiles = [part[lines * g : lines * (g + 1), at] for part in parts for g in range(4)]
                if start < middle:
                    quad = start // 128 + tile + side * quads // 2
                    for part in range(2):
                        for s, value in enumerate(swap_groups(tiles[4 * part : 4 * part + 4], 32)):
                            out_ref[pl.ds((4 * quad + s) * lines, lines), pl.ds(128 * part, 128)] = value.astype(BF16)
                else:
                    for s, value in enumerate(swap_groups(tiles, 8)):
                        value = value.astype(BF16)
                        for half_id in range(2):
                            owner = 16 * side + 8 * half_id + s
                            out_ref[pl.ds(owner * lines, lines), 256:384] = value


def backward_columns(
    recv_ref, sens_ref, first_ref, second_ref, table_hbm, out_ref, part_ref, edge_ref, line_ref, table_ref, sems
):
    copies = table_copies(table_hbm, table_ref, sems, table_ref.shape[0] // 2)
    coils, spots, rows, npar = sens_ref.shape[1:]
    cells = coils * spots * rows
    edges = coils * spots * 2 * REACH
    middle = npar // 2
    low = lax.axis_index("space") // 8 % 2 == 0
    for tile in range(3):
        line_ref[tile] = recv_ref[:, 128 * tile : 128 * tile + 128].astype(F32)
    for tile in range(npar // 128):
        here = pl.ds(tile * 2 * coils * spots * REACH, 2 * coils * spots * REACH)
        above, below = around(first_ref, second_ref, here, slice(0, 128))
        for k in range(2 * coils * spots):
            at = slice(k * REACH, (k + 1) * REACH)
            part, coil, spot = k // (coils * spots), k // spots % coils, k % spots
            edge_ref[part, coil, spot, :, pl.ds(128 * tile, 128)] = jnp.concatenate([below[at], above[at]], axis=0)
    sums = []
    for odd in range(2):
        turned = [line_ref[tile, pl.ds(odd, middle, stride=2), :].T for tile in range(3)]
        border = jnp.where(low, turned[2][: 2 * edges], turned[2][2 * edges :])
        x = jnp.concatenate([turned[0], turned[1], border], axis=0).astype(BF16)
        arrived(copies[odd : odd + 1])
        sums.append(nn(x, table_ref[odd * middle : (odd + 1) * middle, :]))
    for first, count, profile_ref, offset in ((0, cells, sens_ref, 0), (2 * cells, edges, edge_ref, rows)):
        second = first + count
        last = second + count
        per_coil = count // coils
        height = per_coil // spots
        real = [each[first:second, :middle] - each[second:last, middle:] for each in sums]
        imag = [each[second:last, :middle] + each[first:second, middle:] for each in sums]
        for side in range(2):
            here = pl.ds(side * middle, middle)
            whole = [each[0] - each[1] if side else each[0] + each[1] for each in (real, imag)]
            total = [0.0, 0.0]
            for coil in range(coils):
                profile = [
                    jnp.concatenate([profile_ref[part, coil, spot, :, here] for spot in range(spots)], axis=0)
                    for part in range(2)
                ]
                re, im = [each[coil * per_coil : (coil + 1) * per_coil] for each in whole]
                total[0] = total[0] + (profile[0] * re + profile[1] * im)
                total[1] = total[1] + (profile[0] * im - profile[1] * re)
            for part in range(2):
                for spot in range(spots):
                    row = (part * spots + spot) * (rows + 2 * REACH) + offset
                    part_ref[pl.ds(row, height), here] = total[part][spot * height : (spot + 1) * height]
    total = part_ref.shape[0]
    owners = out_ref.shape[0] // total
    width = npar // owners
    lane = lax.broadcasted_iota(jnp.int32, (total, 128), 1)
    count = npar // 128
    for owner in range(owners):
        tile, off = divmod(width * owner, 128)
        value = part_ref[:, pl.ds(128 * tile, 128)]
        if off:
            value = pltpu.roll(value, 128 - off, 1)
            if tile + 1 < count:
                following = pltpu.roll(part_ref[:, pl.ds(128 * (tile + 1), 128)], 128 - off, 1)
                value = jnp.where((lane >= 128 - off) & (lane < 112), following, value)
        elif tile:
            value = jnp.where(lane >= 112, part_ref[:, pl.ds(128 * (tile - 1), 128)], value)
        out_ref[pl.ds(owner * total, total), :] = value.astype(BF16)


def pack_rows(state_ref, sens_ref, first_ref, second_ref):
    channels, spots, rows, cols = state_ref.shape
    coils, npar = sens_ref.shape[1], sens_ref.shape[4]
    even = lax.axis_index("space") % 2 == 0
    at = 0

    def store(tail, head, width):
        first_ref[pl.ds(at, 8), 0:width] = jnp.where(even, tail, head).astype(BF16)
        second_ref[pl.ds(at, 8), 0:width] = jnp.where(even, head, tail).astype(BF16)

    for tile in range(npar // 128):
        here = pl.ds(128 * tile, 128)
        for part in range(2):
            for coil in range(coils):
                pair = [
                    joined_edges([sens_ref[part, coil, spot, pl.ds(low, 8), here] for spot in range(2)], low)
                    for low in (rows - 8, 0)
                ]
                store(*pair, 128)
                at += 8
    for channel in range(channels):
        pair = [
            joined_edges([state_ref[channel, spot, pl.ds(low, 8), :].astype(F32) for spot in range(2)], low)
            for low in (rows - 8, 0)
        ]
        store(*pair, cols)
        at += 8


def joined_edges(pair, low):
    first, second = pair
    if low:
        return jnp.concatenate([first[REACH:], second[REACH:]], axis=0)
    return jnp.concatenate([first[:REACH], second[:REACH]], axis=0)


def around(first_ref, second_ref, here, cols):
    even = lax.axis_index("space") % 2 == 0
    first, second = first_ref[here, cols].astype(F32), second_ref[here, cols].astype(F32)
    return jnp.where(even, second, first), jnp.where(even, first, second)


def tall_state(state_ref, first_ref, second_ref, channel, spot, skip):
    cols = state_ref.shape[3]
    above, below = around(first_ref, second_ref, pl.ds(skip + 8 * channel, 8), slice(0, cols))
    below = below[spot * REACH : (spot + 1) * REACH]
    above = above[spot * REACH : (spot + 1) * REACH]
    value = jnp.concatenate([state_ref[channel, spot].astype(F32), jnp.concatenate([below, above], axis=0)], axis=0)
    return jnp.concatenate([value, jnp.zeros((value.shape[0], 128 - cols), F32)], axis=1)


def pack_cols(state_ref, first_ref, second_ref, tail_ref, head_ref):
    channels, spots, rows, cols = state_ref.shape
    tall = rows + 2 * REACH
    skip = first_ref.shape[0] - channels * spots * REACH
    per = 128 // REACH
    lane = lax.broadcasted_iota(jnp.int32, (tall, 128), 1)
    for group in range(channels * spots // per):
        tail = head = jnp.zeros((tall, 128), F32)
        for k in range(per):
            channel, spot = divmod(group * per + k, spots)
            value = tall_state(state_ref, first_ref, second_ref, channel, spot, skip)
            here = lane // REACH == k
            tail = jnp.where(here, pltpu.roll(value, (REACH * k - cols + REACH) % 128, 1), tail)
            head = jnp.where(here, pltpu.roll(value, REACH * k, 1) if k else value, head)
        tail_ref[pl.ds(group * tall, tall), :] = tail.astype(BF16)
        head_ref[pl.ds(group * tall, tall), :] = head.astype(BF16)


def spread_state(state_ref, first_ref, second_ref, left_ref, right_ref, out_ref, wide_ref):
    channels, spots, rows, cols = state_ref.shape
    tall = rows + 2 * REACH
    half = channels // 2
    skip = first_ref.shape[0] - channels * spots * REACH
    per = 128 // REACH
    lane = lax.broadcasted_iota(jnp.int32, (tall, 128), 1)
    for channel in range(channels):
        for spot in range(spots):
            group, k = divmod(channel * spots + spot, per)
            value = tall_state(state_ref, first_ref, second_ref, channel, spot, skip)
            here = pl.ds(group * tall, tall)
            right = pltpu.roll(right_ref[here, :].astype(F32), (cols - REACH * k) % 128, 1)
            left = pltpu.roll(left_ref[here, :].astype(F32), (128 - REACH - REACH * k) % 128, 1)
            value = jnp.where((lane >= cols) & (lane < cols + REACH), right, value)
            value = jnp.where(lane >= 128 - REACH, left, value)
            at = ((channel // half * spots + spot) * half + channel % half) * tall
            wide_ref[pl.ds(at, tall), :] = value
    count = channels * spots
    for i in range(tall):
        out_ref[pl.ds(i * count, count), :] = wide_ref[pl.ds((i - REACH) % tall, count, stride=tall), :].astype(BF16)


def coupling_weights(kernels_ref, biases_ref, mixers_ref, inject_ref, weight_ref, mixer_ref, bias_ref, added_ref):
    layers = kernels_ref.shape[0]
    half = kernels_ref.shape[2]
    eye = lax.broadcasted_iota(jnp.int32, (half, half), 0) == lax.broadcasted_iota(jnp.int32, (half, half), 1)
    zero = jnp.zeros((half, half), F32)
    for layer in range(layers):
        for c in range(3):
            for out_spot in range(2):
                blocks = [
                    kernels_ref[layer, 9 * (in_spot - out_spot + 1) + 3 * b + c].astype(F32)
                    for b in range(3)
                    for in_spot in range(2)
                ]
                weight_ref[layer, pl.ds((2 * c + out_spot) * half, half), :] = jnp.concatenate(blocks, axis=1).astype(BF16)
        mixer = mixers_ref[layer].astype(F32)
        mixer_ref[layer, 0:half, :] = jnp.concatenate([mixer, zero], axis=1).astype(BF16)
        mixer_ref[layer, half : 2 * half, :] = jnp.concatenate([zero, mixer], axis=1).astype(BF16)
        row = jnp.broadcast_to(biases_ref[pl.ds(layer, 1), :], (half, half))
        column = jnp.sum(jnp.where(eye, row, 0.0), axis=1, keepdims=True)
        bias_ref[layer] = jnp.broadcast_to(jnp.concatenate([column, column], axis=0), (2 * half, 128))
    wide = lax.broadcasted_iota(jnp.int32, (2 * half, 2 * half), 0) == lax.broadcasted_iota(jnp.int32, (2 * half, 2 * half), 1)
    for part in range(2):
        row = jnp.broadcast_to(inject_ref[pl.ds(part, 1), :], (2 * half, 2 * half))
        column = jnp.broadcast_to(jnp.sum(jnp.where(wide, row, 0.0), axis=1, keepdims=True), (2 * half, 128))
        added_ref[part] = jnp.concatenate(
            [column[:half], column[:half], column[half:], column[half:]], axis=0
        )


def couple(recv_ref, state_ref, weight_ref, mixer_ref, bias_ref, inject_ref, new_ref, grad_ref, wide_ref, a_ref, b_ref):
    channels, spots, rows, cols = new_ref.shape
    tall = rows + 2 * REACH
    half = channels // 2
    block = spots * half
    total = 2 * spots * tall
    owners = recv_ref.shape[0] // total
    grad = recv_ref[0:total, :].astype(F32)
    for owner in range(1, owners):
        grad = grad + recv_ref[pl.ds(owner * total, total), :].astype(F32)
    for part in range(2):
        for spot in range(spots):
            row = (part * spots + spot) * tall
            grad_ref[part, spot] = grad[row : row + rows, :cols]
    space, coil = lax.axis_index("space"), lax.axis_index("coil")
    lane = lax.broadcasted_iota(jnp.int32, (1, 128), 1)
    col_id = coil * cols + jnp.where(lane < 112, lane, lane - 128)
    col_keep = ((col_id >= 0) & (col_id < cols * owners)).astype(F32)
    upper = jnp.where(space > 0, col_keep, 0.0)
    lower = jnp.where(space < lax.axis_size("space") - 1, col_keep, 0.0)

    def keep(i):
        return upper if i < REACH else lower if i >= REACH + rows else col_keep

    scale = [inject_ref[part] for part in range(2)]
    for i in range(tall):
        source = (i - REACH) % tall
        here = [
            jnp.concatenate(
                [
                    jnp.broadcast_to(grad[at : at + 1, :], (half, 128))
                    for at in ((part * spots + spot) * tall + source for spot in range(spots))
                ],
                axis=0,
            )
            for part in range(2)
        ]
        for which, ref in enumerate((a_ref, b_ref)):
            at = slice(which * block, (which + 1) * block)
            value = state_ref[pl.ds((2 * i + which) * block, block), :].astype(F32)
            value = value + (scale[0][at] * here[0] + scale[1][at] * here[1])
            ref[pl.ds(i * block, block), :] = (value * keep(i)).astype(BF16)
    for layer in range(weight_ref.shape[0]):
        source_ref, target_ref = (a_ref, b_ref) if layer % 2 == 0 else (b_ref, a_ref)
        weight = weight_ref[layer]
        mixer = mixer_ref[layer]
        bias = bias_ref[layer]
        first, last = 1 + layer, tall - 1 - layer
        for start in range(first, last, BATCH):
            lines = range(start, min(start + BATCH, last))
            cells = jnp.concatenate([source_ref[pl.ds((i - 1) * block, 3 * block), :] for i in lines], axis=1)
            taps = nn(weight, cells)
            raw = []
            for j in range(len(lines)):
                at = slice(128 * j, 128 * j + 128)
                value = pltpu.roll(taps[0:block, at], 1, 1) + taps[block : 2 * block, at]
                value = value + pltpu.roll(taps[2 * block :, at], 127, 1)
                raw.append(jnp.maximum(value + bias, 0.0).astype(BF16))
            mixed = nn(mixer, jnp.concatenate(raw, axis=1))
            for j, i in enumerate(lines):
                here = pl.ds(i * block, block)
                value = target_ref[here, :].astype(F32) + mixed[:, 128 * j : 128 * j + 128]
                target_ref[here, :] = (value * keep(i)).astype(BF16)
    for i in range(REACH, REACH + rows):
        source = i - REACH
        wide_ref[pl.ds(source, block, stride=rows), :] = a_ref[pl.ds(i * block, block), :].astype(F32)
        wide_ref[pl.ds(block * rows + source, block, stride=rows), :] = b_ref[pl.ds(i * block, block), :].astype(F32)
    for channel in range(channels):
        for spot in range(spots):
            at = (channel // half * block + spot * half + channel % half) * rows
            new_ref[channel, spot] = wide_ref[pl.ds(at, rows), :][:, :cols].astype(BF16)


def from_previous(tail, axis):
    return lax.ppermute(tail, axis, [(i, i + 1) for i in range(lax.axis_size(axis) - 1)])


def from_next(head, axis):
    return lax.ppermute(head, axis, [(i + 1, i) for i in range(lax.axis_size(axis) - 1)])


def swapped(array, axis, start):
    count = lax.axis_size(axis)
    pairs = [(i, i + 1) for i in range(start, count - 1, 2)]
    return lax.ppermute(array, axis, pairs + [(j, i) for i, j in pairs])


def per_device(state, sens, kdata, mask, inject, kernels, biases, mixers):
    channels, spots, rows, cols = state.shape
    coils = sens.shape[1]
    npar = sens.shape[4]
    npe = kdata.shape[4]
    lines = kdata.shape[3]
    groups = lax.axis_size("space")
    owners = lax.axis_size("coil")
    tall = rows + 2 * REACH
    cells = coils * spots * rows
    layers = kernels.shape[0]
    block = channels // 2 * spots

    estimate = jnp.pad(state[0:2], ((0, 0), (0, 0), (0, 0), (0, 128 - cols)))
    estimate = jnp.broadcast_to(estimate[None], (owners, *estimate.shape))
    estimate = lax.all_to_all(estimate, "coil", 0, 0, tiled=True)

    edge_columns = [rows * d + r for d in range(groups // 2) for r in (*range(rows, rows + REACH), *range(-REACH, 0))]
    pe_columns = [*range(npe // 2), *edge_columns]
    depth = 2 * coils * spots * REACH * (npar // 128) + channels * spots * REACH
    par_factors = jnp.asarray(dft_factors(npar, range(npar // 2)))
    pe_factors = jnp.asarray(dft_factors(npe, pe_columns))
    par_table = ((npar, npar), BF16)
    pe_table = ((npe, 2 * len(pe_columns)), BF16)
    data_form = ((8 * lines, npe), F32)
    first, second, state, sens, sampled, par, pe, data = call(
        prepare,
        [((depth, 128), BF16)] * 2
        + [(state.shape, BF16), (sens.shape, F32), (mask.shape, F32)]
        + [pltpu.HBM(*form) for form in (par_table, pe_table, data_form)],
        [
            (par_factors.shape, F32),
            (pe_factors.shape, F32),
            par_table,
            pe_table,
            (kdata.shape, F32),
            (mask.shape, mask.dtype),
            data_form,
            pltpu.SemaphoreType.DMA((7,)),
            pltpu.SemaphoreType.DMA((npar // FINE // 4,)),
            pltpu.SemaphoreType.DMA((npe // FINE // 4,)),
        ],
        "prepare",
        *[in_hbm(each) for each in (state, sens, par_factors, pe_factors, kdata, mask)],
    )

    (sent,) = call(
        forward_columns,
        [jax.ShapeDtypeStruct((npar, 2 * cells), BF16)],
        [((2, 2 * cells, npar // 2), BF16), ((2, npar, 128), F32), par_table, pltpu.SemaphoreType.DMA((npar // 128,))],
        "forward_columns",
        estimate, sens, in_hbm(par),
    )
    sent, first, second = lax.optimization_barrier((sent, first, second))
    spectra = lax.all_to_all(sent, "space", 0, 0, tiled=True)
    first, second = swapped(first, "space", 0), swapped(second, "space", 1)

    (sent,) = call(
        consistency,
        [jax.ShapeDtypeStruct((npar, 384), BF16)],
        [
            ((2, 8 * lines, npe // 2), BF16),
            ((8 * lines, npe), BF16),
            ((8 * lines, npe), F32),
            pe_table,
            pltpu.SemaphoreType.DMA((npe // 256,)),
            pltpu.SemaphoreType.DMA,
        ],
        "consistency",
        spectra, in_hbm(data), sampled, in_hbm(pe),
    )
    sent, first, second = lax.optimization_barrier((sent, first, second))
    returned = lax.all_to_all(sent, "space", 0, 0, tiled=True)

    packed = [((channels * spots * REACH // 128 * tall, 128), BF16)] * 2
    tail, head = call(pack_cols, packed, [], "pack_cols", state, first, second)
    left, right = from_previous(tail, "coil"), from_next(head, "coil")

    (sent,) = call(
        backward_columns,
        [jax.ShapeDtypeStruct((owners * 2 * spots * tall, 128), BF16)],
        [
            ((2 * spots * tall, npar), F32),
            ((2, coils, spots, 2 * REACH, npar), F32),
            ((3, npar, 128), F32),
            par_table,
            pltpu.SemaphoreType.DMA((2,)),
        ],
        "backward_columns",
        returned, sens, first, second, in_hbm(par),
    )
    sent, left, right = lax.optimization_barrier((sent, left, right))
    shares = lax.all_to_all(sent, "coil", 0, 0, tiled=True)

    (spread,) = call(
        spread_state,
        [((tall * channels * spots, 128), BF16)],
        [((channels * spots * tall, 128), F32)],
        "spread_state",
        state, first, second, left, right,
    )

    weight, mixer, bias, added = call(
        coupling_weights,
        [
            ((layers, 3 * block, 3 * block), BF16),
            ((layers, block, block), BF16),
            ((layers, block, 128), F32),
            ((2, 2 * block, 128), F32),
        ],
        [],
        "coupling_weights",
        plain(kernels), plain(biases), plain(mixers), plain(inject.T),
    )
    new_state, gradient = call(
        couple,
        [jax.ShapeDtypeStruct(state.shape, BF16), jax.ShapeDtypeStruct((2, spots, rows, cols), F32)],
        [((2 * block * rows, 128), F32), ((block * tall, 128), BF16), ((block * tall, 128), BF16)],
        "couple",
        shares, spread, weight, mixer, bias, added,
    )
    return (new_state, gradient)


def solution(mesh):
    return jax.shard_map(
        per_device,
        mesh=mesh,
        in_specs=(
            P(None, None, "space", "coil"),
            P(None, "coil", None, "space", None),
            P(None, "coil", None, "space", None),
            P("space", None),
            P(),
            P(),
            P(),
            P(),
        ),
        out_specs=(P(None, None, "space", "coil"), P(None, None, "space", "coil")),
        check_vma=False,
    )
```

```python
import numpy as np

import jax
import jax.numpy as jnp
from jax import lax
from jax.experimental import pallas as pl
from jax.experimental.pallas import tpu as pltpu
from jax.sharding import PartitionSpec as P


F32 = jnp.float32
BF16 = jnp.bfloat16
REACH = 4
FINE = 32
BATCH = 38
VMEM = pl.BlockSpec(memory_space=pltpu.VMEM)
HBM = pl.BlockSpec(memory_space=pltpu.HBM)


def call(body, outs, scratch, *args):
    specs, values = [], []
    for arg in args:
        where, value = arg if isinstance(arg, tuple) else ("vmem", arg)
        if where != "plain":
            value = pltpu.with_memory_space_constraint(value, pltpu.HBM if where == "hbm" else pltpu.VMEM)
        specs.append(HBM if where == "hbm" else VMEM)
        values.append(value)
    shapes = [pltpu.VMEM(*out) if isinstance(out, tuple) else out for out in outs]
    placed = [VMEM if isinstance(out, (tuple, jax.ShapeDtypeStruct)) else HBM for out in outs]
    return pl.pallas_call(
        body,
        out_shape=shapes,
        in_specs=specs,
        out_specs=placed,
        scratch_shapes=[each if not isinstance(each, tuple) else pltpu.VMEM(*each) for each in scratch],
        compiler_params=pltpu.CompilerParams(vmem_limit_bytes=20 * 2**20),
    )(*values)


def in_hbm(value):
    return ("hbm", value)


def plain(value):
    return ("plain", value)


def table_copies(source, target, sems, step):
    copies = []
    for start in range(0, source.shape[0], step):
        here = pl.ds(start, step)
        copy = pltpu.make_async_copy(source.at[here, :], target.at[here, :], sems.at[len(copies)])
        copy.start()
        copies.append(copy)
    return copies


def sent_off(copies, source, target, sems, start, size):
    here = pl.ds(start, size)
    copy = pltpu.make_async_copy(source.at[here, :], target.at[here, :], sems.at[len(copies)])
    copy.start()
    copies.append(copy)


def arrived(block):
    for copy in block:
        copy.wait()


def dft_factors(length, columns):
    columns = np.asarray(columns)[None, :]
    steps = 2 * FINE * np.arange(length // 2 // FINE)
    coarse = np.concatenate([steps, steps + 1])[:, None] * columns % length
    fine = 2 * np.arange(FINE)[:, None] * columns % length
    angle_coarse = coarse * (2.0 * np.pi / length)
    angle_fine = fine * (2.0 * np.pi / length)
    scale = 1.0 / np.sqrt(length)
    parts = (np.cos(angle_coarse) * scale, np.sin(angle_coarse) * scale, np.cos(angle_fine), np.sin(angle_fine))
    return np.concatenate(parts).astype(np.float32)


def fill_table(factors_ref, table_hbm, table_ref, sems):
    count = table_ref.shape[0] // FINE
    width = factors_ref.shape[1]
    cos_b = factors_ref[pl.ds(2 * count, FINE), :]
    sin_b = factors_ref[pl.ds(2 * count + FINE, FINE), :]
    copies = []
    for a in range(count):
        here = pl.ds(a * FINE, FINE)
        cos, sin = factors_ref[pl.ds(a, 1), :], factors_ref[pl.ds(count + a, 1), :]
        table_ref[here, 0:width] = (cos * cos_b - sin * sin_b).astype(BF16)
        table_ref[here, width : 2 * width] = (sin * cos_b + cos * sin_b).astype(BF16)
        if a % 4 == 3:
            done = pl.ds((a - 3) * FINE, 4 * FINE)
            copy = pltpu.make_async_copy(table_ref.at[done, :], table_hbm.at[done, :], sems.at[len(copies)])
            copy.start()
            copies.append(copy)
    return copies


def prepare(
    state_hbm, sens_hbm, par_factors_hbm, pe_factors_hbm, kdata_hbm, mask_hbm,
    first_ref, second_ref, state_ref, sens_ref, sampled_ref, par_ref, par_hbm, pe_hbm, data_hbm,
    par_factors, pe_factors, pe_ref, kdata_ref, mask_ref, data_ref, sems, par_sems, pe_sems,
):
    pairs = (
        (par_factors_hbm, par_factors), (pe_factors_hbm, pe_factors), (state_hbm, state_ref), (sens_hbm, sens_ref),
        (kdata_hbm, kdata_ref), (mask_hbm, mask_ref),
    )
    copies = []
    for k, (source, target) in enumerate(pairs):
        copy = pltpu.make_async_copy(source, target, sems.at[k])
        copy.start()
        copies.append(copy)
    arrived(copies[0:1])
    sent = fill_table(par_factors, par_hbm, par_ref, par_sems)
    arrived(copies[1:2])
    sent = sent + fill_table(pe_factors, pe_hbm, pe_ref, pe_sems)
    arrived(copies[2:])
    sort_lines(kdata_ref, mask_ref, data_ref, sampled_ref)
    last = pltpu.make_async_copy(data_ref, data_hbm, sems.at[len(pairs)])
    last.start()
    pack_rows(state_ref, sens_ref, first_ref, second_ref)
    arrived(sent + [last])


def sort_lines(kdata_ref, mask_ref, data_ref, sampled_ref):
    step = 256
    row = lax.broadcasted_iota(jnp.int32, (step, step), 0)
    lane = lax.broadcasted_iota(jnp.int32, (step, step), 1)
    pick = jnp.where(row == 2 * (lane % 128) + lane // 128, 1.0, 0.0).astype(BF16)
    coils, spots, _, npe = kdata_ref.shape[1:]
    for block in range(npe // step):
        here = pl.ds(step * block, step)
        value = jnp.concatenate(
            [kdata_ref[part, c, p, :, here] for part in range(2) for c in range(coils) for p in range(spots)], axis=0
        )
        high = value.astype(BF16)
        low = (value - high.astype(F32)).astype(BF16)
        value = nn(high, pick) + nn(low, pick)
        sampled = nn(mask_ref[:, here].astype(F32).astype(BF16), pick)
        for side in range(2):
            to = pl.ds(side * npe // 2 + 128 * block, 128)
            data_ref[:, to] = value[:, 128 * side : 128 * side + 128]
            sampled_ref[:, to] = sampled[:, 128 * side : 128 * side + 128]


def swap_groups(tiles, group):
    tiles = list(tiles)
    count = len(tiles)
    lane = lax.broadcasted_iota(jnp.int32, tiles[0].shape, 1)
    bit = count // 2
    while bit:
        shift = bit * group
        high = (lane // shift) % 2 == 1
        for low in range(count):
            if low & bit:
                continue
            a, b = tiles[low], tiles[low | bit]
            tiles[low] = jnp.where(high, pltpu.roll(b, shift, 1), a)
            tiles[low | bit] = jnp.where(high, b, pltpu.roll(a, 128 - shift, 1))
        bit //= 2
    return tiles


def nn(a, b):
    return lax.dot_general(a, b, (((1,), (0,)), ((), ())), preferred_element_type=F32)


def nt(a, b):
    return lax.dot_general(a, b, (((1,), (1,)), ((), ())), preferred_element_type=F32)


def forward_columns(est_ref, sens_ref, table_ref, out_hbm, img_ref, line_ref, out_ref, sems):
    owners = est_ref.shape[0]
    coils, spots, rows, npar = sens_ref.shape[1:]
    step = 128
    width = npar // owners
    lane = lax.broadcasted_iota(jnp.int32, (rows, 128), 1)
    middle = npar // 2

    def estimate(spot, tile):
        full = []
        for part in range(2):
            value = None
            for owner in range(128 * tile // width, (128 * tile + 127) // width + 1):
                at = width * owner - 128 * tile
                piece = est_ref[owner, part, spot].astype(F32)
                if at % 128:
                    piece = pltpu.roll(piece, at % 128, 1)
                value = piece if value is None else jnp.where(lane >= at, piece, value)
            full.append(value)
        return full

    for spot in range(spots):
        for tile in range(middle // 128):
            sides = [estimate(spot, tile + side * middle // 128) for side in range(2)]
            for coil in range(coils):
                images = []
                for side in range(2):
                    cols = pl.ds(128 * tile + side * middle, 128)
                    sens_re = sens_ref[0, coil, spot, :, cols]
                    sens_im = sens_ref[1, coil, spot, :, cols]
                    est_re, est_im = sides[side]
                    images.append((sens_re * est_re - sens_im * est_im, sens_re * est_im + sens_im * est_re))
                row = (coil * spots + spot) * rows
                cols = pl.ds(128 * tile, 128)
                for part in range(2):
                    here = pl.ds(128 * part + row, rows)
                    img_ref[0, here, cols] = (images[0][part] + images[1][part]).astype(BF16)
                    img_ref[1, here, cols] = (images[0][part] - images[1][part]).astype(BF16)
    copies = []
    for start in range(0, middle, step):
        for odd in range(2):
            here = pl.ds(odd * middle + start, step)
            by_cos = nt(table_ref[here, 0:middle], img_ref[odd])
            by_sin = nt(table_ref[here, middle:npar], img_ref[odd])
            to = pl.ds(2 * start + odd, step, stride=2)
            line_ref[0, to, :] = by_cos[:, :128] + by_sin[:, 128:]
            line_ref[1, to, :] = by_cos[:, 128:] - by_sin[:, :128]
        here = pl.ds(2 * start, 2 * step)
        out_ref[here, 0:128] = line_ref[0, here, :].astype(BF16)
        out_ref[here, 128:256] = line_ref[1, here, :].astype(BF16)
        sent_off(copies, out_ref, out_hbm, sems, 2 * start, 2 * step)
    arrived(copies)


def consistency(
    recv_ref, data_hbm, sampled_ref, table_hbm, out_hbm,
    x_ref, res_ref, data_ref, table_ref, out_ref, sems, data_sem, out_sems,
):
    step = 256
    copies = table_copies(table_hbm, table_ref, sems, step)
    data_copy = pltpu.make_async_copy(data_hbm, data_ref, data_sem)
    data_copy.start()
    lines, npe = sampled_ref.shape
    middle = npe // 2
    width = table_ref.shape[1] // 2
    half = 4 * lines
    quads = npe // 128

    def gathered(quad):
        stacked = []
        for part in range(2):
            tiles = [
                recv_ref[pl.ds((4 * quad + s) * lines, lines), pl.ds(128 * part, 128)].astype(F32) for s in range(4)
            ]
            stacked += swap_groups(tiles, 32)
        return jnp.concatenate(stacked, axis=0)

    for quad in range(quads // 2):
        low, high = gathered(quad), gathered(quad + quads // 2)
        x_ref[0, :, pl.ds(128 * quad, 128)] = (low + high).astype(BF16)
        x_ref[1, :, pl.ds(128 * quad, 128)] = (low - high).astype(BF16)
    data_copy.wait()
    for odd in range(2):
        x = x_ref[odd]
        for start in range(odd * middle, (odd + 1) * middle, step):
            here = pl.ds(start, step)
            arrived(copies[start // step : start // step + 1])
            by_cos = nt(x, table_ref[here, 0:middle])
            by_sin = nt(x, table_ref[here, width : width + middle])
            sampled = jnp.concatenate([sampled_ref[:, here]] * 4, axis=0)
            real = sampled * (by_cos[:half] + by_sin[half:] - data_ref[0:half, here])
            imag = sampled * (by_cos[half:] - by_sin[:half] - data_ref[half : 2 * half, here])
            res_ref[0:half, here] = real.astype(BF16)
            res_ref[half : 2 * half, here] = imag.astype(BF16)
    res = [res_ref[:, 0:middle], res_ref[:, middle:npe]]

    off = []
    for start in (middle, *range(0, middle, step)):
        size = min(step, width - start)
        sums = []
        for odd in range(2):
            rows = pl.ds(odd * middle, middle)
            by_cos = nn(res[odd], table_ref[rows, pl.ds(start, size)])
            by_sin = nn(res[odd], table_ref[rows, pl.ds(width + start, size)])
            sums.append((by_cos[:half] - by_sin[half:], by_cos[half:] + by_sin[:half]))
        for side in range(2):
            parts = [sums[0][part] - sums[1][part] if side else sums[0][part] + sums[1][part] for part in range(2)]
            for tile in range(size // 128):
                at = slice(128 * tile, 128 * tile + 128)
                tiles = [part[lines * g : lines * (g + 1), at] for part in parts for g in range(4)]
                if start < middle:
                    quad = start // 128 + tile + side * quads // 2
                    for part in range(2):
                        for s, value in enumerate(swap_groups(tiles[4 * part : 4 * part + 4], 32)):
                            out_ref[pl.ds((4 * quad + s) * lines, lines), pl.ds(128 * part, 128)] = value.astype(BF16)
                    sent_off(off, out_ref, out_hbm, out_sems, 4 * quad * lines, 4 * lines)
                else:
                    for s, value in enumerate(swap_groups(tiles, 8)):
                        value = value.astype(BF16)
                        for half_id in range(2):
                            owner = 16 * side + 8 * half_id + s
                            out_ref[pl.ds(owner * lines, lines), 256:384] = value
    arrived(off)


def backward_columns(
    recv_ref, sens_ref, first_ref, second_ref, table_hbm, out_hbm,
    part_ref, edge_ref, line_ref, table_ref, out_ref, sems, out_sems,
):
    copies = table_copies(table_hbm, table_ref, sems, table_ref.shape[0] // 2)
    coils, spots, rows, npar = sens_ref.shape[1:]
    cells = coils * spots * rows
    edges = coils * spots * 2 * REACH
    middle = npar // 2
    low = lax.axis_index("space") // 8 % 2 == 0
    for tile in range(3):
        line_ref[tile] = recv_ref[:, 128 * tile : 128 * tile + 128].astype(F32)
    for tile in range(npar // 128):
        here = pl.ds(tile * 2 * coils * spots * REACH, 2 * coils * spots * REACH)
        above, below = around(first_ref, second_ref, here, slice(0, 128))
        for k in range(2 * coils * spots):
            at = slice(k * REACH, (k + 1) * REACH)
            part, coil, spot = k // (coils * spots), k // spots % coils, k % spots
            edge_ref[part, coil, spot, :, pl.ds(128 * tile, 128)] = jnp.concatenate([below[at], above[at]], axis=0)
    sums = []
    for odd in range(2):
        turned = [line_ref[tile, pl.ds(odd, middle, stride=2), :].T for tile in range(3)]
        border = jnp.where(low, turned[2][: 2 * edges], turned[2][2 * edges :])
        x = jnp.concatenate([turned[0], turned[1], border], axis=0).astype(BF16)
        arrived(copies[odd : odd + 1])
        sums.append(nn(x, table_ref[odd * middle : (odd + 1) * middle, :]))
    for first, count, profile_ref, offset in ((0, cells, sens_ref, 0), (2 * cells, edges, edge_ref, rows)):
        second = first + count
        last = second + count
        per_coil = count // coils
        height = per_coil // spots
        real = [each[first:second, :middle] - each[second:last, middle:] for each in sums]
        imag = [each[second:last, :middle] + each[first:second, middle:] for each in sums]
        for side in range(2):
            here = pl.ds(side * middle, middle)
            whole = [each[0] - each[1] if side else each[0] + each[1] for each in (real, imag)]
            total = [0.0, 0.0]
            for coil in range(coils):
                profile = [
                    jnp.concatenate([profile_ref[part, coil, spot, :, here] for spot in range(spots)], axis=0)
                    for part in range(2)
                ]
                re, im = [each[coil * per_coil : (coil + 1) * per_coil] for each in whole]
                total[0] = total[0] + (profile[0] * re + profile[1] * im)
                total[1] = total[1] + (profile[0] * im - profile[1] * re)
            for part in range(2):
                for spot in range(spots):
                    row = (part * spots + spot) * (rows + 2 * REACH) + offset
                    part_ref[pl.ds(row, height), here] = total[part][spot * height : (spot + 1) * height]
    total = part_ref.shape[0]
    owners = out_ref.shape[0] // total
    width = npar // owners
    lane = lax.broadcasted_iota(jnp.int32, (total, 128), 1)
    count = npar // 128
    copies = []
    for owner in range(owners):
        tile, off = divmod(width * owner, 128)
        value = part_ref[:, pl.ds(128 * tile, 128)]
        if off:
            value = pltpu.roll(value, 128 - off, 1)
            if tile + 1 < count:
                following = pltpu.roll(part_ref[:, pl.ds(128 * (tile + 1), 128)], 128 - off, 1)
                value = jnp.where((lane >= 128 - off) & (lane < 112), following, value)
        elif tile:
            value = jnp.where(lane >= 112, part_ref[:, pl.ds(128 * (tile - 1), 128)], value)
        out_ref[pl.ds(owner * total, total), :] = value.astype(BF16)
        sent_off(copies, out_ref, out_hbm, out_sems, owner * total, total)
    arrived(copies)


def pack_rows(state_ref, sens_ref, first_ref, second_ref):
    channels, _, rows, cols = state_ref.shape
    coils, npar = sens_ref.shape[1], sens_ref.shape[4]
    even = lax.axis_index("space") % 2 == 0
    at = 0

    def store(tail, head, width):
        first_ref[pl.ds(at, 8), 0:width] = jnp.where(even, tail, head).astype(BF16)
        second_ref[pl.ds(at, 8), 0:width] = jnp.where(even, head, tail).astype(BF16)

    for tile in range(npar // 128):
        here = pl.ds(128 * tile, 128)
        for part in range(2):
            for coil in range(coils):
                pair = [
                    joined_edges([sens_ref[part, coil, spot, pl.ds(low, 8), here] for spot in range(2)], low)
                    for low in (rows - 8, 0)
                ]
                store(*pair, 128)
                at += 8
    for channel in range(channels):
        pair = [
            joined_edges([state_ref[channel, spot, pl.ds(low, 8), :].astype(F32) for spot in range(2)], low)
            for low in (rows - 8, 0)
        ]
        store(*pair, cols)
        at += 8


def joined_edges(pair, low):
    first, second = pair
    if low:
        return jnp.concatenate([first[REACH:], second[REACH:]], axis=0)
    return jnp.concatenate([first[:REACH], second[:REACH]], axis=0)


def around(first_ref, second_ref, here, cols):
    even = lax.axis_index("space") % 2 == 0
    first, second = first_ref[here, cols].astype(F32), second_ref[here, cols].astype(F32)
    return jnp.where(even, second, first), jnp.where(even, first, second)


def tall_state(state_ref, first_ref, second_ref, channel, spot, skip):
    cols = state_ref.shape[3]
    above, below = around(first_ref, second_ref, pl.ds(skip + 8 * channel, 8), slice(0, cols))
    below = below[spot * REACH : (spot + 1) * REACH]
    above = above[spot * REACH : (spot + 1) * REACH]
    value = jnp.concatenate([state_ref[channel, spot].astype(F32), jnp.concatenate([below, above], axis=0)], axis=0)
    return jnp.concatenate([value, jnp.zeros((value.shape[0], 128 - cols), F32)], axis=1)


def pack_cols(state_ref, first_ref, second_ref, tail_ref, head_ref):
    channels, spots, rows, cols = state_ref.shape
    tall = rows + 2 * REACH
    skip = first_ref.shape[0] - channels * spots * REACH
    per = 128 // REACH
    lane = lax.broadcasted_iota(jnp.int32, (tall, 128), 1)
    for group in range(channels * spots // per):
        tail = head = jnp.zeros((tall, 128), F32)
        for k in range(per):
            channel, spot = divmod(group * per + k, spots)
            value = tall_state(state_ref, first_ref, second_ref, channel, spot, skip)
            here = lane // REACH == k
            tail = jnp.where(here, pltpu.roll(value, (REACH * k - cols + REACH) % 128, 1), tail)
            head = jnp.where(here, pltpu.roll(value, REACH * k, 1) if k else value, head)
        tail_ref[pl.ds(group * tall, tall), :] = tail.astype(BF16)
        head_ref[pl.ds(group * tall, tall), :] = head.astype(BF16)


def spread_state(state_ref, first_ref, second_ref, left_ref, right_ref, out_ref, wide_ref):
    channels, spots, rows, cols = state_ref.shape
    tall = rows + 2 * REACH
    half = channels // 2
    skip = first_ref.shape[0] - channels * spots * REACH
    per = 128 // REACH
    lane = lax.broadcasted_iota(jnp.int32, (tall, 128), 1)
    for channel in range(channels):
        for spot in range(spots):
            group, k = divmod(channel * spots + spot, per)
            value = tall_state(state_ref, first_ref, second_ref, channel, spot, skip)
            here = pl.ds(group * tall, tall)
            right = pltpu.roll(right_ref[here, :].astype(F32), (cols - REACH * k) % 128, 1)
            left = pltpu.roll(left_ref[here, :].astype(F32), (128 - REACH - REACH * k) % 128, 1)
            value = jnp.where((lane >= cols) & (lane < cols + REACH), right, value)
            value = jnp.where(lane >= 128 - REACH, left, value)
            at = ((channel // half * spots + spot) * half + channel % half) * tall
            wide_ref[pl.ds(at, tall), :] = value
    count = channels * spots
    for i in range(tall):
        out_ref[pl.ds(i * count, count), :] = wide_ref[pl.ds((i - REACH) % tall, count, stride=tall), :].astype(BF16)


def coupling_weights(kernels_ref, biases_ref, mixers_ref, inject_ref, weight_ref, mixer_ref, bias_ref, added_ref):
    layers = kernels_ref.shape[0]
    half = kernels_ref.shape[2]
    eye = lax.broadcasted_iota(jnp.int32, (half, half), 0) == lax.broadcasted_iota(jnp.int32, (half, half), 1)
    zero = jnp.zeros((half, half), F32)
    for layer in range(layers):
        for c in range(3):
            for out_spot in range(2):
                blocks = [
                    kernels_ref[layer, 9 * (in_spot - out_spot + 1) + 3 * b + c].astype(F32)
                    for b in range(3)
                    for in_spot in range(2)
                ]
                weight_ref[layer, pl.ds((2 * c + out_spot) * half, half), :] = jnp.concatenate(blocks, axis=1).astype(BF16)
        mixer = mixers_ref[layer].astype(F32)
        mixer_ref[layer, 0:half, :] = jnp.concatenate([mixer, zero], axis=1).astype(BF16)
        mixer_ref[layer, half : 2 * half, :] = jnp.concatenate([zero, mixer], axis=1).astype(BF16)
        row = jnp.broadcast_to(biases_ref[pl.ds(layer, 1), :], (half, half))
        column = jnp.sum(jnp.where(eye, row, 0.0), axis=1, keepdims=True)
        bias_ref[layer] = jnp.broadcast_to(jnp.concatenate([column, column], axis=0), (2 * half, 128))
    wide = lax.broadcasted_iota(jnp.int32, (2 * half, 2 * half), 0) == lax.broadcasted_iota(jnp.int32, (2 * half, 2 * half), 1)
    for part in range(2):
        row = jnp.broadcast_to(inject_ref[pl.ds(part, 1), :], (2 * half, 2 * half))
        column = jnp.broadcast_to(jnp.sum(jnp.where(wide, row, 0.0), axis=1, keepdims=True), (2 * half, 128))
        added_ref[part] = jnp.concatenate(
            [column[:half], column[:half], column[half:], column[half:]], axis=0
        )


def couple(recv_ref, state_ref, weight_ref, mixer_ref, bias_ref, inject_ref, new_ref, grad_ref, wide_ref, a_ref, b_ref):
    channels, spots, rows, cols = new_ref.shape
    tall = rows + 2 * REACH
    half = channels // 2
    block = spots * half
    total = 2 * spots * tall
    owners = recv_ref.shape[0] // total
    grad = recv_ref[0:total, :].astype(F32)
    for owner in range(1, owners):
        grad = grad + recv_ref[pl.ds(owner * total, total), :].astype(F32)
    for part in range(2):
        for spot in range(spots):
            row = (part * spots + spot) * tall
            grad_ref[part, spot] = grad[row : row + rows, :cols]
    space, coil = lax.axis_index("space"), lax.axis_index("coil")
    lane = lax.broadcasted_iota(jnp.int32, (1, 128), 1)
    col_id = coil * cols + jnp.where(lane < 112, lane, lane - 128)
    col_keep = ((col_id >= 0) & (col_id < cols * owners)).astype(F32)
    upper = jnp.where(space > 0, col_keep, 0.0)
    lower = jnp.where(space < lax.axis_size("space") - 1, col_keep, 0.0)

    def keep(i):
        return upper if i < REACH else lower if i >= REACH + rows else col_keep

    scale = [inject_ref[part] for part in range(2)]
    for i in range(tall):
        source = (i - REACH) % tall
        here = [
            jnp.concatenate(
                [
                    jnp.broadcast_to(grad[at : at + 1, :], (half, 128))
                    for at in ((part * spots + spot) * tall + source for spot in range(spots))
                ],
                axis=0,
            )
            for part in range(2)
        ]
        for which, ref in enumerate((a_ref, b_ref)):
            at = slice(which * block, (which + 1) * block)
            value = state_ref[pl.ds((2 * i + which) * block, block), :].astype(F32)
            value = value + (scale[0][at] * here[0] + scale[1][at] * here[1])
            ref[pl.ds(i * block, block), :] = (value * keep(i)).astype(BF16)
    for layer in range(weight_ref.shape[0]):
        source_ref, target_ref = (a_ref, b_ref) if layer % 2 == 0 else (b_ref, a_ref)
        weight = weight_ref[layer]
        mixer = mixer_ref[layer]
        bias = bias_ref[layer]
        first, last = 1 + layer, tall - 1 - layer
        for start in range(first, last, BATCH):
            lines = range(start, min(start + BATCH, last))
            cells = jnp.concatenate([source_ref[pl.ds((i - 1) * block, 3 * block), :] for i in lines], axis=1)
            taps = nn(weight, cells)
            raw = []
            for j in range(len(lines)):
                at = slice(128 * j, 128 * j + 128)
                value = pltpu.roll(taps[0:block, at], 1, 1) + taps[block : 2 * block, at]
                value = value + pltpu.roll(taps[2 * block :, at], 127, 1)
                raw.append(jnp.maximum(value + bias, 0.0).astype(BF16))
            mixed = nn(mixer, jnp.concatenate(raw, axis=1))
            for j, i in enumerate(lines):
                here = pl.ds(i * block, block)
                value = target_ref[here, :].astype(F32) + mixed[:, 128 * j : 128 * j + 128]
                target_ref[here, :] = (value * keep(i)).astype(BF16)
    for i in range(REACH, REACH + rows):
        source = i - REACH
        wide_ref[pl.ds(source, block, stride=rows), :] = a_ref[pl.ds(i * block, block), :].astype(F32)
        wide_ref[pl.ds(block * rows + source, block, stride=rows), :] = b_ref[pl.ds(i * block, block), :].astype(F32)
    for channel in range(channels):
        for spot in range(spots):
            at = (channel // half * block + spot * half + channel % half) * rows
            new_ref[channel, spot] = wide_ref[pl.ds(at, rows), :][:, :cols].astype(BF16)


def from_previous(tail, axis):
    return lax.ppermute(tail, axis, [(i, i + 1) for i in range(lax.axis_size(axis) - 1)])


def from_next(head, axis):
    return lax.ppermute(head, axis, [(i + 1, i) for i in range(lax.axis_size(axis) - 1)])


def swapped(array, axis, start):
    count = lax.axis_size(axis)
    pairs = [(i, i + 1) for i in range(start, count - 1, 2)]
    return lax.ppermute(array, axis, pairs + [(j, i) for i, j in pairs])


def step(state, sens, kdata, mask, inject, kernels, biases, mixers):
    channels, spots, rows, cols = state.shape
    coils = sens.shape[1]
    npar = sens.shape[4]
    npe = kdata.shape[4]
    lines = kdata.shape[3]
    groups = lax.axis_size("space")
    owners = lax.axis_size("coil")
    tall = rows + 2 * REACH
    cells = coils * spots * rows
    layers = kernels.shape[0]
    block = channels // 2 * spots

    estimate = jnp.pad(state[0:2], ((0, 0), (0, 0), (0, 0), (0, 128 - cols)))
    estimate = jnp.broadcast_to(estimate[None], (owners, *estimate.shape))
    estimate = lax.all_to_all(estimate, "coil", 0, 0, tiled=True)

    edge_columns = [rows * d + r for d in range(groups // 2) for r in (*range(rows, rows + REACH), *range(-REACH, 0))]
    pe_columns = [*range(npe // 2), *edge_columns]
    depth = 2 * coils * spots * REACH * (npar // 128) + channels * spots * REACH
    par_factors = jnp.asarray(dft_factors(npar, range(npar // 2)))
    pe_factors = jnp.asarray(dft_factors(npe, pe_columns))
    par_table = ((npar, npar), BF16)
    pe_table = ((npe, 2 * len(pe_columns)), BF16)
    data_form = ((8 * lines, npe), F32)
    first, second, state, sens, sampled, near_par, par, pe, data = call(
        prepare,
        [((depth, 128), BF16)] * 2
        + [(state.shape, BF16), (sens.shape, F32), (mask.shape, F32), par_table]
        + [pltpu.HBM(*form) for form in (par_table, pe_table, data_form)],
        [
            (par_factors.shape, F32),
            (pe_factors.shape, F32),
            pe_table,
            (kdata.shape, F32),
            (mask.shape, mask.dtype),
            data_form,
            pltpu.SemaphoreType.DMA((7,)),
            pltpu.SemaphoreType.DMA((npar // FINE // 4,)),
            pltpu.SemaphoreType.DMA((npe // FINE // 4,)),
        ],
        *[in_hbm(each) for each in (state, sens, par_factors, pe_factors, kdata, mask)],
    )

    (sent,) = call(
        forward_columns,
        [pltpu.HBM((npar, 2 * cells), BF16)],
        [
            ((2, 2 * cells, npar // 2), BF16),
            ((2, npar, 128), F32),
            ((npar, 2 * cells), BF16),
            pltpu.SemaphoreType.DMA((npar // 256,)),
        ],
        estimate, sens, near_par,
    )
    first = swapped(first, "space", 0)
    sent, second = lax.optimization_barrier((sent, second))
    spectra = lax.all_to_all(sent, "space", 0, 0, tiled=True)
    second = swapped(second, "space", 1)

    (sent,) = call(
        consistency,
        [pltpu.HBM((npar, 384), BF16)],
        [
            ((2, 8 * lines, npe // 2), BF16),
            ((8 * lines, npe), BF16),
            ((8 * lines, npe), F32),
            pe_table,
            ((npar, 384), BF16),
            pltpu.SemaphoreType.DMA((npe // 256,)),
            pltpu.SemaphoreType.DMA,
            pltpu.SemaphoreType.DMA((npe // 128,)),
        ],
        spectra, in_hbm(data), sampled, in_hbm(pe),
    )
    sent, first, second = lax.optimization_barrier((sent, first, second))
    returned = lax.all_to_all(sent, "space", 0, 0, tiled=True)

    packed = [((channels * spots * REACH // 128 * tall, 128), BF16)] * 2
    tail, head = call(pack_cols, packed, [], state, first, second)
    left, right = from_previous(tail, "coil"), from_next(head, "coil")

    (sent,) = call(
        backward_columns,
        [pltpu.HBM((owners * 2 * spots * tall, 128), BF16)],
        [
            ((2 * spots * tall, npar), F32),
            ((2, coils, spots, 2 * REACH, npar), F32),
            ((3, npar, 128), F32),
            par_table,
            ((owners * 2 * spots * tall, 128), BF16),
            pltpu.SemaphoreType.DMA((2,)),
            pltpu.SemaphoreType.DMA((owners,)),
        ],
        returned, sens, first, second, in_hbm(par),
    )
    sent, left, right = lax.optimization_barrier((sent, left, right))
    shares = lax.all_to_all(sent, "coil", 0, 0, tiled=True)

    (spread,) = call(
        spread_state,
        [((tall * channels * spots, 128), BF16)],
        [((channels * spots * tall, 128), F32)],
        state, first, second, left, right,
    )

    weight, mixer, bias, added = call(
        coupling_weights,
        [
            ((layers, 3 * block, 3 * block), BF16),
            ((layers, block, block), BF16),
            ((layers, block, 128), F32),
            ((2, 2 * block, 128), F32),
        ],
        [],
        plain(kernels), plain(biases), plain(mixers), plain(inject.T),
    )
    new_state, gradient = call(
        couple,
        [jax.ShapeDtypeStruct(state.shape, BF16), jax.ShapeDtypeStruct((2, spots, rows, cols), F32)],
        [((2 * block * rows, 128), F32), ((block * tall, 128), BF16), ((block * tall, 128), BF16)],
        shares, spread, weight, mixer, bias, added,
    )
    return (new_state, gradient)


def solution(mesh):
    return jax.shard_map(
        step,
        mesh=mesh,
        in_specs=(
            P(None, None, "space", "coil"),
            P(None, "coil", None, "space", None),
            P(None, "coil", None, "space", None),
            P("space", None),
            P(),
            P(),
            P(),
            P(),
        ),
        out_specs=(P(None, None, "space", "coil"), P(None, None, "space", "coil")),
        check_vma=False,
    )
```

```python
import numpy as np

import jax
import jax.numpy as jnp
from jax import lax
from jax.experimental import pallas as pl
from jax.experimental.pallas import tpu as pltpu
from jax.sharding import PartitionSpec as P


F32 = jnp.float32
BF16 = jnp.bfloat16
REACH = 4
FINE = 32
BATCH = 38
VMEM = pl.BlockSpec(memory_space=pltpu.VMEM)
HBM = pl.BlockSpec(memory_space=pltpu.HBM)


def call(body, outs, scratch, *args):
    specs, values = [], []
    for arg in args:
        where, value = arg if isinstance(arg, tuple) else ("vmem", arg)
        if where != "plain":
            value = pltpu.with_memory_space_constraint(value, pltpu.HBM if where == "hbm" else pltpu.VMEM)
        specs.append(HBM if where == "hbm" else VMEM)
        values.append(value)
    shapes = [pltpu.VMEM(*out) if isinstance(out, tuple) else out for out in outs]
    placed = [VMEM if isinstance(out, (tuple, jax.ShapeDtypeStruct)) else HBM for out in outs]
    return pl.pallas_call(
        body,
        out_shape=shapes,
        in_specs=specs,
        out_specs=placed,
        scratch_shapes=[each if not isinstance(each, tuple) else pltpu.VMEM(*each) for each in scratch],
        compiler_params=pltpu.CompilerParams(vmem_limit_bytes=20 * 2**20),
    )(*values)


def in_hbm(value):
    return ("hbm", value)


def plain(value):
    return ("plain", value)


def table_copies(source, target, sems, step):
    copies = []
    for start in range(0, source.shape[0], step):
        here = pl.ds(start, step)
        copy = pltpu.make_async_copy(source.at[here, :], target.at[here, :], sems.at[len(copies)])
        copy.start()
        copies.append(copy)
    return copies


def sent_off(copies, source, target, sems, start, size):
    here = pl.ds(start, size)
    copy = pltpu.make_async_copy(source.at[here, :], target.at[here, :], sems.at[len(copies)])
    copy.start()
    copies.append(copy)


def arrived(block):
    for copy in block:
        copy.wait()


def dft_factors(length, columns):
    columns = np.asarray(columns)[None, :]
    steps = 2 * FINE * np.arange(length // 2 // FINE)
    coarse = np.concatenate([steps, steps + 1])[:, None] * columns % length
    fine = 2 * np.arange(FINE)[:, None] * columns % length
    angle_coarse = coarse * (2.0 * np.pi / length)
    angle_fine = fine * (2.0 * np.pi / length)
    scale = 1.0 / np.sqrt(length)
    parts = (np.cos(angle_coarse) * scale, np.sin(angle_coarse) * scale, np.cos(angle_fine), np.sin(angle_fine))
    return np.concatenate(parts).astype(np.float32)


def fill_table(factors_ref, table_hbm, table_ref, sems):
    count = table_ref.shape[0] // FINE
    width = factors_ref.shape[1]
    cos_b = factors_ref[pl.ds(2 * count, FINE), :]
    sin_b = factors_ref[pl.ds(2 * count + FINE, FINE), :]
    copies = []
    for a in range(count):
        here = pl.ds(a * FINE, FINE)
        cos, sin = factors_ref[pl.ds(a, 1), :], factors_ref[pl.ds(count + a, 1), :]
        table_ref[here, 0:width] = (cos * cos_b - sin * sin_b).astype(BF16)
        table_ref[here, width : 2 * width] = (sin * cos_b + cos * sin_b).astype(BF16)
        if a % 4 == 3:
            done = pl.ds((a - 3) * FINE, 4 * FINE)
            copy = pltpu.make_async_copy(table_ref.at[done, :], table_hbm.at[done, :], sems.at[len(copies)])
            copy.start()
            copies.append(copy)
    return copies


def prepare(
    state_hbm, sens_hbm, par_factors_hbm, pe_factors_hbm, kdata_hbm, mask_hbm,
    first_ref, second_ref, sens_ref, sampled_ref, par_ref, data_ref, par_hbm, pe_hbm,
    par_factors, pe_factors, pe_ref, kdata_ref, mask_ref, state_ref, sems, par_sems, pe_sems,
):
    pairs = (
        (par_factors_hbm, par_factors), (pe_factors_hbm, pe_factors), (state_hbm, state_ref), (sens_hbm, sens_ref),
        (kdata_hbm, kdata_ref), (mask_hbm, mask_ref),
    )
    copies = []
    for k, (source, target) in enumerate(pairs):
        copy = pltpu.make_async_copy(source, target, sems.at[k])
        copy.start()
        copies.append(copy)
    arrived(copies[0:1])
    sent = fill_table(par_factors, par_hbm, par_ref, par_sems)
    arrived(copies[1:2])
    sent = sent + fill_table(pe_factors, pe_hbm, pe_ref, pe_sems)
    arrived(copies[2:])
    sort_lines(kdata_ref, mask_ref, data_ref, sampled_ref)
    pack_rows(state_ref, sens_ref, first_ref, second_ref)
    arrived(sent)


def sort_lines(kdata_ref, mask_ref, data_ref, sampled_ref):
    step = 256
    row = lax.broadcasted_iota(jnp.int32, (step, step), 0)
    lane = lax.broadcasted_iota(jnp.int32, (step, step), 1)
    pick = jnp.where(row == 2 * (lane % 128) + lane // 128, 1.0, 0.0).astype(BF16)
    coils, spots, _, npe = kdata_ref.shape[1:]
    for block in range(npe // step):
        here = pl.ds(step * block, step)
        value = jnp.concatenate(
            [kdata_ref[part, c, p, :, here] for part in range(2) for c in range(coils) for p in range(spots)], axis=0
        )
        value = nn(value.astype(BF16), pick).astype(BF16)
        sampled = nn(mask_ref[:, here].astype(F32).astype(BF16), pick)
        for side in range(2):
            to = pl.ds(side * npe // 2 + 128 * block, 128)
            data_ref[:, to] = value[:, 128 * side : 128 * side + 128]
            sampled_ref[:, to] = sampled[:, 128 * side : 128 * side + 128]


def swap_groups(tiles, group):
    tiles = list(tiles)
    count = len(tiles)
    lane = lax.broadcasted_iota(jnp.int32, tiles[0].shape, 1)
    bit = count // 2
    while bit:
        shift = bit * group
        high = (lane // shift) % 2 == 1
        for low in range(count):
            if low & bit:
                continue
            a, b = tiles[low], tiles[low | bit]
            tiles[low] = jnp.where(high, pltpu.roll(b, shift, 1), a)
            tiles[low | bit] = jnp.where(high, b, pltpu.roll(a, 128 - shift, 1))
        bit //= 2
    return tiles


def nn(a, b):
    return lax.dot_general(a, b, (((1,), (0,)), ((), ())), preferred_element_type=F32)


def nt(a, b):
    return lax.dot_general(a, b, (((1,), (1,)), ((), ())), preferred_element_type=F32)


def forward_columns(est_ref, sens_ref, table_ref, out_hbm, img_ref, line_ref, out_ref, sems):
    owners = est_ref.shape[0]
    coils, spots, rows, npar = sens_ref.shape[1:]
    step = 128
    width = npar // owners
    lane = lax.broadcasted_iota(jnp.int32, (rows, 128), 1)
    middle = npar // 2

    def estimate(spot, tile):
        full = []
        for part in range(2):
            value = None
            for owner in range(128 * tile // width, (128 * tile + 127) // width + 1):
                at = width * owner - 128 * tile
                piece = est_ref[owner, part, spot].astype(F32)
                if at % 128:
                    piece = pltpu.roll(piece, at % 128, 1)
                value = piece if value is None else jnp.where(lane >= at, piece, value)
            full.append(value)
        return full

    for spot in range(spots):
        for tile in range(middle // 128):
            sides = [estimate(spot, tile + side * middle // 128) for side in range(2)]
            for coil in range(coils):
                images = []
                for side in range(2):
                    cols = pl.ds(128 * tile + side * middle, 128)
                    sens_re = sens_ref[0, coil, spot, :, cols]
                    sens_im = sens_ref[1, coil, spot, :, cols]
                    est_re, est_im = sides[side]
                    images.append((sens_re * est_re - sens_im * est_im, sens_re * est_im + sens_im * est_re))
                row = (coil * spots + spot) * rows
                cols = pl.ds(128 * tile, 128)
                for part in range(2):
                    here = pl.ds(128 * part + row, rows)
                    img_ref[0, here, cols] = (images[0][part] + images[1][part]).astype(BF16)
                    img_ref[1, here, cols] = (images[0][part] - images[1][part]).astype(BF16)
    copies = []
    for start in range(0, middle, step):
        for odd in range(2):
            here = pl.ds(odd * middle + start, step)
            by_cos = nt(table_ref[here, 0:middle], img_ref[odd])
            by_sin = nt(table_ref[here, middle:npar], img_ref[odd])
            to = pl.ds(2 * start + odd, step, stride=2)
            line_ref[0, to, :] = by_cos[:, :128] + by_sin[:, 128:]
            line_ref[1, to, :] = by_cos[:, 128:] - by_sin[:, :128]
        here = pl.ds(2 * start, 2 * step)
        out_ref[here, 0:128] = line_ref[0, here, :].astype(BF16)
        out_ref[here, 128:256] = line_ref[1, here, :].astype(BF16)
        sent_off(copies, out_ref, out_hbm, sems, 2 * start, 2 * step)
    arrived(copies)


def consistency(
    recv_ref, data_ref, sampled_ref, table_hbm, out_hbm, x_ref, res_ref, table_ref, out_ref, sems, out_sems
):
    step = 256
    copies = table_copies(table_hbm, table_ref, sems, step)
    lines, npe = sampled_ref.shape
    middle = npe // 2
    width = table_ref.shape[1] // 2
    half = 4 * lines
    quads = npe // 128

    def gathered(quad):
        stacked = []
        for part in range(2):
            tiles = [
                recv_ref[pl.ds((4 * quad + s) * lines, lines), pl.ds(128 * part, 128)].astype(F32) for s in range(4)
            ]
            stacked += swap_groups(tiles, 32)
        return jnp.concatenate(stacked, axis=0)

    for quad in range(quads // 2):
        low, high = gathered(quad), gathered(quad + quads // 2)
        x_ref[0, :, pl.ds(128 * quad, 128)] = (low + high).astype(BF16)
        x_ref[1, :, pl.ds(128 * quad, 128)] = (low - high).astype(BF16)
    for odd in range(2):
        x = x_ref[odd]
        for start in range(odd * middle, (odd + 1) * middle, step):
            here = pl.ds(start, step)
            arrived(copies[start // step : start // step + 1])
            by_cos = nt(x, table_ref[here, 0:middle])
            by_sin = nt(x, table_ref[here, width : width + middle])
            sampled = jnp.concatenate([sampled_ref[:, here]] * 4, axis=0)
            real = sampled * (by_cos[:half] + by_sin[half:] - data_ref[0:half, here].astype(F32))
            imag = sampled * (by_cos[half:] - by_sin[:half] - data_ref[half : 2 * half, here].astype(F32))
            res_ref[0:half, here] = real.astype(BF16)
            res_ref[half : 2 * half, here] = imag.astype(BF16)
    res = [res_ref[:, 0:middle], res_ref[:, middle:npe]]

    off = []
    for start in (middle, *range(0, middle, step)):
        size = min(step, width - start)
        sums = []
        for odd in range(2):
            rows = pl.ds(odd * middle, middle)
            by_cos = nn(res[odd], table_ref[rows, pl.ds(start, size)])
            by_sin = nn(res[odd], table_ref[rows, pl.ds(width + start, size)])
            sums.append((by_cos[:half] - by_sin[half:], by_cos[half:] + by_sin[:half]))
        for side in range(2):
            parts = [sums[0][part] - sums[1][part] if side else sums[0][part] + sums[1][part] for part in range(2)]
            for tile in range(size // 128):
                at = slice(128 * tile, 128 * tile + 128)
                tiles = [part[lines * g : lines * (g + 1), at] for part in parts for g in range(4)]
                if start < middle:
                    quad = start // 128 + tile + side * quads // 2
                    for part in range(2):
                        for s, value in enumerate(swap_groups(tiles[4 * part : 4 * part + 4], 32)):
                            out_ref[pl.ds((4 * quad + s) * lines, lines), pl.ds(128 * part, 128)] = value.astype(BF16)
                    sent_off(off, out_ref, out_hbm, out_sems, 4 * quad * lines, 4 * lines)
                else:
                    for s, value in enumerate(swap_groups(tiles, 8)):
                        value = value.astype(BF16)
                        for half_id in range(2):
                            owner = 16 * side + 8 * half_id + s
                            out_ref[pl.ds(owner * lines, lines), 256:384] = value
    arrived(off)


def backward_columns(
    recv_ref, sens_ref, first_ref, second_ref, table_hbm, out_hbm,
    part_ref, edge_ref, line_ref, table_ref, out_ref, sems, out_sems,
):
    copies = table_copies(table_hbm, table_ref, sems, table_ref.shape[0] // 2)
    coils, spots, rows, npar = sens_ref.shape[1:]
    cells = coils * spots * rows
    edges = coils * spots * 2 * REACH
    middle = npar // 2
    low = lax.axis_index("space") // 8 % 2 == 0
    for tile in range(3):
        line_ref[tile] = recv_ref[:, 128 * tile : 128 * tile + 128].astype(F32)
    for tile in range(npar // 128):
        here = pl.ds(tile * 2 * coils * spots * REACH, 2 * coils * spots * REACH)
        above, below = around(first_ref, second_ref, here, slice(0, 128))
        for k in range(2 * coils * spots):
            at = slice(k * REACH, (k + 1) * REACH)
            part, coil, spot = k // (coils * spots), k // spots % coils, k % spots
            edge_ref[part, coil, spot, :, pl.ds(128 * tile, 128)] = jnp.concatenate([below[at], above[at]], axis=0)
    sums = []
    for odd in range(2):
        turned = [line_ref[tile, pl.ds(odd, middle, stride=2), :].T for tile in range(3)]
        border = jnp.where(low, turned[2][: 2 * edges], turned[2][2 * edges :])
        x = jnp.concatenate([turned[0], turned[1], border], axis=0).astype(BF16)
        arrived(copies[odd : odd + 1])
        sums.append(nn(x, table_ref[odd * middle : (odd + 1) * middle, :]))
    for first, count, profile_ref, offset in ((0, cells, sens_ref, 0), (2 * cells, edges, edge_ref, rows)):
        second = first + count
        last = second + count
        per_coil = count // coils
        height = per_coil // spots
        real = [each[first:second, :middle] - each[second:last, middle:] for each in sums]
        imag = [each[second:last, :middle] + each[first:second, middle:] for each in sums]
        for side in range(2):
            here = pl.ds(side * middle, middle)
            whole = [each[0] - each[1] if side else each[0] + each[1] for each in (real, imag)]
            total = [0.0, 0.0]
            for coil in range(coils):
                profile = [
                    jnp.concatenate([profile_ref[part, coil, spot, :, here] for spot in range(spots)], axis=0)
                    for part in range(2)
                ]
                re, im = [each[coil * per_coil : (coil + 1) * per_coil] for each in whole]
                total[0] = total[0] + (profile[0] * re + profile[1] * im)
                total[1] = total[1] + (profile[0] * im - profile[1] * re)
            for part in range(2):
                for spot in range(spots):
                    row = (part * spots + spot) * (rows + 2 * REACH) + offset
                    part_ref[pl.ds(row, height), here] = total[part][spot * height : (spot + 1) * height]
    total = part_ref.shape[0]
    owners = out_ref.shape[0] // total
    width = npar // owners
    lane = lax.broadcasted_iota(jnp.int32, (total, 128), 1)
    count = npar // 128
    copies = []
    for owner in range(owners):
        tile, off = divmod(width * owner, 128)
        value = part_ref[:, pl.ds(128 * tile, 128)]
        if off:
            value = pltpu.roll(value, 128 - off, 1)
            if tile + 1 < count:
                following = pltpu.roll(part_ref[:, pl.ds(128 * (tile + 1), 128)], 128 - off, 1)
                value = jnp.where((lane >= 128 - off) & (lane < 112), following, value)
        elif tile:
            value = jnp.where(lane >= 112, part_ref[:, pl.ds(128 * (tile - 1), 128)], value)
        out_ref[pl.ds(owner * total, total), :] = value.astype(BF16)
        sent_off(copies, out_ref, out_hbm, out_sems, owner * total, total)
    arrived(copies)


def pack_rows(state_ref, sens_ref, first_ref, second_ref):
    channels, _, rows, cols = state_ref.shape
    coils, npar = sens_ref.shape[1], sens_ref.shape[4]
    even = lax.axis_index("space") % 2 == 0
    at = 0

    def store(tail, head, width):
        first_ref[pl.ds(at, 8), 0:width] = jnp.where(even, tail, head).astype(BF16)
        second_ref[pl.ds(at, 8), 0:width] = jnp.where(even, head, tail).astype(BF16)

    for tile in range(npar // 128):
        here = pl.ds(128 * tile, 128)
        for part in range(2):
            for coil in range(coils):
                pair = [
                    joined_edges([sens_ref[part, coil, spot, pl.ds(low, 8), here] for spot in range(2)], low)
                    for low in (rows - 8, 0)
                ]
                store(*pair, 128)
                at += 8
    for channel in range(channels):
        pair = [
            joined_edges([state_ref[channel, spot, pl.ds(low, 8), :].astype(F32) for spot in range(2)], low)
            for low in (rows - 8, 0)
        ]
        store(*pair, cols)
        at += 8


def joined_edges(pair, low):
    first, second = pair
    if low:
        return jnp.concatenate([first[REACH:], second[REACH:]], axis=0)
    return jnp.concatenate([first[:REACH], second[:REACH]], axis=0)


def around(first_ref, second_ref, here, cols):
    even = lax.axis_index("space") % 2 == 0
    first, second = first_ref[here, cols].astype(F32), second_ref[here, cols].astype(F32)
    return jnp.where(even, second, first), jnp.where(even, first, second)


def tall_state(state_ref, first_ref, second_ref, channel, spot, skip):
    cols = state_ref.shape[3]
    above, below = around(first_ref, second_ref, pl.ds(skip + 8 * channel, 8), slice(0, cols))
    below = below[spot * REACH : (spot + 1) * REACH]
    above = above[spot * REACH : (spot + 1) * REACH]
    value = jnp.concatenate([state_ref[channel, spot].astype(F32), jnp.concatenate([below, above], axis=0)], axis=0)
    return jnp.concatenate([value, jnp.zeros((value.shape[0], 128 - cols), F32)], axis=1)


def pack_cols(state_ref, first_ref, second_ref, tail_ref, head_ref):
    channels, spots, rows, cols = state_ref.shape
    tall = rows + 2 * REACH
    skip = first_ref.shape[0] - channels * spots * REACH
    per = 128 // REACH
    lane = lax.broadcasted_iota(jnp.int32, (tall, 128), 1)
    for group in range(channels * spots // per):
        tail = head = jnp.zeros((tall, 128), F32)
        for k in range(per):
            channel, spot = divmod(group * per + k, spots)
            value = tall_state(state_ref, first_ref, second_ref, channel, spot, skip)
            here = lane // REACH == k
            tail = jnp.where(here, pltpu.roll(value, (REACH * k - cols + REACH) % 128, 1), tail)
            head = jnp.where(here, pltpu.roll(value, REACH * k, 1) if k else value, head)
        tail_ref[pl.ds(group * tall, tall), :] = tail.astype(BF16)
        head_ref[pl.ds(group * tall, tall), :] = head.astype(BF16)


def spread_state(state_ref, first_ref, second_ref, left_ref, right_ref, out_ref, wide_ref):
    channels, spots, rows, cols = state_ref.shape
    tall = rows + 2 * REACH
    half = channels // 2
    skip = first_ref.shape[0] - channels * spots * REACH
    per = 128 // REACH
    lane = lax.broadcasted_iota(jnp.int32, (tall, 128), 1)
    for channel in range(channels):
        for spot in range(spots):
            group, k = divmod(channel * spots + spot, per)
            value = tall_state(state_ref, first_ref, second_ref, channel, spot, skip)
            here = pl.ds(group * tall, tall)
            right = pltpu.roll(right_ref[here, :].astype(F32), (cols - REACH * k) % 128, 1)
            left = pltpu.roll(left_ref[here, :].astype(F32), (128 - REACH - REACH * k) % 128, 1)
            value = jnp.where((lane >= cols) & (lane < cols + REACH), right, value)
            value = jnp.where(lane >= 128 - REACH, left, value)
            at = ((channel // half * spots + spot) * half + channel % half) * tall
            wide_ref[pl.ds(at, tall), :] = value
    count = channels * spots
    for i in range(tall):
        out_ref[pl.ds(i * count, count), :] = wide_ref[pl.ds((i - REACH) % tall, count, stride=tall), :].astype(BF16)


def coupling_weights(kernels_ref, biases_ref, mixers_ref, inject_ref, weight_ref, mixer_ref, bias_ref, added_ref):
    layers = kernels_ref.shape[0]
    half = kernels_ref.shape[2]
    eye = lax.broadcasted_iota(jnp.int32, (half, half), 0) == lax.broadcasted_iota(jnp.int32, (half, half), 1)
    zero = jnp.zeros((half, half), F32)
    for layer in range(layers):
        for c in range(3):
            for out_spot in range(2):
                blocks = [
                    kernels_ref[layer, 9 * (in_spot - out_spot + 1) + 3 * b + c].astype(F32)
                    for b in range(3)
                    for in_spot in range(2)
                ]
                weight_ref[layer, pl.ds((2 * c + out_spot) * half, half), :] = jnp.concatenate(blocks, axis=1).astype(BF16)
        mixer = mixers_ref[layer].astype(F32)
        mixer_ref[layer, 0:half, :] = jnp.concatenate([mixer, zero], axis=1).astype(BF16)
        mixer_ref[layer, half : 2 * half, :] = jnp.concatenate([zero, mixer], axis=1).astype(BF16)
        row = jnp.broadcast_to(biases_ref[pl.ds(layer, 1), :], (half, half))
        column = jnp.sum(jnp.where(eye, row, 0.0), axis=1, keepdims=True)
        bias_ref[layer] = jnp.broadcast_to(jnp.concatenate([column, column], axis=0), (2 * half, 128))
    wide = lax.broadcasted_iota(jnp.int32, (2 * half, 2 * half), 0) == lax.broadcasted_iota(jnp.int32, (2 * half, 2 * half), 1)
    for part in range(2):
        row = jnp.broadcast_to(inject_ref[pl.ds(part, 1), :], (2 * half, 2 * half))
        column = jnp.broadcast_to(jnp.sum(jnp.where(wide, row, 0.0), axis=1, keepdims=True), (2 * half, 128))
        added_ref[part] = jnp.concatenate(
            [column[:half], column[:half], column[half:], column[half:]], axis=0
        )


def couple(
    recv_ref, state_ref, weight_ref, mixer_ref, bias_ref, inject_ref, new_hbm, grad_hbm,
    wide_ref, a_ref, b_ref, new_ref, grad_ref, sems,
):
    channels, spots, rows, cols = new_hbm.shape
    tall = rows + 2 * REACH
    half = channels // 2
    block = spots * half
    total = 2 * spots * tall
    owners = recv_ref.shape[0] // total
    grad = recv_ref[0:total, :].astype(F32)
    for owner in range(1, owners):
        grad = grad + recv_ref[pl.ds(owner * total, total), :].astype(F32)
    for part in range(2):
        for spot in range(spots):
            row = (part * spots + spot) * tall
            grad_ref[part, spot] = grad[row : row + rows, :cols]
    copies = [pltpu.make_async_copy(grad_ref, grad_hbm, sems.at[0])]
    copies[0].start()

    def finish(ref, which):
        for source in range(rows):
            to = pl.ds(which * block * rows + source, block, stride=rows)
            wide_ref[to, :] = ref[pl.ds((source + REACH) * block, block), :].astype(F32)
        for channel in range(half):
            for spot in range(spots):
                at = (which * block + spot * half + channel) * rows
                new_ref[which * half + channel, spot] = wide_ref[pl.ds(at, rows), :][:, :cols].astype(BF16)
            if channel % 4 == 3:
                here = pl.ds(which * half + channel - 3, 4)
                copy = pltpu.make_async_copy(new_ref.at[here], new_hbm.at[here], sems.at[len(copies)])
                copy.start()
                copies.append(copy)

    space, coil = lax.axis_index("space"), lax.axis_index("coil")
    lane = lax.broadcasted_iota(jnp.int32, (1, 128), 1)
    col_id = coil * cols + jnp.where(lane < 112, lane, lane - 128)
    col_keep = ((col_id >= 0) & (col_id < cols * owners)).astype(F32)
    upper = jnp.where(space > 0, col_keep, 0.0)
    lower = jnp.where(space < lax.axis_size("space") - 1, col_keep, 0.0)

    def keep(i):
        return upper if i < REACH else lower if i >= REACH + rows else col_keep

    scale = [inject_ref[part] for part in range(2)]
    for i in range(tall):
        source = (i - REACH) % tall
        here = [
            jnp.concatenate(
                [
                    jnp.broadcast_to(grad[at : at + 1, :], (half, 128))
                    for at in ((part * spots + spot) * tall + source for spot in range(spots))
                ],
                axis=0,
            )
            for part in range(2)
        ]
        for which, ref in enumerate((a_ref, b_ref)):
            at = slice(which * block, (which + 1) * block)
            value = state_ref[pl.ds((2 * i + which) * block, block), :].astype(F32)
            value = value + (scale[0][at] * here[0] + scale[1][at] * here[1])
            ref[pl.ds(i * block, block), :] = (value * keep(i)).astype(BF16)
    for layer in range(weight_ref.shape[0]):
        source_ref, target_ref = (a_ref, b_ref) if layer % 2 == 0 else (b_ref, a_ref)
        weight = weight_ref[layer]
        mixer = mixer_ref[layer]
        bias = bias_ref[layer]
        first, last = 1 + layer, tall - 1 - layer
        for start in range(first, last, BATCH):
            lines = range(start, min(start + BATCH, last))
            cells = jnp.concatenate([source_ref[pl.ds((i - 1) * block, 3 * block), :] for i in lines], axis=1)
            taps = nn(weight, cells)
            raw = []
            for j in range(len(lines)):
                at = slice(128 * j, 128 * j + 128)
                value = pltpu.roll(taps[0:block, at], 1, 1) + taps[block : 2 * block, at]
                value = value + pltpu.roll(taps[2 * block :, at], 127, 1)
                raw.append(jnp.maximum(value + bias, 0.0).astype(BF16))
            mixed = nn(mixer, jnp.concatenate(raw, axis=1))
            for j, i in enumerate(lines):
                here = pl.ds(i * block, block)
                value = target_ref[here, :].astype(F32) + mixed[:, 128 * j : 128 * j + 128]
                target_ref[here, :] = (value * keep(i)).astype(BF16)
        if layer >= weight_ref.shape[0] - 2:
            finish(target_ref, 1 - layer % 2)
    arrived(copies)


def from_previous(tail, axis):
    return lax.ppermute(tail, axis, [(i, i + 1) for i in range(lax.axis_size(axis) - 1)])


def from_next(head, axis):
    return lax.ppermute(head, axis, [(i + 1, i) for i in range(lax.axis_size(axis) - 1)])


def swapped(array, axis, start):
    count = lax.axis_size(axis)
    pairs = [(i, i + 1) for i in range(start, count - 1, 2)]
    return lax.ppermute(array, axis, pairs + [(j, i) for i, j in pairs])


def step(state, sens, kdata, mask, inject, kernels, biases, mixers):
    channels, spots, rows, cols = state.shape
    coils = sens.shape[1]
    npar = sens.shape[4]
    npe = kdata.shape[4]
    lines = kdata.shape[3]
    groups = lax.axis_size("space")
    owners = lax.axis_size("coil")
    tall = rows + 2 * REACH
    cells = coils * spots * rows
    layers = kernels.shape[0]
    block = channels // 2 * spots

    estimate = jnp.pad(state[0:2], ((0, 0), (0, 0), (0, 0), (0, 128 - cols)))
    estimate = jnp.broadcast_to(estimate[None], (owners, *estimate.shape))
    estimate = lax.all_to_all(estimate, "coil", 0, 0, tiled=True)

    edge_columns = [rows * d + r for d in range(groups // 2) for r in (*range(rows, rows + REACH), *range(-REACH, 0))]
    pe_columns = [*range(npe // 2), *edge_columns]
    depth = 2 * coils * spots * REACH * (npar // 128) + channels * spots * REACH
    par_factors = jnp.asarray(dft_factors(npar, range(npar // 2)))
    pe_factors = jnp.asarray(dft_factors(npe, pe_columns))
    par_table = ((npar, npar), BF16)
    pe_table = ((npe, 2 * len(pe_columns)), BF16)
    data_form = ((8 * lines, npe), BF16)
    first, second, sens, sampled, near_par, data, par, pe = call(
        prepare,
        [((depth, 128), BF16)] * 2
        + [(sens.shape, F32), (mask.shape, F32), par_table, data_form]
        + [pltpu.HBM(*form) for form in (par_table, pe_table)],
        [
            (par_factors.shape, F32),
            (pe_factors.shape, F32),
            pe_table,
            (kdata.shape, F32),
            (mask.shape, mask.dtype),
            (state.shape, BF16),
            pltpu.SemaphoreType.DMA((6,)),
            pltpu.SemaphoreType.DMA((npar // FINE // 4,)),
            pltpu.SemaphoreType.DMA((npe // FINE // 4,)),
        ],
        *[in_hbm(each) for each in (state, sens, par_factors, pe_factors, kdata, mask)],
    )

    (sent,) = call(
        forward_columns,
        [pltpu.HBM((npar, 2 * cells), BF16)],
        [
            ((2, 2 * cells, npar // 2), BF16),
            ((2, npar, 128), F32),
            ((npar, 2 * cells), BF16),
            pltpu.SemaphoreType.DMA((npar // 256,)),
        ],
        estimate, sens, near_par,
    )
    first = swapped(first, "space", 0)
    sent, second = lax.optimization_barrier((sent, second))
    spectra = lax.all_to_all(sent, "space", 0, 0, tiled=True)
    second = swapped(second, "space", 1)

    (sent,) = call(
        consistency,
        [pltpu.HBM((npar, 384), BF16)],
        [
            ((2, 8 * lines, npe // 2), BF16),
            ((8 * lines, npe), BF16),
            pe_table,
            ((npar, 384), BF16),
            pltpu.SemaphoreType.DMA((npe // 256,)),
            pltpu.SemaphoreType.DMA((npe // 128,)),
        ],
        spectra, data, sampled, in_hbm(pe),
    )
    sent, first, second = lax.optimization_barrier((sent, first, second))
    returned = lax.all_to_all(sent, "space", 0, 0, tiled=True)

    packed = [((channels * spots * REACH // 128 * tall, 128), BF16)] * 2
    tail, head = call(pack_cols, packed, [], plain(state), first, second)
    left, right = from_previous(tail, "coil"), from_next(head, "coil")

    (sent,) = call(
        backward_columns,
        [pltpu.HBM((owners * 2 * spots * tall, 128), BF16)],
        [
            ((2 * spots * tall, npar), F32),
            ((2, coils, spots, 2 * REACH, npar), F32),
            ((3, npar, 128), F32),
            par_table,
            ((owners * 2 * spots * tall, 128), BF16),
            pltpu.SemaphoreType.DMA((2,)),
            pltpu.SemaphoreType.DMA((owners,)),
        ],
        returned, sens, first, second, in_hbm(par),
    )
    sent, left, right = lax.optimization_barrier((sent, left, right))
    shares = lax.all_to_all(sent, "coil", 0, 0, tiled=True)

    (spread,) = call(
        spread_state,
        [((tall * channels * spots, 128), BF16)],
        [((channels * spots * tall, 128), F32)],
        plain(state), first, second, left, right,
    )

    weight, mixer, bias, added = call(
        coupling_weights,
        [
            ((layers, 3 * block, 3 * block), BF16),
            ((layers, block, block), BF16),
            ((layers, block, 128), F32),
            ((2, 2 * block, 128), F32),
        ],
        [],
        plain(kernels), plain(biases), plain(mixers), plain(inject.T),
    )
    new_state, gradient = call(
        couple,
        [pltpu.HBM(state.shape, BF16), pltpu.HBM((2, spots, rows, cols), F32)],
        [
            ((2 * block * rows, 128), F32),
            ((block * tall, 128), BF16),
            ((block * tall, 128), BF16),
            (state.shape, BF16),
            ((2, spots, rows, cols), F32),
            pltpu.SemaphoreType.DMA((1 + channels // 4,)),
        ],
        shares, spread, weight, mixer, bias, added,
    )
    return (new_state, gradient)


def solution(mesh):
    return jax.shard_map(
        step,
        mesh=mesh,
        in_specs=(
            P(None, None, "space", "coil"),
            P(None, "coil", None, "space", None),
            P(None, "coil", None, "space", None),
            P("space", None),
            P(),
            P(),
            P(),
            P(),
        ),
        out_specs=(P(None, None, "space", "coil"), P(None, None, "space", "coil")),
        check_vma=False,
    )
```

```python
import numpy as np

import jax
import jax.numpy as jnp
from jax import lax
from jax.experimental import pallas as pl
from jax.experimental.pallas import tpu as pltpu
from jax.sharding import PartitionSpec as P

F32 = jnp.float32
BF16 = jnp.bfloat16
REACH = 4
FINE = 32
BATCH = 38
VMEM = pl.BlockSpec(memory_space=pltpu.VMEM)
HBM = pl.BlockSpec(memory_space=pltpu.HBM)


def call(body, outs, scratch, name, *args):
    specs, values = [], []
    for arg in args:
        where, value = arg if isinstance(arg, tuple) else ("vmem", arg)
        if where != "plain":
            value = pltpu.with_memory_space_constraint(value, pltpu.HBM if where == "hbm" else pltpu.VMEM)
        specs.append(HBM if where == "hbm" else VMEM)
        values.append(value)
    shapes = [pltpu.VMEM(*out) if isinstance(out, tuple) else out for out in outs]
    placed = [VMEM if isinstance(out, (tuple, jax.ShapeDtypeStruct)) else HBM for out in outs]
    return pl.pallas_call(
        body,
        out_shape=shapes,
        in_specs=specs,
        out_specs=placed,
        scratch_shapes=[each if not isinstance(each, tuple) else pltpu.VMEM(*each) for each in scratch],
        compiler_params=pltpu.CompilerParams(vmem_limit_bytes=20 * 2**20),
        name=name,
    )(*values)


def in_hbm(value):
    return ("hbm", value)


def plain(value):
    return ("plain", value)


def table_copies(source, target, sems, step):
    copies = []
    for start in range(0, source.shape[0], step):
        here = pl.ds(start, step)
        copy = pltpu.make_async_copy(source.at[here, :], target.at[here, :], sems.at[len(copies)])
        copy.start()
        copies.append(copy)
    return copies


def sent_off(copies, source, target, sems, start, size):
    here = pl.ds(start, size)
    copy = pltpu.make_async_copy(source.at[here, :], target.at[here, :], sems.at[len(copies)])
    copy.start()
    copies.append(copy)


def arrived(block):
    for copy in block:
        copy.wait()


def dft_factors(length, columns):
    columns = np.asarray(columns)[None, :]
    steps = 2 * FINE * np.arange(length // 2 // FINE)
    coarse = np.concatenate([steps, steps + 1])[:, None] * columns % length
    fine = 2 * np.arange(FINE)[:, None] * columns % length
    angle_coarse = coarse * (2.0 * np.pi / length)
    angle_fine = fine * (2.0 * np.pi / length)
    scale = 1.0 / np.sqrt(length)
    parts = (np.cos(angle_coarse) * scale, np.sin(angle_coarse) * scale, np.cos(angle_fine), np.sin(angle_fine))
    return np.concatenate(parts).astype(np.float32)


def fill_table(factors_ref, table_hbm, table_ref, sems):
    count = table_ref.shape[0] // FINE
    width = factors_ref.shape[1]
    cos_b = factors_ref[pl.ds(2 * count, FINE), :]
    sin_b = factors_ref[pl.ds(2 * count + FINE, FINE), :]
    copies = []
    for a in range(count):
        here = pl.ds(a * FINE, FINE)
        cos, sin = factors_ref[pl.ds(a, 1), :], factors_ref[pl.ds(count + a, 1), :]
        table_ref[here, 0:width] = (cos * cos_b - sin * sin_b).astype(BF16)
        table_ref[here, width : 2 * width] = (sin * cos_b + cos * sin_b).astype(BF16)
        if a % 4 == 3:
            done = pl.ds((a - 3) * FINE, 4 * FINE)
            copy = pltpu.make_async_copy(table_ref.at[done, :], table_hbm.at[done, :], sems.at[len(copies)])
            copy.start()
            copies.append(copy)
    return copies


def prepare(
    state_hbm, sens_hbm, par_factors_hbm, pe_factors_hbm, kdata_hbm, mask_hbm,
    first_ref, second_ref, sens_ref, sampled_ref, par_ref, data_ref, par_hbm, pe_hbm,
    par_factors, pe_factors, pe_ref, kdata_ref, mask_ref, state_ref, sems, par_sems, pe_sems,
):
    pairs = (
        (par_factors_hbm, par_factors), (pe_factors_hbm, pe_factors), (state_hbm, state_ref), (sens_hbm, sens_ref),
        (kdata_hbm, kdata_ref), (mask_hbm, mask_ref),
    )
    copies = []
    for k, (source, target) in enumerate(pairs):
        copy = pltpu.make_async_copy(source, target, sems.at[k])
        copy.start()
        copies.append(copy)
    arrived(copies[0:1])
    sent = fill_table(par_factors, par_hbm, par_ref, par_sems)
    arrived(copies[1:2])
    sent = sent + fill_table(pe_factors, pe_hbm, pe_ref, pe_sems)
    arrived(copies[2:])
    sort_lines(kdata_ref, mask_ref, data_ref, sampled_ref)
    pack_rows(state_ref, sens_ref, first_ref, second_ref)
    arrived(sent)


def sort_lines(kdata_ref, mask_ref, data_ref, sampled_ref):
    step = 256
    row = lax.broadcasted_iota(jnp.int32, (step, step), 0)
    lane = lax.broadcasted_iota(jnp.int32, (step, step), 1)
    pick = jnp.where(row == 2 * (lane % 128) + lane // 128, 1.0, 0.0).astype(BF16)
    coils, spots, lines, npe = kdata_ref.shape[1:]
    for block in range(npe // step):
        here = pl.ds(step * block, step)
        value = jnp.concatenate(
            [kdata_ref[part, c, p, :, here] for part in range(2) for c in range(coils) for p in range(spots)], axis=0
        )
        value = nn(value.astype(BF16), pick).astype(BF16)
        sampled = nn(mask_ref[:, here].astype(F32).astype(BF16), pick)
        for side in range(2):
            to = pl.ds(side * npe // 2 + 128 * block, 128)
            data_ref[:, to] = value[:, 128 * side : 128 * side + 128]
            sampled_ref[:, to] = sampled[:, 128 * side : 128 * side + 128]


def swap_groups(tiles, group):
    tiles = list(tiles)
    count = len(tiles)
    lane = lax.broadcasted_iota(jnp.int32, tiles[0].shape, 1)
    bit = count // 2
    while bit:
        shift = bit * group
        high = (lane // shift) % 2 == 1
        for low in range(count):
            if low & bit:
                continue
            a, b = tiles[low], tiles[low | bit]
            tiles[low] = jnp.where(high, pltpu.roll(b, shift, 1), a)
            tiles[low | bit] = jnp.where(high, b, pltpu.roll(a, 128 - shift, 1))
        bit //= 2
    return tiles


def nn(a, b):
    return lax.dot_general(a, b, (((1,), (0,)), ((), ())), preferred_element_type=F32)


def nt(a, b):
    return lax.dot_general(a, b, (((1,), (1,)), ((), ())), preferred_element_type=F32)


def forward_columns(est_ref, sens_ref, table_ref, out_hbm, img_ref, line_ref, out_ref, sems):
    owners = est_ref.shape[0]
    coils, spots, rows, npar = sens_ref.shape[1:]
    step = 128
    width = npar // owners
    lane = lax.broadcasted_iota(jnp.int32, (rows, 128), 1)
    middle = npar // 2

    def estimate(spot, tile):
        full = []
        for part in range(2):
            value = None
            for owner in range(128 * tile // width, (128 * tile + 127) // width + 1):
                at = width * owner - 128 * tile
                piece = est_ref[owner, part, spot].astype(F32)
                if at % 128:
                    piece = pltpu.roll(piece, at % 128, 1)
                value = piece if value is None else jnp.where(lane >= at, piece, value)
            full.append(value)
        return full

    for spot in range(spots):
        for tile in range(middle // 128):
            sides = [estimate(spot, tile + side * middle // 128) for side in range(2)]
            for coil in range(coils):
                images = []
                for side in range(2):
                    cols = pl.ds(128 * tile + side * middle, 128)
                    sens_re = sens_ref[0, coil, spot, :, cols]
                    sens_im = sens_ref[1, coil, spot, :, cols]
                    est_re, est_im = sides[side]
                    images.append((sens_re * est_re - sens_im * est_im, sens_re * est_im + sens_im * est_re))
                row = (coil * spots + spot) * rows
                cols = pl.ds(128 * tile, 128)
                for part in range(2):
                    here = pl.ds(128 * part + row, rows)
                    img_ref[0, here, cols] = (images[0][part] + images[1][part]).astype(BF16)
                    img_ref[1, here, cols] = (images[0][part] - images[1][part]).astype(BF16)
    copies = []
    for start in range(0, middle, step):
        for odd in range(2):
            here = pl.ds(odd * middle + start, step)
            by_cos = nt(table_ref[here, 0:middle], img_ref[odd])
            by_sin = nt(table_ref[here, middle:npar], img_ref[odd])
            to = pl.ds(2 * start + odd, step, stride=2)
            line_ref[0, to, :] = by_cos[:, :128] + by_sin[:, 128:]
            line_ref[1, to, :] = by_cos[:, 128:] - by_sin[:, :128]
        here = pl.ds(2 * start, 2 * step)
        out_ref[here, 0:128] = line_ref[0, here, :].astype(BF16)
        out_ref[here, 128:256] = line_ref[1, here, :].astype(BF16)
        sent_off(copies, out_ref, out_hbm, sems, 2 * start, 2 * step)
    arrived(copies)


def consistency(
    recv_ref, data_ref, sampled_ref, table_hbm, out_hbm, x_ref, res_ref, table_ref, out_ref, sems, out_sems
):
    step = 256
    copies = table_copies(table_hbm, table_ref, sems, step)
    lines, npe = sampled_ref.shape
    middle = npe // 2
    width = table_ref.shape[1] // 2
    half = 4 * lines
    quads = npe // 128

    def gathered(quad):
        stacked = []
        for part in range(2):
            tiles = [
                recv_ref[pl.ds((4 * quad + s) * lines, lines), pl.ds(128 * part, 128)].astype(F32) for s in range(4)
            ]
            stacked += swap_groups(tiles, 32)
        return jnp.concatenate(stacked, axis=0)

    for quad in range(quads // 2):
        low, high = gathered(quad), gathered(quad + quads // 2)
        x_ref[0, :, pl.ds(128 * quad, 128)] = (low + high).astype(BF16)
        x_ref[1, :, pl.ds(128 * quad, 128)] = (low - high).astype(BF16)
    for odd in range(2):
        x = x_ref[odd]
        for start in range(odd * middle, (odd + 1) * middle, step):
            here = pl.ds(start, step)
            arrived(copies[start // step : start // step + 1])
            by_cos = nt(x, table_ref[here, 0:middle])
            by_sin = nt(x, table_ref[here, width : width + middle])
            sampled = jnp.concatenate([sampled_ref[:, here]] * 4, axis=0)
            real = sampled * (by_cos[:half] + by_sin[half:] - data_ref[0:half, here].astype(F32))
            imag = sampled * (by_cos[half:] - by_sin[:half] - data_ref[half : 2 * half, here].astype(F32))
            res_ref[0:half, here] = real.astype(BF16)
            res_ref[half : 2 * half, here] = imag.astype(BF16)
    res = [res_ref[:, 0:middle], res_ref[:, middle:npe]]

    off = []
    for start in (middle, *range(0, middle, step)):
        size = min(step, width - start)
        sums = []
        for odd in range(2):
            rows = pl.ds(odd * middle, middle)
            by_cos = nn(res[odd], table_ref[rows, pl.ds(start, size)])
            by_sin = nn(res[odd], table_ref[rows, pl.ds(width + start, size)])
            sums.append((by_cos[:half] - by_sin[half:], by_cos[half:] + by_sin[:half]))
        for side in range(2):
            parts = [sums[0][part] - sums[1][part] if side else sums[0][part] + sums[1][part] for part in range(2)]
            for tile in range(size // 128):
                at = slice(128 * tile, 128 * tile + 128)
                tiles = [part[lines * g : lines * (g + 1), at] for part in parts for g in range(4)]
                if start < middle:
                    quad = start // 128 + tile + side * quads // 2
                    for part in range(2):
                        for s, value in enumerate(swap_groups(tiles[4 * part : 4 * part + 4], 32)):
                            out_ref[pl.ds((4 * quad + s) * lines, lines), pl.ds(128 * part, 128)] = value.astype(BF16)
                    sent_off(off, out_ref, out_hbm, out_sems, 4 * quad * lines, 4 * lines)
                else:
                    for s, value in enumerate(swap_groups(tiles, 8)):
                        value = value.astype(BF16)
                        for half_id in range(2):
                            owner = 16 * side + 8 * half_id + s
                            out_ref[pl.ds(owner * lines, lines), 256:384] = value
    arrived(off)


def backward_columns(
    recv_ref, sens_ref, first_ref, second_ref, table_hbm, out_hbm,
    part_ref, edge_ref, line_ref, table_ref, out_ref, sems, out_sems,
):
    copies = table_copies(table_hbm, table_ref, sems, table_ref.shape[0] // 2)
    coils, spots, rows, npar = sens_ref.shape[1:]
    cells = coils * spots * rows
    edges = coils * spots * 2 * REACH
    middle = npar // 2
    low = lax.axis_index("space") // 8 % 2 == 0
    for tile in range(3):
        line_ref[tile] = recv_ref[:, 128 * tile : 128 * tile + 128].astype(F32)
    for tile in range(npar // 128):
        here = pl.ds(tile * 2 * coils * spots * REACH, 2 * coils * spots * REACH)
        above, below = around(first_ref, second_ref, here, slice(0, 128))
        for k in range(2 * coils * spots):
            at = slice(k * REACH, (k + 1) * REACH)
            part, coil, spot = k // (coils * spots), k // spots % coils, k % spots
            edge_ref[part, coil, spot, :, pl.ds(128 * tile, 128)] = jnp.concatenate([below[at], above[at]], axis=0)
    sums = []
    for odd in range(2):
        turned = [line_ref[tile, pl.ds(odd, middle, stride=2), :].T for tile in range(3)]
        border = jnp.where(low, turned[2][: 2 * edges], turned[2][2 * edges :])
        x = jnp.concatenate([turned[0], turned[1], border], axis=0).astype(BF16)
        arrived(copies[odd : odd + 1])
        sums.append(nn(x, table_ref[odd * middle : (odd + 1) * middle, :]))
    for first, count, profile_ref, offset in ((0, cells, sens_ref, 0), (2 * cells, edges, edge_ref, rows)):
        second = first + count
        last = second + count
        per_coil = count // coils
        height = per_coil // spots
        real = [each[first:second, :middle] - each[second:last, middle:] for each in sums]
        imag = [each[second:last, :middle] + each[first:second, middle:] for each in sums]
        for side in range(2):
            here = pl.ds(side * middle, middle)
            whole = [each[0] - each[1] if side else each[0] + each[1] for each in (real, imag)]
            total = [0.0, 0.0]
            for coil in range(coils):
                profile = [
                    jnp.concatenate([profile_ref[part, coil, spot, :, here] for spot in range(spots)], axis=0)
                    for part in range(2)
                ]
                re, im = [each[coil * per_coil : (coil + 1) * per_coil] for each in whole]
                total[0] = total[0] + (profile[0] * re + profile[1] * im)
                total[1] = total[1] + (profile[0] * im - profile[1] * re)
            for part in range(2):
                for spot in range(spots):
                    row = (part * spots + spot) * (rows + 2 * REACH) + offset
                    part_ref[pl.ds(row, height), here] = total[part][spot * height : (spot + 1) * height]
    total = part_ref.shape[0]
    owners = out_ref.shape[0] // total
    width = npar // owners
    lane = lax.broadcasted_iota(jnp.int32, (total, 128), 1)
    count = npar // 128
    copies = []
    for owner in range(owners):
        tile, off = divmod(width * owner, 128)
        value = part_ref[:, pl.ds(128 * tile, 128)]
        if off:
            value = pltpu.roll(value, 128 - off, 1)
            if tile + 1 < count:
                following = pltpu.roll(part_ref[:, pl.ds(128 * (tile + 1), 128)], 128 - off, 1)
                value = jnp.where((lane >= 128 - off) & (lane < 112), following, value)
        elif tile:
            value = jnp.where(lane >= 112, part_ref[:, pl.ds(128 * (tile - 1), 128)], value)
        out_ref[pl.ds(owner * total, total), :] = value.astype(BF16)
        sent_off(copies, out_ref, out_hbm, out_sems, owner * total, total)
    arrived(copies)


def pack_rows(state_ref, sens_ref, first_ref, second_ref):
    channels, spots, rows, cols = state_ref.shape
    coils, npar = sens_ref.shape[1], sens_ref.shape[4]
    even = lax.axis_index("space") % 2 == 0
    at = 0

    def store(tail, head, width):
        first_ref[pl.ds(at, 8), 0:width] = jnp.where(even, tail, head).astype(BF16)
        second_ref[pl.ds(at, 8), 0:width] = jnp.where(even, head, tail).astype(BF16)

    for tile in range(npar // 128):
        here = pl.ds(128 * tile, 128)
        for part in range(2):
            for coil in range(coils):
                pair = [
                    joined_edges([sens_ref[part, coil, spot, pl.ds(low, 8), here] for spot in range(2)], low)
                    for low in (rows - 8, 0)
                ]
                store(*pair, 128)
                at += 8
    for channel in range(channels):
        pair = [
            joined_edges([state_ref[channel, spot, pl.ds(low, 8), :].astype(F32) for spot in range(2)], low)
            for low in (rows - 8, 0)
        ]
        store(*pair, cols)
        at += 8


def joined_edges(pair, low):
    first, second = pair
    if low:
        return jnp.concatenate([first[REACH:], second[REACH:]], axis=0)
    return jnp.concatenate([first[:REACH], second[:REACH]], axis=0)


def around(first_ref, second_ref, here, cols):
    even = lax.axis_index("space") % 2 == 0
    first, second = first_ref[here, cols].astype(F32), second_ref[here, cols].astype(F32)
    return jnp.where(even, second, first), jnp.where(even, first, second)


def tall_state(state_ref, first_ref, second_ref, channel, spot, skip):
    cols = state_ref.shape[3]
    above, below = around(first_ref, second_ref, pl.ds(skip + 8 * channel, 8), slice(0, cols))
    below = below[spot * REACH : (spot + 1) * REACH]
    above = above[spot * REACH : (spot + 1) * REACH]
    value = jnp.concatenate([state_ref[channel, spot].astype(F32), jnp.concatenate([below, above], axis=0)], axis=0)
    return jnp.concatenate([value, jnp.zeros((value.shape[0], 128 - cols), F32)], axis=1)


def pack_cols(state_ref, first_ref, second_ref, tail_ref, head_ref):
    channels, spots, rows, cols = state_ref.shape
    tall = rows + 2 * REACH
    skip = first_ref.shape[0] - channels * spots * REACH
    per = 128 // REACH
    lane = lax.broadcasted_iota(jnp.int32, (tall, 128), 1)
    for group in range(channels * spots // per):
        tail = head = jnp.zeros((tall, 128), F32)
        for k in range(per):
            channel, spot = divmod(group * per + k, spots)
            value = tall_state(state_ref, first_ref, second_ref, channel, spot, skip)
            here = lane // REACH == k
            tail = jnp.where(here, pltpu.roll(value, (REACH * k - cols + REACH) % 128, 1), tail)
            head = jnp.where(here, pltpu.roll(value, REACH * k, 1) if k else value, head)
        tail_ref[pl.ds(group * tall, tall), :] = tail.astype(BF16)
        head_ref[pl.ds(group * tall, tall), :] = head.astype(BF16)


def spread_state(state_ref, first_ref, second_ref, left_ref, right_ref, out_ref, wide_ref):
    channels, spots, rows, cols = state_ref.shape
    tall = rows + 2 * REACH
    half = channels // 2
    skip = first_ref.shape[0] - channels * spots * REACH
    per = 128 // REACH
    lane = lax.broadcasted_iota(jnp.int32, (tall, 128), 1)
    for channel in range(channels):
        for spot in range(spots):
            group, k = divmod(channel * spots + spot, per)
            value = tall_state(state_ref, first_ref, second_ref, channel, spot, skip)
            here = pl.ds(group * tall, tall)
            right = pltpu.roll(right_ref[here, :].astype(F32), (cols - REACH * k) % 128, 1)
            left = pltpu.roll(left_ref[here, :].astype(F32), (128 - REACH - REACH * k) % 128, 1)
            value = jnp.where((lane >= cols) & (lane < cols + REACH), right, value)
            value = jnp.where(lane >= 128 - REACH, left, value)
            at = ((channel // half * spots + spot) * half + channel % half) * tall
            wide_ref[pl.ds(at, tall), :] = value
    count = channels * spots
    for i in range(tall):
        out_ref[pl.ds(i * count, count), :] = wide_ref[pl.ds((i - REACH) % tall, count, stride=tall), :].astype(BF16)


def coupling_weights(kernels_ref, biases_ref, mixers_ref, inject_ref, weight_ref, mixer_ref, bias_ref, added_ref):
    layers = kernels_ref.shape[0]
    half = kernels_ref.shape[2]
    eye = lax.broadcasted_iota(jnp.int32, (half, half), 0) == lax.broadcasted_iota(jnp.int32, (half, half), 1)
    zero = jnp.zeros((half, half), F32)
    for layer in range(layers):
        for c in range(3):
            for out_spot in range(2):
                blocks = [
                    kernels_ref[layer, 9 * (in_spot - out_spot + 1) + 3 * b + c].astype(F32)
                    for b in range(3)
                    for in_spot in range(2)
                ]
                weight_ref[layer, pl.ds((2 * c + out_spot) * half, half), :] = jnp.concatenate(blocks, axis=1).astype(BF16)
        mixer = mixers_ref[layer].astype(F32)
        mixer_ref[layer, 0:half, :] = jnp.concatenate([mixer, zero], axis=1).astype(BF16)
        mixer_ref[layer, half : 2 * half, :] = jnp.concatenate([zero, mixer], axis=1).astype(BF16)
        row = jnp.broadcast_to(biases_ref[pl.ds(layer, 1), :], (half, half))
        column = jnp.sum(jnp.where(eye, row, 0.0), axis=1, keepdims=True)
        bias_ref[layer] = jnp.broadcast_to(jnp.concatenate([column, column], axis=0), (2 * half, 128))
    wide = lax.broadcasted_iota(jnp.int32, (2 * half, 2 * half), 0) == lax.broadcasted_iota(jnp.int32, (2 * half, 2 * half), 1)
    for part in range(2):
        row = jnp.broadcast_to(inject_ref[pl.ds(part, 1), :], (2 * half, 2 * half))
        column = jnp.broadcast_to(jnp.sum(jnp.where(wide, row, 0.0), axis=1, keepdims=True), (2 * half, 128))
        added_ref[part] = jnp.concatenate(
            [column[:half], column[:half], column[half:], column[half:]], axis=0
        )


def couple(
    recv_ref, state_ref, weight_ref, mixer_ref, bias_ref, inject_ref, new_hbm, grad_hbm,
    wide_ref, a_ref, b_ref, new_ref, grad_ref, sems,
):
    channels, spots, rows, cols = new_hbm.shape
    tall = rows + 2 * REACH
    half = channels // 2
    block = spots * half
    total = 2 * spots * tall
    owners = recv_ref.shape[0] // total
    grad = recv_ref[0:total, :].astype(F32)
    for owner in range(1, owners):
        grad = grad + recv_ref[pl.ds(owner * total, total), :].astype(F32)
    for part in range(2):
        for spot in range(spots):
            row = (part * spots + spot) * tall
            grad_ref[part, spot] = grad[row : row + rows, :cols]
    copies = [pltpu.make_async_copy(grad_ref, grad_hbm, sems.at[0])]
    copies[0].start()

    def finish(ref, which):
        for source in range(rows):
            to = pl.ds(which * block * rows + source, block, stride=rows)
            wide_ref[to, :] = ref[pl.ds((source + REACH) * block, block), :].astype(F32)
        for channel in range(half):
            for spot in range(spots):
                at = (which * block + spot * half + channel) * rows
                new_ref[which * half + channel, spot] = wide_ref[pl.ds(at, rows), :][:, :cols].astype(BF16)
            if channel % 4 == 3:
                here = pl.ds(which * half + channel - 3, 4)
                copy = pltpu.make_async_copy(new_ref.at[here], new_hbm.at[here], sems.at[len(copies)])
                copy.start()
                copies.append(copy)

    space, coil = lax.axis_index("space"), lax.axis_index("coil")
    lane = lax.broadcasted_iota(jnp.int32, (1, 128), 1)
    col_id = coil * cols + jnp.where(lane < 112, lane, lane - 128)
    col_keep = ((col_id >= 0) & (col_id < cols * owners)).astype(F32)
    upper = jnp.where(space > 0, col_keep, 0.0)
    lower = jnp.where(space < lax.axis_size("space") - 1, col_keep, 0.0)

    def keep(i):
        return upper if i < REACH else lower if i >= REACH + rows else col_keep

    scale = [inject_ref[part] for part in range(2)]
    for i in range(tall):
        source = (i - REACH) % tall
        here = [
            jnp.concatenate(
                [
                    jnp.broadcast_to(grad[at : at + 1, :], (half, 128))
                    for at in ((part * spots + spot) * tall + source for spot in range(spots))
                ],
                axis=0,
            )
            for part in range(2)
        ]
        for which, ref in enumerate((a_ref, b_ref)):
            at = slice(which * block, (which + 1) * block)
            value = state_ref[pl.ds((2 * i + which) * block, block), :].astype(F32)
            value = value + (scale[0][at] * here[0] + scale[1][at] * here[1])
            ref[pl.ds(i * block, block), :] = (value * keep(i)).astype(BF16)
    for layer in range(weight_ref.shape[0]):
        source_ref, target_ref = (a_ref, b_ref) if layer % 2 == 0 else (b_ref, a_ref)
        weight = weight_ref[layer]
        mixer = mixer_ref[layer]
        bias = bias_ref[layer]
        first, last = 1 + layer, tall - 1 - layer
        for start in range(first, last, BATCH):
            lines = range(start, min(start + BATCH, last))
            cells = jnp.concatenate([source_ref[pl.ds((i - 1) * block, 3 * block), :] for i in lines], axis=1)
            taps = nn(weight, cells)
            raw = []
            for j in range(len(lines)):
                at = slice(128 * j, 128 * j + 128)
                value = pltpu.roll(taps[0:block, at], 1, 1) + taps[block : 2 * block, at]
                value = value + pltpu.roll(taps[2 * block :, at], 127, 1)
                raw.append(jnp.maximum(value + bias, 0.0).astype(BF16))
            mixed = nn(mixer, jnp.concatenate(raw, axis=1))
            for j, i in enumerate(lines):
                here = pl.ds(i * block, block)
                value = target_ref[here, :].astype(F32) + mixed[:, 128 * j : 128 * j + 128]
                target_ref[here, :] = (value * keep(i)).astype(BF16)
        if layer >= weight_ref.shape[0] - 2:
            finish(target_ref, 1 - layer % 2)
    arrived(copies)


def from_previous(tail, axis):
    return lax.ppermute(tail, axis, [(i, i + 1) for i in range(lax.axis_size(axis) - 1)])


def from_next(head, axis):
    return lax.ppermute(head, axis, [(i + 1, i) for i in range(lax.axis_size(axis) - 1)])


def swapped(array, axis, start):
    count = lax.axis_size(axis)
    pairs = [(i, i + 1) for i in range(start, count - 1, 2)]
    return lax.ppermute(array, axis, pairs + [(j, i) for i, j in pairs])


def per_device(state, sens, kdata, mask, inject, kernels, biases, mixers):
    channels, spots, rows, cols = state.shape
    coils = sens.shape[1]
    npar = sens.shape[4]
    npe = kdata.shape[4]
    lines = kdata.shape[3]
    groups = lax.axis_size("space")
    owners = lax.axis_size("coil")
    tall = rows + 2 * REACH
    cells = coils * spots * rows
    layers = kernels.shape[0]
    block = channels // 2 * spots

    estimate = jnp.pad(state[0:2], ((0, 0), (0, 0), (0, 0), (0, 128 - cols)))
    estimate = jnp.broadcast_to(estimate[None], (owners, *estimate.shape))
    estimate = lax.all_to_all(estimate, "coil", 0, 0, tiled=True)

    edge_columns = [rows * d + r for d in range(groups // 2) for r in (*range(rows, rows + REACH), *range(-REACH, 0))]
    pe_columns = [*range(npe // 2), *edge_columns]
    depth = 2 * coils * spots * REACH * (npar // 128) + channels * spots * REACH
    par_factors = jnp.asarray(dft_factors(npar, range(npar // 2)))
    pe_factors = jnp.asarray(dft_factors(npe, pe_columns))
    par_table = ((npar, npar), BF16)
    pe_table = ((npe, 2 * len(pe_columns)), BF16)
    data_form = ((8 * lines, npe), BF16)
    first, second, sens, sampled, near_par, data, par, pe = call(
        prepare,
        [((depth, 128), BF16)] * 2
        + [(sens.shape, F32), (mask.shape, F32), par_table, data_form]
        + [pltpu.HBM(*form) for form in (par_table, pe_table)],
        [
            (par_factors.shape, F32),
            (pe_factors.shape, F32),
            pe_table,
            (kdata.shape, F32),
            (mask.shape, mask.dtype),
            (state.shape, BF16),
            pltpu.SemaphoreType.DMA((6,)),
            pltpu.SemaphoreType.DMA((npar // FINE // 4,)),
            pltpu.SemaphoreType.DMA((npe // FINE // 4,)),
        ],
        "prepare",
        *[in_hbm(each) for each in (state, sens, par_factors, pe_factors, kdata, mask)],
    )

    (sent,) = call(
        forward_columns,
        [pltpu.HBM((npar, 2 * cells), BF16)],
        [
            ((2, 2 * cells, npar // 2), BF16),
            ((2, npar, 128), F32),
            ((npar, 2 * cells), BF16),
            pltpu.SemaphoreType.DMA((npar // 256,)),
        ],
        "forward_columns",
        estimate, sens, near_par,
    )
    sent, first, second = lax.optimization_barrier((sent, first, second))
    spectra = lax.all_to_all(sent, "space", 0, 0, tiled=True)
    first, second = swapped(first, "space", 0), swapped(second, "space", 1)

    (sent,) = call(
        consistency,
        [pltpu.HBM((npar, 384), BF16)],
        [
            ((2, 8 * lines, npe // 2), BF16),
            ((8 * lines, npe), BF16),
            pe_table,
            ((npar, 384), BF16),
            pltpu.SemaphoreType.DMA((npe // 256,)),
            pltpu.SemaphoreType.DMA((npe // 128,)),
        ],
        "consistency",
        spectra, data, sampled, in_hbm(pe),
    )
    sent, first, second = lax.optimization_barrier((sent, first, second))
    returned = lax.all_to_all(sent, "space", 0, 0, tiled=True)

    packed = [((channels * spots * REACH // 128 * tall, 128), BF16)] * 2
    tail, head = call(pack_cols, packed, [], "pack_cols", plain(state), first, second)
    left, right = from_previous(tail, "coil"), from_next(head, "coil")

    (sent,) = call(
        backward_columns,
        [pltpu.HBM((owners * 2 * spots * tall, 128), BF16)],
        [
            ((2 * spots * tall, npar), F32),
            ((2, coils, spots, 2 * REACH, npar), F32),
            ((3, npar, 128), F32),
            par_table,
            ((owners * 2 * spots * tall, 128), BF16),
            pltpu.SemaphoreType.DMA((2,)),
            pltpu.SemaphoreType.DMA((owners,)),
        ],
        "backward_columns",
        returned, sens, first, second, in_hbm(par),
    )
    sent, left, right = lax.optimization_barrier((sent, left, right))
    shares = lax.all_to_all(sent, "coil", 0, 0, tiled=True)

    (spread,) = call(
        spread_state,
        [((tall * channels * spots, 128), BF16)],
        [((channels * spots * tall, 128), F32)],
        "spread_state",
        plain(state), first, second, left, right,
    )

    weight, mixer, bias, added = call(
        coupling_weights,
        [
            ((layers, 3 * block, 3 * block), BF16),
            ((layers, block, block), BF16),
            ((layers, block, 128), F32),
            ((2, 2 * block, 128), F32),
        ],
        [],
        "coupling_weights",
        plain(kernels), plain(biases), plain(mixers), plain(inject.T),
    )
    new_state, gradient = call(
        couple,
        [pltpu.HBM(state.shape, BF16), pltpu.HBM((2, spots, rows, cols), F32)],
        [
            ((2 * block * rows, 128), F32),
            ((block * tall, 128), BF16),
            ((block * tall, 128), BF16),
            (state.shape, BF16),
            ((2, spots, rows, cols), F32),
            pltpu.SemaphoreType.DMA((1 + channels // 4,)),
        ],
        "couple",
        shares, spread, weight, mixer, bias, added,
    )
    return (new_state, gradient)


def solution(mesh):
    return jax.shard_map(
        per_device,
        mesh=mesh,
        in_specs=(
            P(None, None, "space", "coil"),
            P(None, "coil", None, "space", None),
            P(None, "coil", None, "space", None),
            P("space", None),
            P(),
            P(),
            P(),
            P(),
        ),
        out_specs=(P(None, None, "space", "coil"), P(None, None, "space", "coil")),
        check_vma=False,
    )
```
